32 devices in a mesh: dp: 2 (over x), ctx: 4 (over y, core), head: 4 (over z).
Axes of the slice: x: 2, y: 2, z: 4, core: 2. Of those that a mesh axis runs over, the one named last changes fastest.
Arguments:
- inputs: bfloat16 [2, 8, 512, 1536], P('dp', 'ctx', 'head'), may hold values from -6 to 6
- block_order: int32 [2, 8], P('dp'), may hold values from 0 to 7, each once within a row
- mixer_gain: float32 [1536], replicated, may hold values from 0.5 to 1.5
- query_weight: bfloat16 [1536, 1536], P(None, 'head'), may hold values from -0.15625 to 0.15625
- key_weight: bfloat16 [1536, 1536], P(None, 'head'), may hold values from -0.15625 to 0.15625
- value_weight: bfloat16 [1536, 1536], P(None, 'head'), may hold values from -0.15625 to 0.15625
- lambda_qone: float32 [12, 64], P('head'), may hold values from -0.6 to 0.6
- lambda_kone: float32 [12, 64], P('head'), may hold values from -0.6 to 0.6
- lambda_qtwo: float32 [12, 64], P('head'), may hold values from -0.6 to 0.6
- lambda_ktwo: float32 [12, 64], P('head'), may hold values from -0.6 to 0.6
- group_gain: float32 [1536], P('head'), may hold values from 0.5 to 1.5
- output_weight: bfloat16 [1536, 1536], P('head'), may hold values from -0.625 to 0.625
- feed_gain: float32 [1536], replicated, may hold values from 0.5 to 1.5
- gate_weight: bfloat16 [1536, 4096], P(None, 'head'), may hold values from -0.15625 to 0.15625
- up_weight: bfloat16 [1536, 4096], P(None, 'head'), may hold values from -0.15625 to 0.15625
- down_weight: bfloat16 [4096, 1536], P('head'), may hold values from -0.1875 to 0.1875
- cotangent: bfloat16 [2, 8, 512, 1536], P('dp', 'ctx', 'head'), may hold values from -6 to 6
Outputs:
- block_out: bfloat16 [2, 8, 512, 1536], P('dp', 'ctx', 'head')
- input_grad: float32 [2, 8, 512, 1536], P('dp', 'ctx', 'head')
- mixer_grad: float32 [1536], replicated
- query_grad: float32 [1536, 1536], P(('dp', 'ctx'), 'head')
- key_grad: float32 [1536, 1536], P(('dp', 'ctx'), 'head')
- value_grad: float32 [1536, 1536], P(('dp', 'ctx'), 'head')
- qone_grad: float32 [12, 64], P('head')
- kone_grad: float32 [12, 64], P('head')
- qtwo_grad: float32 [12, 64], P('head')
- ktwo_grad: float32 [12, 64], P('head')
- group_grad: float32 [1536], P('head')
- output_grad: float32 [1536, 1536], P('head', ('dp', 'ctx'))
- feed_grad: float32 [1536], replicated
- gate_grad: float32 [1536, 4096], P(('dp', 'ctx'), 'head')
- up_grad: float32 [1536, 4096], P(('dp', 'ctx'), 'head')
- down_grad: float32 [4096, 1536], P('head', ('dp', 'ctx'))
The draws below stay inside these ranges and needn't reach their ends.
Inputs may be any that keep to these rules, and one draw needn't show every extreme that they name: `block_order`: row s lists, for each of the 8 slots of sequence s, which of its 8 blocks of 512 consecutive positions that slot holds; each block once.
All inputs are finite; a program needn't handle non-finite values.
Results may differ from the reference program's by a relative error of at most 0.023.
Values may be sent and summed in bfloat16 or wider, within the bound.
A program may use at most 192 MiB of HBM per device.

```python
import math
import jax
import jax.numpy as jnp
from jax import lax

D = 1536
H = 12
HD = 64
FF = 4096
BLOCK_POSITIONS = 512
BLOCK_COUNT = 8
SEQS = 2


def with_spikes(entries, rng, source, target, shards_of, factor):
    owner, partner = [(jnp.arange(entries.shape[position]) // (entries.shape[position] // shards_of)).reshape([-1 if axis == position else 1 for axis in range(entries.ndim)]) for position in (source, target)]
    chosen = jax.random.permutation(rng, shards_of)[partner]
    strong = (owner == chosen) | (owner == (partner + shards_of // 2) % shards_of)
    return jnp.where(strong, factor * entries, entries)


def block_scale(own_key, shape, split, least, largest):
    level = 1.0
    for position, blocks in split:
        heights = jax.random.uniform(jax.random.fold_in(jax.random.fold_in(own_key, 6), position), (blocks,), jnp.float32, least / len(split), largest / len(split))
        level = level * jnp.repeat(jnp.exp(heights), shape[position] // blocks).reshape((-1,) + (1,) * (len(shape) - 1 - position))
    return level


def normal_values(stream_key, shape, deviation, limit, pieces=(), kind=jnp.bfloat16):
    gain = block_scale(stream_key, shape, pieces, -0.22, 0.18) if pieces else 1.0
    entries = jax.random.normal(stream_key, shape, jnp.float32) * deviation * gain
    return jnp.minimum(jnp.maximum(entries, -limit), limit).astype(kind)


def noise_with(own_key, extent, deviation, most, cuts, heavy, kind=jnp.bfloat16):
    drawn = deviation * jax.random.normal(own_key, extent, jnp.float32)
    if cuts:
        drawn = drawn * block_scale(own_key, extent, cuts, -0.22, 0.18)
    return jnp.clip(with_spikes(drawn, jax.random.fold_in(own_key, 3), *heavy), -most, most).astype(kind)


def setup_inputs(seed: int = 0) -> dict:
    keys = jax.random.split(jax.random.key(seed), 18)
    inputs = noise_with(keys[0], (SEQS, BLOCK_COUNT, BLOCK_POSITIONS, D), 1.0, 6.0, ((0, 2), (1, 4), (2, 4)), (0, 3, 2, 2.0))
    block_order = jax.vmap(lambda own: jax.random.permutation(own, BLOCK_COUNT))(jax.random.split(keys[1], SEQS)).reshape((SEQS, BLOCK_COUNT)).astype(jnp.int32)
    mixer_gain = jnp.clip(1.0 + 0.1 * jax.random.normal(keys[2], (D,), jnp.float32), 0.5, 1.5)
    query_weight = normal_values(keys[3], (D, H * 2 * HD), D ** -0.5, 0.15625, ((1, 4),))
    key_weight = normal_values(keys[4], (D, H * 2 * HD), D ** -0.5, 0.15625, ((1, 4),))
    value_weight = normal_values(keys[5], (D, H * 2 * HD), D ** -0.5, 0.15625, ((1, 4),))
    lambda_qone = normal_values(keys[6], (H, HD), 0.15, 0.6, ((0, 4),), jnp.float32)
    lambda_kone = normal_values(keys[7], (H, HD), 0.15, 0.6, ((0, 4),), jnp.float32)
    lambda_qtwo = normal_values(keys[8], (H, HD), 0.15, 0.6, ((0, 4),), jnp.float32)
    lambda_ktwo = normal_values(keys[9], (H, HD), 0.15, 0.6, ((0, 4),), jnp.float32)
    group_gain = jnp.clip(1.0 + 0.1 * jax.random.normal(keys[10], (H * 2 * HD,), jnp.float32), 0.5, 1.5)
    output_weight = normal_values(keys[11], (H * 2 * HD, D), (H * 2 * HD // 20) ** -0.5, 0.625, ((0, 4),))
    feed_gain = jnp.clip(1.0 + 0.1 * jax.random.normal(keys[12], (D,), jnp.float32), 0.5, 1.5)
    gate_weight = normal_values(keys[13], (D, FF), D ** -0.5, 0.15625, ((1, 4),))
    up_weight = normal_values(keys[14], (D, FF), D ** -0.5, 0.15625, ((1, 4),))
    down_weight = normal_values(keys[15], (FF, D), (FF // 4) ** -0.5, 0.1875, ((0, 4),))
    cotangent = noise_with(keys[16], (SEQS, BLOCK_COUNT, BLOCK_POSITIONS, D), 1.0, 6.0, ((0, 2), (1, 4), (2, 4)), (0, 3, 2, 2.0))
    return dict(inputs=inputs, block_order=block_order, mixer_gain=mixer_gain, query_weight=query_weight, key_weight=key_weight, value_weight=value_weight, lambda_qone=lambda_qone, lambda_kone=lambda_kone, lambda_qtwo=lambda_qtwo, lambda_ktwo=lambda_ktwo, group_gain=group_gain, output_weight=output_weight, feed_gain=feed_gain, gate_weight=gate_weight, up_weight=up_weight, down_weight=down_weight, cotangent=cotangent)


EPSILON = 1e-05
LAMBDA_INIT = 0.8 - 0.6 * math.exp(-0.3 * 12)
THETA = 10000.0
NEGATIVE = -1e+30
TOP_PRECISION = lax.Precision.HIGHEST

@jax.custom_vjp
def lower_forward(v):
    return lax.optimization_barrier(v.astype(jnp.bfloat16)).astype(jnp.float32)

@jax.custom_vjp
def lower_backward(v):
    return v

def low_keep(v):
    return (lower_forward(v), None)

def low_pass(kept, grad):
    return (grad,)

def back_keep(v):
    return (v, None)

def back_low(kept, grad):
    return (lower_forward(grad),)
lower_forward.defvjp(low_keep, low_pass)
lower_backward.defvjp(back_keep, back_low)

def product(left, right):
    return jnp.dot(left, right, precision=TOP_PRECISION, preferred_element_type=jnp.float32)

def rms_scale(value_rows):
    return lax.rsqrt(lax.optimization_barrier(jnp.mean(value_rows * value_rows, axis=-1, keepdims=True)) + EPSILON)

def rotate(tensor, places):
    half_dim = tensor.shape[-1] // 2
    frequency = THETA ** (-jnp.arange(half_dim, dtype=jnp.float32) / half_dim)
    angles = places.astype(jnp.float32)[..., None] * frequency
    angles = angles.reshape(places.shape + (1,) * (tensor.ndim - places.ndim - 1) + (half_dim,))
    cosine = jnp.cos(angles)
    sine_part = jnp.sin(angles)
    leading = tensor[..., :half_dim]
    trailing = tensor[..., half_dim:]
    return jnp.concatenate([leading * cosine - trailing * sine_part, leading * sine_part + trailing * cosine], axis=-1)

def one_map(query_map, key_map, value_rows, allowed):
    length = query_map.shape[0]
    scores = lower_backward(product(query_map, key_map.T) * HD ** (-0.5))
    scores = jnp.where(allowed, scores.reshape(length, BLOCK_COUNT, BLOCK_POSITIONS), NEGATIVE)
    row_peaks = lax.optimization_barrier(jnp.max(scores, axis=2))
    weight_set = jnp.exp(scores - row_peaks[:, :, None])
    block_list = lower_backward(jnp.einsum('umi,mit->umt', lower_forward(weight_set), value_rows.reshape(BLOCK_COUNT, BLOCK_POSITIONS, value_rows.shape[-1]), precision=TOP_PRECISION))
    highest = lax.optimization_barrier(jnp.max(row_peaks, axis=1, keepdims=True))
    factor = jnp.exp(row_peaks - highest)
    totals = lax.optimization_barrier(jnp.sum(factor * lax.optimization_barrier(jnp.sum(weight_set, axis=2)), axis=1, keepdims=True))
    return lax.optimization_barrier(jnp.sum(factor[:, :, None] * block_list, axis=1)) / totals

def attend(queries, keys_all, value_rows, places, lambda_head):
    length = places.shape[0]
    allowed = (places[None, :] <= places[:, None]).reshape(length, BLOCK_COUNT, BLOCK_POSITIONS)

    def per_head(head_items):
        head_query, head_key, head_value, head_lambda = head_items
        first_map = one_map(head_query[:, 0], head_key[:, 0], head_value, allowed)
        second_map = one_map(head_query[:, 1], head_key[:, 1], head_value, allowed)
        return first_map - head_lambda * second_map
    outputs = lax.map(jax.checkpoint(per_head), (jnp.transpose(queries, (1, 0, 2, 3)), jnp.transpose(keys_all, (1, 0, 2, 3)), jnp.transpose(value_rows, (1, 0, 2)), lambda_head))
    return jnp.transpose(outputs, (1, 0, 2))

def forward(inputs, mixer_gain, query_weight, key_weight, value_weight, lambda_qone, lambda_kone, lambda_qtwo, lambda_ktwo, group_gain, output_weight, feed_gain, gate_weight, up_weight, down_weight, block_order):
    length = BLOCK_COUNT * BLOCK_POSITIONS
    lambda_head = jnp.exp(lax.optimization_barrier(jnp.sum(lambda_qone * lambda_kone, axis=-1))) - jnp.exp(lax.optimization_barrier(jnp.sum(lambda_qtwo * lambda_ktwo, axis=-1))) + LAMBDA_INIT

    def per_sequence(seq_items):
        tokens, seq_order = seq_items
        places = (seq_order[:, None] * BLOCK_POSITIONS + jnp.arange(BLOCK_POSITIONS, dtype=jnp.int32)[None, :]).reshape(length)
        normed = lower_forward(tokens * rms_scale(tokens) * mixer_gain)
        queries = lower_forward(rotate(lower_backward(product(normed, query_weight)).reshape(length, H, 2, HD), places))
        keys_all = lower_forward(rotate(lower_backward(product(normed, key_weight)).reshape(length, H, 2, HD), places))
        value_rows = lower_forward(lower_backward(product(normed, value_weight))).reshape(length, H, 2 * HD)
        mixed_out = attend(queries, keys_all, value_rows, places, lambda_head)
        grouped = (mixed_out * rms_scale(mixed_out)).reshape(length, H * 2 * HD) * group_gain * (1.0 - LAMBDA_INIT)
        hidden = tokens + lower_backward(product(lower_forward(grouped), output_weight))
        normed_two = lower_forward(hidden * rms_scale(hidden) * feed_gain)
        gate_vals = lower_backward(product(normed_two, gate_weight))
        up_vals = lower_backward(product(normed_two, up_weight))
        activation = lower_forward(jax.nn.silu(gate_vals) * up_vals)
        return hidden + lower_backward(product(activation, down_weight))
    results = lax.map(jax.checkpoint(per_sequence), (inputs.reshape(SEQS, length, D), block_order))
    return results.reshape(SEQS, BLOCK_COUNT, BLOCK_POSITIONS, D)

def reference(inputs, block_order, mixer_gain, query_weight, key_weight, value_weight, lambda_qone, lambda_kone, lambda_qtwo, lambda_ktwo, group_gain, output_weight, feed_gain, gate_weight, up_weight, down_weight, cotangent):
    float_args = (inputs.astype(jnp.float32), mixer_gain.astype(jnp.float32), query_weight.astype(jnp.float32), key_weight.astype(jnp.float32), value_weight.astype(jnp.float32), lambda_qone.astype(jnp.float32), lambda_kone.astype(jnp.float32), lambda_qtwo.astype(jnp.float32), lambda_ktwo.astype(jnp.float32), group_gain.astype(jnp.float32), output_weight.astype(jnp.float32), feed_gain.astype(jnp.float32), gate_weight.astype(jnp.float32), up_weight.astype(jnp.float32), down_weight.astype(jnp.float32))

    def wrapped(*params):
        return forward(*params, block_order)
    result, pullback = jax.vjp(wrapped, *float_args)
    gradients = pullback(cotangent.astype(jnp.float32))
    return (result.astype(jnp.bfloat16), gradients[0], gradients[1], gradients[2], gradients[3], gradients[4], gradients[5], gradients[6], gradients[7], gradients[8], gradients[9], gradients[10], gradients[11], gradients[12], gradients[13], gradients[14])
```

```python
from functools import partial
import math

import jax
import jax.numpy as jnp
from jax import lax
from jax.experimental import pallas as pl
from jax.experimental.pallas import tpu as pltpu
from jax.sharding import PartitionSpec as P

EPSILON = 1e-05
LAMBDA_INIT = 0.8 - 0.6 * math.exp(-0.3 * 12)
SHRINK = 1.0 - LAMBDA_INIT
THETA = 10000.0
NEGATIVE = -1e30
F32 = jnp.float32
BF16 = jnp.bfloat16


def rms_scale(value_rows):
    return lax.rsqrt(jnp.mean(value_rows * value_rows, axis=-1, keepdims=True) + EPSILON)


def norm_back(grad_in, value_rows, scale, gain):
    upstream = grad_in * gain
    return scale * upstream - value_rows * scale**3 * jnp.mean(
        upstream * value_rows, axis=-1, keepdims=True
    )


def rotate(tensor, places, direction):
    half_dim = tensor.shape[-1] // 2
    frequency = THETA ** (-jnp.arange(half_dim, dtype=jnp.float32) / half_dim)
    angles = places.astype(jnp.float32)[..., None] * frequency
    angles = angles.reshape(places.shape + (1,) * (tensor.ndim - places.ndim - 1) + (half_dim,))
    cosine = jnp.cos(angles)
    sine_part = jnp.sin(angles) * direction
    leading = tensor[..., :half_dim]
    trailing = tensor[..., half_dim:]
    return jnp.concatenate(
        [leading * cosine - trailing * sine_part, leading * sine_part + trailing * cosine], axis=-1
    )


def contract_rows(left, right):
    return lax.dot_general(
        left, right, (((0,), (0,)), ((), ())), preferred_element_type=jnp.float32
    )


def contract_cols(left, right):
    return lax.dot_general(
        left, right, (((1,), (1,)), ((), ())), preferred_element_type=jnp.float32
    )


def dot(left, right):
    return lax.dot_general(left, right, (((1,), (0,)), ((), ())), preferred_element_type=F32)


def offsets_of(part, parts, strip, axis, shape):
    index = lax.broadcasted_iota(jnp.int32, shape, axis)
    return (index // strip) * (parts * strip) + part * strip + index % strip


def block_diag_cols(turned, half, lanes):
    row = lax.broadcasted_iota(jnp.int32, (turned.shape[0], lanes), 0)
    zero = jnp.zeros_like(turned)
    return jnp.concatenate(
        [jnp.where(row < half, turned, zero), jnp.where(row >= half, turned, zero)], axis=1
    )


def attend_kernel(dims, slot_ref, part_ref, lam_ref, q_ref, k_ref, v_ref, gain_ref,
                  grouped_ref, mixed_ref, second_ref, lse_ref, vt_ref, qbd_ref, acc_ref):
    slots, parts, heads, tile, width, strip = dims
    half = width // 2
    cols = 2 * tile

    def turn(slot, carry):
        for h in range(heads):
            for c in range(parts):
                vt_ref[h, slot, :, c * tile:(c + 1) * tile] = jnp.transpose(
                    v_ref[c, slot, :, h * width:(h + 1) * width])
        return carry

    lax.fori_loop(0, slots, turn, 0)
    query_off = offsets_of(part_ref[0], parts, strip, 1, (1, tile))
    query_off = jnp.concatenate([query_off, query_off], axis=1)

    def one_block(slot, diag, state):
        out = []
        for h in range(heads):
            peak, total = state[2 * h], state[2 * h + 1]
            scores = []
            for c in range(parts):
                s = dot(k_ref[c, slot, :, h * width:(h + 1) * width], qbd_ref[h])
                if diag:
                    key_off = offsets_of(c, parts, strip, 0, (tile, 1))
                    s = jnp.where(key_off <= query_off, s, NEGATIVE)
                scores.append(s)
            top = scores[0]
            for s in scores[1:]:
                top = jnp.maximum(top, s)
            higher = jnp.maximum(peak, jnp.max(top, axis=0, keepdims=True))
            keep = jnp.exp(peak - higher)
            weights = [jnp.exp(s - higher) for s in scores]
            added = weights[0]
            for w in weights[1:]:
                added = added + w
            total = total * keep + jnp.sum(added, axis=0, keepdims=True)
            low = jnp.concatenate([w.astype(BF16) for w in weights], axis=0)
            acc_ref[h] = acc_ref[h] * keep + dot(vt_ref[h, slot], low)
            out += [higher, total]
        return tuple(out)

    def one_place(place, carry):
        own = slot_ref[place]
        for h in range(heads):
            turned = jnp.transpose(q_ref[own, :, h * width:(h + 1) * width])
            turned = turned * jnp.asarray(half ** -0.5, turned.dtype)
            qbd_ref[h] = block_diag_cols(turned, half, tile)
            acc_ref[h] = jnp.zeros((width, cols), F32)
        state = (jnp.full((1, cols), NEGATIVE, F32), jnp.zeros((1, cols), F32)) * heads
        state = one_block(own, True, state)
        state = lax.fori_loop(
            0, place, lambda j, st: one_block(slot_ref[j], False, st), state)
        for h in range(heads):
            peak, total = state[2 * h], state[2 * h + 1]
            result = acc_ref[h] / total
            second = result[:, tile:]
            mixed = result[:, :tile] - lam_ref[h] * second
            scale = lax.rsqrt(jnp.mean(mixed * mixed, axis=0, keepdims=True) + EPSILON)
            gain = gain_ref[h * width:(h + 1) * width, :] * SHRINK
            grouped = (mixed * scale * gain).astype(BF16)
            grouped_ref[own, :, h * width:(h + 1) * width] = jnp.transpose(grouped)
            mixed_ref[own, h] = mixed
            second_ref[own, h] = second
            lse_ref[own, h] = peak + jnp.log(total)
        return carry

    lax.fori_loop(0, slots, one_place, 0)


def attend_back_kernel(dims, slot_ref, part_ref, lam_ref, q_ref, k_ref, v_ref, gg_ref, gain_ref,
                       mixed_ref, second_ref, lse_ref,
                       dq_ref, dk_ref, dv_ref, gpart_ref, lpart_ref,
                       kt_ref, qbdt_ref, qbd_ref, gt_ref, g_ref, delta_ref, dqt_ref,
                       dka_ref, dva_ref):
    slots, parts, heads, tile, width, strip = dims
    half = width // 2
    scale = half ** -0.5

    def turn(slot, carry):
        for h in range(heads):
            for c in range(parts):
                kt_ref[h, slot, :, c * tile:(c + 1) * tile] = jnp.transpose(
                    k_ref[c, slot, :, h * width:(h + 1) * width])
        return carry

    lax.fori_loop(0, slots, turn, 0)
    gpart_ref[...] = jnp.zeros_like(gpart_ref)
    lpart_ref[...] = jnp.zeros_like(lpart_ref)
    query_off = offsets_of(part_ref[0], parts, strip, 1, (1, tile))
    query_off = jnp.concatenate([query_off, query_off], axis=1)

    def one_block(own, slot, diag):
        for h in range(heads):
            lse = lse_ref[own, h]
            delta = delta_ref[h]
            lanes = slice(h * width, (h + 1) * width)
            turned = []
            for c in range(parts):
                keys = k_ref[c, slot, :, lanes]
                s = dot(keys, qbdt_ref[h])
                if diag:
                    key_off = offsets_of(c, parts, strip, 0, (tile, 1))
                    s = jnp.where(key_off <= query_off, s, NEGATIVE)
                weights = jnp.exp(s - lse)
                probs = dot(v_ref[c, slot, :, lanes], gt_ref[h])
                ds = (weights * (probs - delta)).astype(BF16)
                dv = dot(weights.astype(BF16), g_ref[h])
                dk = dot(ds, qbd_ref[h])
                if diag:
                    dva_ref[h, slot, c] = dv
                    dka_ref[h, slot, c] = dk
                else:
                    dva_ref[h, slot, c] += dv
                    dka_ref[h, slot, c] += dk
                turned.append(ds)
            dq = dot(kt_ref[h, slot], jnp.concatenate(turned, axis=0))
            dqt_ref[h, :half] += dq[:half, :tile]
            dqt_ref[h, half:] += dq[half:, tile:]

    def one_place(place, carry):
        own = slot_ref[place]
        for h in range(heads):
            lanes = slice(h * width, (h + 1) * width)
            lam = lam_ref[h]
            start = pl.multiple_of(own * tile, tile)
            grad = gg_ref[lanes, pl.ds(start, tile)]
            mixed = mixed_ref[own, h]
            second = second_ref[own, h]
            rg = lax.rsqrt(jnp.mean(mixed * mixed, axis=0, keepdims=True) + EPSILON)
            gpart_ref[lanes, :] += grad * (mixed * rg)
            up = grad * (gain_ref[lanes, :] * SHRINK)
            gm = rg * up - mixed * (rg * rg * rg * jnp.mean(up * mixed, axis=0, keepdims=True))
            lpart_ref[h] -= gm * second
            along = jnp.sum(gm * second, axis=0, keepdims=True)
            first = jnp.sum(gm * mixed, axis=0, keepdims=True) + lam * along
            delta_ref[h] = jnp.concatenate([first, -lam * along], axis=1)
            both = jnp.concatenate([gm, -lam * gm], axis=1)
            gt_ref[h] = both.astype(BF16)
            g_ref[h] = jnp.transpose(both).astype(BF16)
            query = q_ref[own, :, lanes]
            query = query * jnp.asarray(scale, query.dtype)
            qbdt_ref[h] = block_diag_cols(jnp.transpose(query), half, tile)
            lane = lax.broadcasted_iota(jnp.int32, (tile, width), 1)
            zero = jnp.zeros_like(query)
            qbd_ref[h, :tile] = jnp.where(lane < half, query, zero)
            qbd_ref[h, tile:] = jnp.where(lane >= half, query, zero)
            dqt_ref[h] = jnp.zeros((width, tile), F32)
        one_block(own, own, True)

        def rest(j, c):
            one_block(own, slot_ref[j], False)
            return c

        lax.fori_loop(0, place, rest, 0)
        for h in range(heads):
            dq_ref[own, :, h * width:(h + 1) * width] = jnp.transpose(dqt_ref[h] * scale)
        return carry

    lax.fori_loop(0, slots, one_place, 0)

    def put(slot, carry):
        for h in range(heads):
            lanes = slice(h * width, (h + 1) * width)
            for c in range(parts):
                dk_ref[c, slot, :, lanes] = dka_ref[h, slot, c].astype(BF16)
                dv_ref[c, slot, :, lanes] = dva_ref[h, slot, c].astype(BF16)
        return carry

    lax.fori_loop(0, slots, put, 0)


def specs(count, smem):
    return [pl.BlockSpec(memory_space=pltpu.SMEM)] * smem + [
        pl.BlockSpec(memory_space=pltpu.VMEM)] * (count - smem)


def attend(dims, slot_of, part, lam, queries, keys_all, values_all, gain):
    slots, parts, heads, tile, width, strip = dims
    return pl.pallas_call(
        partial(attend_kernel, dims),
        out_shape=(
            jax.ShapeDtypeStruct((slots, tile, heads * width), BF16),
            jax.ShapeDtypeStruct((slots, heads, width, tile), F32),
            jax.ShapeDtypeStruct((slots, heads, width, tile), F32),
            jax.ShapeDtypeStruct((slots, heads, 1, 2 * tile), F32),
        ),
        in_specs=specs(7, 3),
        out_specs=specs(4, 0),
        scratch_shapes=[
            pltpu.VMEM((heads, slots, width, parts * tile), BF16),
            pltpu.VMEM((heads, width, 2 * tile), BF16),
            pltpu.VMEM((heads, width, 2 * tile), F32),
        ],
        compiler_params=pltpu.CompilerParams(vmem_limit_bytes=48 << 20),
        cost_estimate=pl.CostEstimate(
            flops=20_000_000_000, bytes_accessed=12_000_000, transcendentals=14_000_000),
        name="attend",
    )(slot_of, part, lam, queries, keys_all, values_all, gain)


def attend_back(dims, slot_of, part, lam, queries, keys_all, values_all, gg, gain, mixed, second, lse):
    slots, parts, heads, tile, width, strip = dims
    full = heads * width
    return pl.pallas_call(
        partial(attend_back_kernel, dims),
        out_shape=(
            jax.ShapeDtypeStruct((slots, tile, full), F32),
            jax.ShapeDtypeStruct((parts, slots, tile, full), BF16),
            jax.ShapeDtypeStruct((parts, slots, tile, full), BF16),
            jax.ShapeDtypeStruct((full, tile), F32),
            jax.ShapeDtypeStruct((heads, width, tile), F32),
        ),
        in_specs=specs(11, 3),
        out_specs=specs(5, 0),
        scratch_shapes=[
            pltpu.VMEM((heads, slots, width, parts * tile), BF16),
            pltpu.VMEM((heads, width, 2 * tile), BF16),
            pltpu.VMEM((heads, 2 * tile, width), BF16),
            pltpu.VMEM((heads, width, 2 * tile), BF16),
            pltpu.VMEM((heads, 2 * tile, width), BF16),
            pltpu.VMEM((heads, 1, 2 * tile), F32),
            pltpu.VMEM((heads, width, tile), F32),
            pltpu.VMEM((heads, slots, parts, tile, width), F32),
            pltpu.VMEM((heads, slots, parts, tile, width), F32),
        ],
        compiler_params=pltpu.CompilerParams(vmem_limit_bytes=56 << 20),
        cost_estimate=pl.CostEstimate(
            flops=60_000_000_000, bytes_accessed=24_000_000, transcendentals=14_000_000),
        name="attend_back",
    )(slot_of, part, lam, queries, keys_all, values_all, gg, gain, mixed, second, lse)


def per_device(
    inputs,
    block_order,
    mixer_gain,
    query_weight,
    key_weight,
    value_weight,
    lambda_qone,
    lambda_kone,
    lambda_qtwo,
    lambda_ktwo,
    group_gain,
    output_weight,
    feed_gain,
    gate_weight,
    up_weight,
    down_weight,
    cotangent,
):
    seq_count, pair_count, short_rows, model_width = inputs.shape
    assert seq_count == 1
    parts = lax.axis_size("ctx")
    head_total = lax.axis_size("head")
    part = lax.axis_index("ctx")
    head_place = lax.axis_index("head")
    block_len = short_rows * head_total
    slots = block_order.shape[1]
    heads_here, head_dim = lambda_qone.shape
    qwidth = query_weight.shape[1]
    width = 2 * head_dim
    tile = block_len // parts
    strip = short_rows // parts
    dims = (slots, parts, heads_here, tile, width, strip)
    row_count = slots * tile
    order = block_order.reshape(slots)
    slot_of = jnp.argsort(order).astype(jnp.int32)
    index = jnp.arange(tile, dtype=jnp.int32)
    row_offsets = (index // strip) * short_rows + part * strip + index % strip
    own_places = order[:, None] * block_len + row_offsets[None, :]
    lambda_one = jnp.exp(jnp.sum(lambda_qone * lambda_kone, axis=-1))
    lambda_two = jnp.exp(jnp.sum(lambda_qtwo * lambda_ktwo, axis=-1))
    lambda_head = lambda_one - lambda_two + LAMBDA_INIT
    split_shape = (slots, tile, heads_here, 2, head_dim)
    rows_shape = (slots, tile, model_width)

    def spread(rows):
        cut = rows.reshape(pair_count, parts, strip, model_width).transpose(1, 0, 2, 3)
        cut = lax.all_to_all(cut, "ctx", 0, 0, tiled=True)
        return cut.reshape(slots, strip, model_width)

    def unspread(rows):
        cut = rows.reshape(parts, pair_count, strip, model_width)
        cut = lax.all_to_all(cut, "ctx", 0, 0, tiled=True)
        return cut.transpose(1, 0, 2, 3).reshape(1, pair_count, short_rows, model_width)

    inputs_here = spread(inputs)
    tokens = inputs_here.astype(jnp.float32)
    scale_one = rms_scale(tokens)
    normed = (tokens * scale_one * mixer_gain).astype(jnp.bfloat16)
    normed_rows = lax.all_gather(normed, "head", axis=1, tiled=True).reshape(row_count, model_width)
    query_lin = jnp.dot(normed_rows, query_weight, preferred_element_type=jnp.float32)
    key_lin = jnp.dot(normed_rows, key_weight, preferred_element_type=jnp.float32)
    value_lin = jnp.dot(normed_rows, value_weight, preferred_element_type=jnp.float32)
    queries = rotate(query_lin.reshape(split_shape), own_places, 1.0).astype(jnp.bfloat16)
    keys_own = rotate(key_lin.reshape(split_shape), own_places, 1.0).astype(jnp.bfloat16)
    values_own = value_lin.astype(jnp.bfloat16)
    part_shape = (slots, tile, qwidth)
    keys_all = lax.all_gather(keys_own.reshape(part_shape), "ctx", axis=0)
    values_all = lax.all_gather(values_own.reshape(part_shape), "ctx", axis=0)
    part_arr = part.reshape(1).astype(jnp.int32)
    gain_col = group_gain.reshape(qwidth, 1)
    grouped, mixed, second, lse = attend(
        dims, slot_of, part_arr, lambda_head, queries.reshape(part_shape), keys_all, values_all,
        gain_col)
    grouped = grouped.reshape(row_count, qwidth)
    attn_terms = jnp.dot(grouped, output_weight, preferred_element_type=jnp.float32).reshape(
        rows_shape
    )
    hidden = tokens + lax.psum_scatter(
        attn_terms.astype(jnp.bfloat16), "head", scatter_dimension=1, tiled=True
    ).astype(jnp.float32)
    cotangent_here = spread(cotangent)
    scale_two = rms_scale(hidden)
    normed_two = (hidden * scale_two * feed_gain).astype(jnp.bfloat16)
    feed_rows = lax.all_gather(normed_two, "head", axis=1, tiled=True).reshape(
        row_count, model_width
    )
    gate_vals = jnp.dot(feed_rows, gate_weight, preferred_element_type=jnp.float32)
    up_vals = jnp.dot(feed_rows, up_weight, preferred_element_type=jnp.float32)
    gate_sigmoid = jax.nn.sigmoid(gate_vals)
    silu_gate = gate_vals * gate_sigmoid
    activation = (silu_gate * up_vals).astype(jnp.bfloat16)
    feed_terms = jnp.dot(activation, down_weight, preferred_element_type=jnp.float32).reshape(
        rows_shape
    )
    block_out = (
        hidden
        + lax.psum_scatter(
            feed_terms.astype(jnp.bfloat16), "head", scatter_dimension=1, tiled=True
        ).astype(jnp.float32)
    ).astype(jnp.bfloat16)
    grad_rows = lax.all_gather(cotangent_here, "head", axis=1, tiled=True).reshape(
        row_count, model_width
    )
    down_term = contract_rows(grad_rows, activation)
    grad_activ = contract_cols(grad_rows, down_weight)
    grad_gate = (
        grad_activ * up_vals * gate_sigmoid * (1.0 + gate_vals * (1.0 - gate_sigmoid))
    ).astype(jnp.bfloat16)
    grad_up = (grad_activ * silu_gate).astype(jnp.bfloat16)
    gate_term = contract_rows(feed_rows, grad_gate)
    up_term = contract_rows(feed_rows, grad_up)
    normed_two_terms = (
        contract_cols(grad_gate, gate_weight) + contract_cols(grad_up, up_weight)
    ).reshape(rows_shape)
    grad_normed_two = lax.psum_scatter(
        normed_two_terms.astype(jnp.bfloat16), "head", scatter_dimension=1, tiled=True
    ).astype(jnp.float32)
    feed_part = jnp.sum(grad_normed_two * hidden * scale_two, axis=(0, 1))
    grad_hidden = cotangent_here.astype(jnp.float32) + norm_back(
        grad_normed_two, hidden, scale_two, feed_gain
    )
    branch_rows = lax.all_gather(
        grad_hidden.astype(jnp.bfloat16), "head", axis=1, tiled=True
    ).reshape(row_count, model_width)
    output_term = contract_rows(branch_rows, grouped)
    grad_grouped = contract_cols(output_weight, branch_rows)
    query_acc, key_acc, value_acc, group_part, lambda_part = attend_back(
        dims, slot_of, part_arr, lambda_head, queries.reshape(part_shape), keys_all, values_all,
        grad_grouped, gain_col, mixed, second, lse)
    group_part = jnp.sum(group_part, axis=1) * SHRINK
    lambda_part = jnp.sum(lambda_part, axis=(1, 2))
    key_sums = lax.psum_scatter(key_acc, "ctx", scatter_dimension=0).astype(jnp.float32)
    value_sums = lax.psum_scatter(value_acc, "ctx", scatter_dimension=0)
    grad_query = (
        rotate(query_acc.reshape(split_shape), own_places, -1.0)
        .astype(jnp.bfloat16)
        .reshape(row_count, qwidth)
    )
    grad_key = (
        rotate(key_sums.reshape(split_shape), own_places, -1.0)
        .astype(jnp.bfloat16)
        .reshape(row_count, qwidth)
    )
    grad_value = value_sums.reshape(row_count, qwidth)
    query_term = contract_rows(normed_rows, grad_query)
    key_term = contract_rows(normed_rows, grad_key)
    value_term = contract_rows(normed_rows, grad_value)
    normed_terms = (
        contract_cols(grad_query, query_weight)
        + contract_cols(grad_key, key_weight)
        + contract_cols(grad_value, value_weight)
    ).reshape(rows_shape)
    grad_normed = lax.psum_scatter(
        normed_terms.astype(jnp.bfloat16), "head", scatter_dimension=1, tiled=True
    ).astype(jnp.float32)
    mixer_part = jnp.sum(grad_normed * tokens * scale_one, axis=(0, 1))
    input_grad = grad_hidden + norm_back(grad_normed, tokens, scale_one, mixer_gain)
    block_out = unspread(block_out)
    input_grad = unspread(input_grad.astype(BF16)).astype(F32)
    group_full = lax.dynamic_update_slice(
        jnp.zeros((qwidth * head_total,), jnp.float32), group_part, (head_place * qwidth,)
    )
    lambda_full = lax.dynamic_update_slice(
        jnp.zeros((heads_here * head_total,), jnp.float32), lambda_part, (head_place * heads_here,)
    )
    mixer_sum, feed_sum, group_sum, lambda_sum = lax.psum(
        (mixer_part, feed_part, group_full, lambda_full), ("dp", "ctx", "head")
    )
    group_grad = lax.dynamic_slice(group_sum, (head_place * qwidth,), (qwidth,))
    lambda_grad = lax.dynamic_slice(lambda_sum, (head_place * heads_here,), (heads_here,))
    qone_grad = (lambda_grad * lambda_one)[:, None] * lambda_kone
    kone_grad = (lambda_grad * lambda_one)[:, None] * lambda_qone
    qtwo_grad = -(lambda_grad * lambda_two)[:, None] * lambda_ktwo
    ktwo_grad = -(lambda_grad * lambda_two)[:, None] * lambda_qtwo

    def over_all(term):
        return lax.psum_scatter(
            term.astype(jnp.bfloat16), ("dp", "ctx"), scatter_dimension=0, tiled=True
        ).astype(jnp.float32)

    return (
        block_out,
        input_grad,
        mixer_sum,
        over_all(query_term),
        over_all(key_term),
        over_all(value_term),
        qone_grad,
        kone_grad,
        qtwo_grad,
        ktwo_grad,
        group_grad,
        over_all(output_term).T,
        feed_sum,
        over_all(gate_term),
        over_all(up_term),
        over_all(down_term).T,
    )


def solution(mesh):
    return jax.shard_map(
        per_device,
        mesh=mesh,
        in_specs=(
            P("dp", "ctx", "head", None),
            P("dp", None),
            P(),
            P(None, "head"),
            P(None, "head"),
            P(None, "head"),
            P("head", None),
            P("head", None),
            P("head", None),
            P("head", None),
            P("head"),
            P("head", None),
            P(),
            P(None, "head"),
            P(None, "head"),
            P("head", None),
            P("dp", "ctx", "head", None),
        ),
        out_specs=(
            P("dp", "ctx", "head", None),
            P("dp", "ctx", "head", None),
            P(),
            P(("dp", "ctx"), "head"),
            P(("dp", "ctx"), "head"),
            P(("dp", "ctx"), "head"),
            P("head", None),
            P("head", None),
            P("head", None),
            P("head", None),
            P("head"),
            P("head", ("dp", "ctx")),
            P(),
            P(("dp", "ctx"), "head"),
            P(("dp", "ctx"), "head"),
            P("head", ("dp", "ctx")),
        ),
        check_vma=False,
    )
```

```python
from functools import partial
import math

import jax
import jax.numpy as jnp
from jax import lax
from jax.experimental import pallas as pl
from jax.experimental.pallas import tpu as pltpu
from jax.sharding import PartitionSpec as P

EPSILON = 1e-05
LAMBDA_INIT = 0.8 - 0.6 * math.exp(-0.3 * 12)
SHRINK = 1.0 - LAMBDA_INIT
THETA = 10000.0
NEGATIVE = -1e30
F32 = jnp.float32
BF16 = jnp.bfloat16


def rms_scale(value_rows):
    return lax.rsqrt(jnp.mean(value_rows * value_rows, axis=-1, keepdims=True) + EPSILON)


def norm_back(grad_in, value_rows, scale, gain):
    upstream = grad_in * gain
    return scale * upstream - value_rows * scale**3 * jnp.mean(
        upstream * value_rows, axis=-1, keepdims=True
    )


def rotate(tensor, places, direction):
    half_dim = tensor.shape[-1] // 2
    frequency = THETA ** (-jnp.arange(half_dim, dtype=jnp.float32) / half_dim)
    angles = places.astype(jnp.float32)[..., None] * frequency
    angles = angles.reshape(places.shape + (1,) * (tensor.ndim - places.ndim - 1) + (half_dim,))
    cosine = jnp.cos(angles)
    sine_part = jnp.sin(angles) * direction
    leading = tensor[..., :half_dim]
    trailing = tensor[..., half_dim:]
    return jnp.concatenate(
        [leading * cosine - trailing * sine_part, leading * sine_part + trailing * cosine], axis=-1
    )


def contract_rows(left, right):
    return lax.dot_general(
        left, right, (((0,), (0,)), ((), ())), preferred_element_type=jnp.float32
    )


def contract_cols(left, right):
    return lax.dot_general(
        left, right, (((1,), (1,)), ((), ())), preferred_element_type=jnp.float32
    )


def dot(left, right):
    return lax.dot_general(left, right, (((1,), (0,)), ((), ())), preferred_element_type=F32)


def offsets_of(part, parts, strip, axis, shape):
    index = lax.broadcasted_iota(jnp.int32, shape, axis)
    return (index // strip) * (parts * strip) + part * strip + index % strip


def block_diag_cols(turned, half, lanes):
    row = lax.broadcasted_iota(jnp.int32, (turned.shape[0], lanes), 0)
    zero = jnp.zeros_like(turned)
    return jnp.concatenate(
        [jnp.where(row < half, turned, zero), jnp.where(row >= half, turned, zero)], axis=1
    )


def attend_kernel(dims, part_ref, lam_ref, q_ref, k_ref, v_ref, gain_ref,
                  grouped_ref, mixed_ref, second_ref, lse_ref, vt_ref, qbd_ref, acc_ref):
    slots, parts, heads, tile, width, strip = dims
    half = width // 2
    cols = 2 * tile

    def turn(slot, carry):
        for h in range(heads):
            for c in range(parts):
                vt_ref[h, slot, :, c * tile:(c + 1) * tile] = jnp.transpose(
                    v_ref[c, slot, :, h * width:(h + 1) * width])
        return carry

    lax.fori_loop(0, slots, turn, 0)
    query_off = offsets_of(part_ref[0], parts, strip, 1, (1, tile))
    query_off = jnp.concatenate([query_off, query_off], axis=1)

    def one_block(slot, diag, state):
        out = []
        for h in range(heads):
            peak, total = state[2 * h], state[2 * h + 1]
            scores = []
            for c in range(parts):
                s = dot(k_ref[c, slot, :, h * width:(h + 1) * width], qbd_ref[h])
                if diag:
                    key_off = offsets_of(c, parts, strip, 0, (tile, 1))
                    s = jnp.where(key_off <= query_off, s, NEGATIVE)
                scores.append(s)
            top = scores[0]
            for s in scores[1:]:
                top = jnp.maximum(top, s)
            higher = jnp.maximum(peak, jnp.max(top, axis=0, keepdims=True))
            keep = jnp.exp(peak - higher)
            weights = [jnp.exp(s - higher) for s in scores]
            added = weights[0]
            for w in weights[1:]:
                added = added + w
            total = total * keep + jnp.sum(added, axis=0, keepdims=True)
            low = jnp.concatenate([w.astype(BF16) for w in weights], axis=0)
            acc_ref[h] = acc_ref[h] * keep + dot(vt_ref[h, slot], low)
            out += [higher, total]
        return tuple(out)

    def one_place(place, carry):
        for h in range(heads):
            turned = jnp.transpose(q_ref[place, :, h * width:(h + 1) * width])
            turned = turned * jnp.asarray(half ** -0.5, turned.dtype)
            qbd_ref[h] = block_diag_cols(turned, half, tile)
            acc_ref[h] = jnp.zeros((width, cols), F32)
        state = (jnp.full((1, cols), NEGATIVE, F32), jnp.zeros((1, cols), F32)) * heads
        state = one_block(place, True, state)
        state = lax.fori_loop(
            0, place, lambda j, st: one_block(j, False, st), state)
        for h in range(heads):
            peak, total = state[2 * h], state[2 * h + 1]
            result = acc_ref[h] / total
            second = result[:, tile:]
            mixed = result[:, :tile] - lam_ref[h] * second
            scale = lax.rsqrt(jnp.mean(mixed * mixed, axis=0, keepdims=True) + EPSILON)
            gain = gain_ref[h * width:(h + 1) * width, :] * SHRINK
            grouped = (mixed * scale * gain).astype(BF16)
            grouped_ref[place, :, h * width:(h + 1) * width] = jnp.transpose(grouped)
            mixed_ref[place, h] = mixed
            second_ref[place, h] = second
            lse_ref[place, h] = peak + jnp.log(total)
        return carry

    lax.fori_loop(0, slots, one_place, 0)


def mesh_copy(src, dst, send_sem, recv_sem, device):
    return pltpu.make_async_remote_copy(
        src_ref=src, dst_ref=dst, send_sem=send_sem, recv_sem=recv_sem,
        device_id=device, device_id_type=pl.DeviceIdType.MESH)


def greet(devices):
    barrier = pltpu.get_barrier_semaphore()
    for device in devices:
        pl.semaphore_signal(
            barrier, inc=1, device_id=device, device_id_type=pl.DeviceIdType.MESH)
    pl.semaphore_wait(barrier, len(devices))


def swap_halves(rows, half):
    quarter = half // 2
    lane = lax.broadcasted_iota(jnp.int32, rows.shape, 1)
    back = pltpu.roll(rows, rows.shape[1] - quarter, 1)
    ahead = pltpu.roll(rows, quarter, 1)
    return jnp.where(lane % half < quarter, back, ahead)


def attend_back_kernel(dims, groups, lam_ref, q_ref, k_ref, v_ref, gg_ref, gain_ref,
                       mixed_ref, second_ref, lse_ref, cost_ref, sint_ref, cosn_ref, sinn_ref,
                       wg_ref,
                       gq_ref, gk_ref, gv_ref, gpart_ref, lpart_ref, wsum_ref,
                       kt_ref, qbdt_ref, qbd_ref, gt_ref, g_ref, delta_ref, dqt_ref,
                       dka_ref, dva_ref, sb_ref, r1_ref, s2_ref, r2_ref,
                       wown_ref, wr1_ref, wr2_ref,
                       s1_sem, r1_sem, s2_sem, r2_sem, w1_sem, w2s_sem, w2r_sem):
    slots, parts, heads, tile, width, strip = dims
    half = width // 2
    scale = half ** -0.5
    part = lax.axis_index("ctx")
    row = lax.axis_index("dp")
    core = part % 2
    y = part // 2
    other_core = 1 - core
    other_y = 1 - y
    me = row * 2 + y
    sibling = {"ctx": y * 2 + other_core}
    across = {"ctx": other_y * 2 + core}

    def group_device(index):
        return {"dp": index // 2, "ctx": (index % 2) * 2 + core}

    others = [lax.rem(me + step, groups) for step in range(1, groups)]
    greet([sibling] + [group_device(index) for index in others])

    weights_out = mesh_copy(
        wg_ref.at[:, :, other_core], wr1_ref, w1_sem.at[0], w1_sem.at[1], sibling)
    weights_out.start()
    weights_own = pltpu.make_async_copy(wg_ref.at[:, :, core], wown_ref, w1_sem.at[2])
    weights_own.start()

    def weights_send(step):
        index = others[step]
        return mesh_copy(wown_ref.at[:, index], wr2_ref.at[step], w2s_sem.at[step],
                         w2r_sem.at[step], group_device(index))

    def weights_cross():
        weights_out.wait()
        weights_own.wait()

        def add(index, carry):
            for t in range(wown_ref.shape[0]):
                wown_ref[t, index] = (
                    wown_ref[t, index].astype(F32) + wr1_ref[t, index].astype(F32)).astype(BF16)
            return carry

        lax.fori_loop(0, groups, add, 0)
        for step in range(groups - 1):
            weights_send(step).start()

    def weights_finish():
        for step in range(groups - 1):
            weights_send(step).wait()
        for t in range(wown_ref.shape[0]):
            total = wown_ref[t, me].astype(F32)
            for step in range(groups - 1):
                total = total + wr2_ref[step, t].astype(F32)
            wsum_ref[t] = total

    def first_copy(j):
        return mesh_copy(sb_ref.at[j, other_core], r1_ref.at[j], s1_sem.at[j], r1_sem.at[j],
                         sibling)

    def second_copy(j):
        return mesh_copy(s2_ref.at[j], r2_ref.at[j], s2_sem.at[j], r2_sem.at[j], across)

    def pass_on(j):
        first_copy(j).wait()
        s2_ref[j] = (
            sb_ref[j, core, other_y].astype(F32) + r1_ref[j, other_y].astype(F32)).astype(BF16)

    def finish(j):
        second_copy(j).wait()
        total = (sb_ref[j, core, y].astype(F32) + r1_ref[j, y].astype(F32)
                 + r2_ref[j].astype(F32))
        gv_ref[j] = total[1].astype(BF16)
        for h in range(heads):
            lanes = slice(h * width, (h + 1) * width)
            grad = total[0, :, lanes]
            gk_ref[j, :, lanes] = (
                grad * cosn_ref[j] + swap_halves(grad, half) * sinn_ref[j]).astype(BF16)

    gpart_ref[...] = jnp.zeros_like(gpart_ref)
    lpart_ref[...] = jnp.zeros_like(lpart_ref)
    query_off = offsets_of(part, parts, strip, 1, (1, tile))
    query_off = jnp.concatenate([query_off, query_off], axis=1)

    def prepare(place, carry):
        for h in range(heads):
            lanes = slice(h * width, (h + 1) * width)
            lam = lam_ref[h]
            grad = gg_ref[lanes, pl.ds(pl.multiple_of(place * tile, tile), tile)]
            mixed = mixed_ref[place, h]
            second = second_ref[place, h]
            rg = lax.rsqrt(jnp.mean(mixed * mixed, axis=0, keepdims=True) + EPSILON)
            gpart_ref[lanes, :] += grad * (mixed * rg)
            up = grad * (gain_ref[lanes, :] * SHRINK)
            gm = rg * up - mixed * (rg * rg * rg * jnp.mean(up * mixed, axis=0, keepdims=True))
            lpart_ref[h] -= gm * second
            along = jnp.sum(gm * second, axis=0, keepdims=True)
            first = jnp.sum(gm * mixed, axis=0, keepdims=True) + lam * along
            delta_ref[place, h] = jnp.concatenate([first, -lam * along], axis=1)
            both = jnp.concatenate([gm, -lam * gm], axis=1)
            gt_ref[place, h] = both.astype(BF16)
            g_ref[place, h] = jnp.transpose(both).astype(BF16)
            query = q_ref[place, :, lanes]
            query = query * jnp.asarray(scale, query.dtype)
            qbdt_ref[place, h] = block_diag_cols(jnp.transpose(query), half, tile)
            lane = lax.broadcasted_iota(jnp.int32, (tile, width), 1)
            zero = jnp.zeros_like(query)
            qbd_ref[place, h, :tile] = jnp.where(lane < half, query, zero)
            qbd_ref[place, h, tile:] = jnp.where(lane >= half, query, zero)
            dqt_ref[place, h] = jnp.zeros((width, tile), F32)
        return carry

    lax.fori_loop(0, slots, prepare, 0)

    def one_block(place, slot, diag):
        for h in range(heads):
            lse = lse_ref[place, h]
            delta = delta_ref[place, h]
            lanes = slice(h * width, (h + 1) * width)
            turned = []
            for c in range(parts):
                keys = k_ref[c, slot, :, lanes]
                s = dot(keys, qbdt_ref[place, h])
                if diag:
                    key_off = offsets_of(c, parts, strip, 0, (tile, 1))
                    s = jnp.where(key_off <= query_off, s, NEGATIVE)
                weights = jnp.exp(s - lse)
                probs = dot(v_ref[c, slot, :, lanes], gt_ref[place, h])
                ds = (weights * (probs - delta)).astype(BF16)
                dv = dot(weights.astype(BF16), g_ref[place, h])
                dk = dot(ds, qbd_ref[place, h])
                if diag:
                    dva_ref[h, c] = dv
                    dka_ref[h, c] = dk
                else:
                    dva_ref[h, c] += dv
                    dka_ref[h, c] += dk
                turned.append(ds)
            dq = dot(kt_ref[h], jnp.concatenate(turned, axis=0))
            dqt_ref[place, h, :half] += dq[:half, :tile]
            dqt_ref[place, h, half:] += dq[half:, tile:]

    def one_key_block(j, carry):
        slot = j
        for h in range(heads):
            for c in range(parts):
                kt_ref[h, :, c * tile:(c + 1) * tile] = jnp.transpose(
                    k_ref[c, slot, :, h * width:(h + 1) * width])
        one_block(j, slot, True)

        def rest(place, inner):
            one_block(place, slot, False)
            return inner

        lax.fori_loop(j + 1, slots, rest, 0)
        for h in range(heads):
            lanes = slice(h * width, (h + 1) * width)
            for c in range(parts):
                sb_ref[j, c % 2, c // 2, 0, :, lanes] = dka_ref[h, c].astype(BF16)
                sb_ref[j, c % 2, c // 2, 1, :, lanes] = dva_ref[h, c].astype(BF16)

        @pl.when(j >= 1)
        def _():
            pass_on(j - 1)

        @pl.when(j == 0)
        def _():
            weights_cross()

        @pl.when(j >= 2)
        def _():
            finish(j - 2)

        first_copy(j).start()

        @pl.when(j >= 1)
        def _():
            second_copy(j - 1).start()

        return carry

    lax.fori_loop(0, slots, one_key_block, 0)

    pass_on(slots - 1)

    def put(place, carry):
        quarter = half // 2
        for h in range(heads):
            pieces = []
            for m in range(2):
                lead = dqt_ref[place, h, m * half:m * half + quarter]
                trail = dqt_ref[place, h, m * half + quarter:(m + 1) * half]
                pieces.append(lead * cost_ref[place] + trail * sint_ref[place])
                pieces.append(trail * cost_ref[place] - lead * sint_ref[place])
            turned = jnp.concatenate(pieces, axis=0) * scale
            gq_ref[place, :, h * width:(h + 1) * width] = jnp.transpose(turned).astype(BF16)
        return carry

    lax.fori_loop(0, 1, put, 0)
    second_copy(slots - 1).start()
    lax.fori_loop(1, slots, put, 0)
    finish(slots - 2)
    weights_finish()
    finish(slots - 1)


def specs(count, smem):
    return [pl.BlockSpec(memory_space=pltpu.SMEM)] * smem + [
        pl.BlockSpec(memory_space=pltpu.VMEM)] * (count - smem)


def attend(dims, part, lam, queries, keys_all, values_all, gain):
    slots, parts, heads, tile, width, strip = dims
    return pl.pallas_call(
        partial(attend_kernel, dims),
        out_shape=(
            jax.ShapeDtypeStruct((slots, tile, heads * width), BF16),
            jax.ShapeDtypeStruct((slots, heads, width, tile), F32),
            jax.ShapeDtypeStruct((slots, heads, width, tile), F32),
            jax.ShapeDtypeStruct((slots, heads, 1, 2 * tile), F32),
        ),
        in_specs=specs(6, 2),
        out_specs=specs(4, 0),
        scratch_shapes=[
            pltpu.VMEM((heads, slots, width, parts * tile), BF16),
            pltpu.VMEM((heads, width, 2 * tile), BF16),
            pltpu.VMEM((heads, width, 2 * tile), F32),
        ],
        compiler_params=pltpu.CompilerParams(vmem_limit_bytes=48 << 20),
        cost_estimate=pl.CostEstimate(
            flops=20_000_000_000, bytes_accessed=12_000_000, transcendentals=14_000_000),
        name="attend",
    )(part, lam, queries, keys_all, values_all, gain)


def attend_back(dims, groups, lam, queries, keys_all, values_all, gg, gain, mixed, second,
                lse, tables, wgrads):
    slots, parts, heads, tile, width, strip = dims
    assert parts == 4
    full = heads * width
    kinds, rows, cols = wgrads.shape[0], wgrads.shape[-2], wgrads.shape[-1]
    rows_low = jax.ShapeDtypeStruct((slots, tile, full), BF16)
    return pl.pallas_call(
        partial(attend_back_kernel, dims, groups),
        out_shape=(
            rows_low,
            rows_low,
            rows_low,
            jax.ShapeDtypeStruct((full, tile), F32),
            jax.ShapeDtypeStruct((heads, width, tile), F32),
            jax.ShapeDtypeStruct((kinds, rows, cols), F32),
        ),
        in_specs=specs(13, 1) + [pl.BlockSpec(memory_space=pl.ANY)],
        out_specs=specs(6, 0),
        scratch_shapes=[
            pltpu.VMEM((heads, width, parts * tile), BF16),
            pltpu.VMEM((slots, heads, width, 2 * tile), BF16),
            pltpu.VMEM((slots, heads, 2 * tile, width), BF16),
            pltpu.VMEM((slots, heads, width, 2 * tile), BF16),
            pltpu.VMEM((slots, heads, 2 * tile, width), BF16),
            pltpu.VMEM((slots, heads, 1, 2 * tile), F32),
            pltpu.VMEM((slots, heads, width, tile), F32),
            pltpu.VMEM((heads, parts, tile, width), F32),
            pltpu.VMEM((heads, parts, tile, width), F32),
            pltpu.VMEM((slots, 2, 2, 2, tile, full), BF16),
            pltpu.VMEM((slots, 2, 2, tile, full), BF16),
            pltpu.VMEM((slots, 2, tile, full), BF16),
            pltpu.VMEM((slots, 2, tile, full), BF16),
            pltpu.VMEM((kinds, groups, rows, cols), BF16),
            pltpu.VMEM((kinds, groups, rows, cols), BF16),
            pltpu.VMEM((groups - 1, kinds, rows, cols), BF16),
            pltpu.SemaphoreType.DMA((slots,)),
            pltpu.SemaphoreType.DMA((slots,)),
            pltpu.SemaphoreType.DMA((slots,)),
            pltpu.SemaphoreType.DMA((slots,)),
            pltpu.SemaphoreType.DMA((3,)),
            pltpu.SemaphoreType.DMA((groups - 1,)),
            pltpu.SemaphoreType.DMA((groups - 1,)),
        ],
        compiler_params=pltpu.CompilerParams(
            vmem_limit_bytes=60 << 20, collective_id=1, has_side_effects=True),
        cost_estimate=pl.CostEstimate(
            flops=60_000_000_000, bytes_accessed=24_000_000, transcendentals=14_000_000),
        name="attend_back",
    )(lam, queries, keys_all, values_all, gg, gain, mixed, second, lse, *tables, wgrads)


def per_device(
    inputs,
    block_order,
    mixer_gain,
    query_weight,
    key_weight,
    value_weight,
    lambda_qone,
    lambda_kone,
    lambda_qtwo,
    lambda_ktwo,
    group_gain,
    output_weight,
    feed_gain,
    gate_weight,
    up_weight,
    down_weight,
    cotangent,
):
    seq_count, pair_count, short_rows, model_width = inputs.shape
    assert seq_count == 1
    parts = lax.axis_size("ctx")
    head_total = lax.axis_size("head")
    part = lax.axis_index("ctx")
    head_place = lax.axis_index("head")
    block_len = short_rows * head_total
    slots = block_order.shape[1]
    heads_here, head_dim = lambda_qone.shape
    qwidth = query_weight.shape[1]
    width = 2 * head_dim
    tile = block_len // parts
    strip = short_rows // parts
    dims = (slots, parts, heads_here, tile, width, strip)
    row_count = slots * tile
    order = block_order.reshape(slots)
    slot_of = jnp.argsort(order).astype(jnp.int32)
    index = jnp.arange(tile, dtype=jnp.int32)
    row_offsets = (index // strip) * short_rows + part * strip + index % strip
    own_places = jnp.arange(slots, dtype=jnp.int32)[:, None] * block_len + row_offsets[None, :]
    groups = lax.axis_size("dp") * parts // 2
    quarter = head_dim // 2
    frequency = THETA ** (-jnp.arange(quarter, dtype=jnp.float32) / quarter)
    angles = own_places.astype(F32)[:, None, :] * frequency[None, :, None]
    cos_turned, sin_turned = jnp.cos(angles), jnp.sin(angles)
    cos_rows = jnp.tile(cos_turned.transpose(0, 2, 1), (1, 1, 4))
    sin_rows = jnp.tile(sin_turned.transpose(0, 2, 1), (1, 1, 4))
    lane = jnp.arange(width)
    sin_rows = jnp.where(lane % head_dim < quarter, sin_rows, -sin_rows)
    tables = (cos_turned, sin_turned, cos_rows, sin_rows)
    lambda_one = jnp.exp(jnp.sum(lambda_qone * lambda_kone, axis=-1))
    lambda_two = jnp.exp(jnp.sum(lambda_qtwo * lambda_ktwo, axis=-1))
    lambda_head = lambda_one - lambda_two + LAMBDA_INIT
    split_shape = (slots, tile, heads_here, 2, head_dim)
    rows_shape = (slots, tile, model_width)

    def spread(rows):
        cut = rows.reshape(pair_count, parts, strip, model_width).transpose(1, 0, 2, 3)
        cut = lax.all_to_all(cut, "ctx", 0, 0, tiled=True)
        return jnp.take(cut.reshape(slots, strip, model_width), slot_of, axis=0)

    def unspread(rows):
        cut = jnp.take(rows, order, axis=0).reshape(parts, pair_count, strip, model_width)
        cut = lax.all_to_all(cut, "ctx", 0, 0, tiled=True)
        return cut.transpose(1, 0, 2, 3).reshape(1, pair_count, short_rows, model_width)

    inputs_here = spread(inputs)
    tokens = inputs_here.astype(jnp.float32)
    scale_one = rms_scale(tokens)
    normed = (tokens * scale_one * mixer_gain).astype(jnp.bfloat16)
    normed_rows = lax.all_gather(normed, "head", axis=1, tiled=True).reshape(row_count, model_width)
    query_lin = jnp.dot(normed_rows, query_weight, preferred_element_type=jnp.float32)
    key_lin = jnp.dot(normed_rows, key_weight, preferred_element_type=jnp.float32)
    value_lin = jnp.dot(normed_rows, value_weight, preferred_element_type=jnp.float32)
    queries = rotate(query_lin.reshape(split_shape), own_places, 1.0).astype(jnp.bfloat16)
    keys_own = rotate(key_lin.reshape(split_shape), own_places, 1.0).astype(jnp.bfloat16)
    values_own = value_lin.astype(jnp.bfloat16)
    part_shape = (slots, tile, qwidth)
    keys_all = lax.all_gather(keys_own.reshape(part_shape), "ctx", axis=0)
    values_all = lax.all_gather(values_own.reshape(part_shape), "ctx", axis=0)
    part_arr = part.reshape(1).astype(jnp.int32)
    gain_col = group_gain.reshape(qwidth, 1)
    grouped, mixed, second, lse = attend(
        dims, part_arr, lambda_head, queries.reshape(part_shape), keys_all, values_all,
        gain_col)
    grouped = grouped.reshape(row_count, qwidth)
    attn_terms = jnp.dot(grouped, output_weight, preferred_element_type=jnp.float32).reshape(
        rows_shape
    )
    hidden = tokens + lax.psum_scatter(
        attn_terms.astype(jnp.bfloat16), "head", scatter_dimension=1, tiled=True
    ).astype(jnp.float32)
    cotangent_here = spread(cotangent)
    scale_two = rms_scale(hidden)
    normed_two = (hidden * scale_two * feed_gain).astype(jnp.bfloat16)
    feed_rows = lax.all_gather(normed_two, "head", axis=1, tiled=True).reshape(
        row_count, model_width
    )
    gate_vals = jnp.dot(feed_rows, gate_weight, preferred_element_type=jnp.float32)
    up_vals = jnp.dot(feed_rows, up_weight, preferred_element_type=jnp.float32)
    gate_sigmoid = jax.nn.sigmoid(gate_vals)
    silu_gate = gate_vals * gate_sigmoid
    activation = (silu_gate * up_vals).astype(jnp.bfloat16)
    feed_terms = jnp.dot(activation, down_weight, preferred_element_type=jnp.float32).reshape(
        rows_shape
    )
    block_out = (
        hidden
        + lax.psum_scatter(
            feed_terms.astype(jnp.bfloat16), "head", scatter_dimension=1, tiled=True
        ).astype(jnp.float32)
    ).astype(jnp.bfloat16)
    grad_rows = lax.all_gather(cotangent_here, "head", axis=1, tiled=True).reshape(
        row_count, model_width
    )
    down_term = contract_rows(grad_rows, activation)
    grad_activ = contract_cols(grad_rows, down_weight)
    grad_gate = (
        grad_activ * up_vals * gate_sigmoid * (1.0 + gate_vals * (1.0 - gate_sigmoid))
    ).astype(jnp.bfloat16)
    grad_up = (grad_activ * silu_gate).astype(jnp.bfloat16)
    gate_term = contract_rows(feed_rows, grad_gate)
    up_term = contract_rows(feed_rows, grad_up)
    normed_two_terms = (
        contract_cols(grad_gate, gate_weight) + contract_cols(grad_up, up_weight)
    ).reshape(rows_shape)
    grad_normed_two = lax.psum_scatter(
        normed_two_terms.astype(jnp.bfloat16), "head", scatter_dimension=1, tiled=True
    ).astype(jnp.float32)
    feed_part = jnp.sum(grad_normed_two * hidden * scale_two, axis=(0, 1))
    grad_hidden = cotangent_here.astype(jnp.float32) + norm_back(
        grad_normed_two, hidden, scale_two, feed_gain
    )
    branch_rows = lax.all_gather(
        grad_hidden.astype(jnp.bfloat16), "head", axis=1, tiled=True
    ).reshape(row_count, model_width)
    output_term = contract_rows(branch_rows, grouped)
    grad_grouped = contract_cols(output_weight, branch_rows)
    shares = lax.axis_size("dp") * parts
    wgrads = jnp.stack([gate_term.astype(BF16), up_term.astype(BF16), down_term.astype(BF16)])
    wgrads = wgrads.reshape(3, groups, 2, model_width // shares, wgrads.shape[-1])
    grad_query, grad_key, grad_value, group_part, lambda_part, feed_sums = attend_back(
        dims, groups, lambda_head, queries.reshape(part_shape), keys_all, values_all,
        grad_grouped, gain_col, mixed, second, lse, tables, wgrads)
    group_part = jnp.sum(group_part, axis=1) * SHRINK
    lambda_part = jnp.sum(lambda_part, axis=(1, 2))
    grad_query, grad_key, grad_value = (
        grad.reshape(row_count, qwidth)
        for grad in (grad_query, grad_key, grad_value))
    query_term = contract_rows(normed_rows, grad_query)
    key_term = contract_rows(normed_rows, grad_key)
    value_term = contract_rows(normed_rows, grad_value)
    normed_terms = (
        contract_cols(grad_query, query_weight)
        + contract_cols(grad_key, key_weight)
        + contract_cols(grad_value, value_weight)
    ).reshape(rows_shape)
    grad_normed = lax.psum_scatter(
        normed_terms.astype(jnp.bfloat16), "head", scatter_dimension=1, tiled=True
    ).astype(jnp.float32)
    mixer_part = jnp.sum(grad_normed * tokens * scale_one, axis=(0, 1))
    input_grad = grad_hidden + norm_back(grad_normed, tokens, scale_one, mixer_gain)
    block_out = unspread(block_out)
    input_grad = unspread(input_grad.astype(BF16)).astype(F32)
    group_full = lax.dynamic_update_slice(
        jnp.zeros((qwidth * head_total,), jnp.float32), group_part, (head_place * qwidth,)
    )
    lambda_full = lax.dynamic_update_slice(
        jnp.zeros((heads_here * head_total,), jnp.float32), lambda_part, (head_place * heads_here,)
    )
    mixer_sum, feed_sum, group_sum, lambda_sum = lax.psum(
        (mixer_part, feed_part, group_full, lambda_full), ("dp", "ctx", "head")
    )
    group_grad = lax.dynamic_slice(group_sum, (head_place * qwidth,), (qwidth,))
    lambda_grad = lax.dynamic_slice(lambda_sum, (head_place * heads_here,), (heads_here,))
    qone_grad = (lambda_grad * lambda_one)[:, None] * lambda_kone
    kone_grad = (lambda_grad * lambda_one)[:, None] * lambda_qone
    qtwo_grad = -(lambda_grad * lambda_two)[:, None] * lambda_ktwo
    ktwo_grad = -(lambda_grad * lambda_two)[:, None] * lambda_qtwo

    def over_all(term):
        return lax.psum_scatter(
            term.astype(jnp.bfloat16), ("dp", "ctx"), scatter_dimension=0, tiled=True
        ).astype(jnp.float32)

    return (
        block_out,
        input_grad,
        mixer_sum,
        over_all(query_term),
        over_all(key_term),
        over_all(value_term),
        qone_grad,
        kone_grad,
        qtwo_grad,
        ktwo_grad,
        group_grad,
        over_all(output_term).T,
        feed_sum,
        feed_sums[0],
        feed_sums[1],
        feed_sums[2].T,
    )


def solution(mesh):
    return jax.shard_map(
        per_device,
        mesh=mesh,
        in_specs=(
            P("dp", "ctx", "head", None),
            P("dp", None),
            P(),
            P(None, "head"),
            P(None, "head"),
            P(None, "head"),
            P("head", None),
            P("head", None),
            P("head", None),
            P("head", None),
            P("head"),
            P("head", None),
            P(),
            P(None, "head"),
            P(None, "head"),
            P("head", None),
            P("dp", "ctx", "head", None),
        ),
        out_specs=(
            P("dp", "ctx", "head", None),
            P("dp", "ctx", "head", None),
            P(),
            P(("dp", "ctx"), "head"),
            P(("dp", "ctx"), "head"),
            P(("dp", "ctx"), "head"),
            P("head", None),
            P("head", None),
            P("head", None),
            P("head", None),
            P("head"),
            P("head", ("dp", "ctx")),
            P(),
            P(("dp", "ctx"), "head"),
            P(("dp", "ctx"), "head"),
            P("head", ("dp", "ctx")),
        ),
        check_vma=False,
    )
```

```python
from functools import partial
import math

import jax
import jax.numpy as jnp
from jax import lax
from jax.experimental import pallas as pl
from jax.experimental.pallas import tpu as pltpu
from jax.sharding import PartitionSpec as P

EPSILON = 1e-05
LAMBDA_INIT = 0.8 - 0.6 * math.exp(-0.3 * 12)
SHRINK = 1.0 - LAMBDA_INIT
THETA = 10000.0
NEGATIVE = -1e30
F32 = jnp.float32
BF16 = jnp.bfloat16


def rms_scale(value_rows):
    return lax.rsqrt(jnp.mean(value_rows * value_rows, axis=-1, keepdims=True) + EPSILON)


def norm_back(grad_in, value_rows, scale, gain):
    upstream = grad_in * gain
    return scale * upstream - value_rows * scale**3 * jnp.mean(
        upstream * value_rows, axis=-1, keepdims=True
    )


def rotate(tensor, places, direction):
    half_dim = tensor.shape[-1] // 2
    frequency = THETA ** (-jnp.arange(half_dim, dtype=jnp.float32) / half_dim)
    angles = places.astype(jnp.float32)[..., None] * frequency
    angles = angles.reshape(places.shape + (1,) * (tensor.ndim - places.ndim - 1) + (half_dim,))
    cosine = jnp.cos(angles)
    sine_part = jnp.sin(angles) * direction
    leading = tensor[..., :half_dim]
    trailing = tensor[..., half_dim:]
    return jnp.concatenate(
        [leading * cosine - trailing * sine_part, leading * sine_part + trailing * cosine], axis=-1
    )


def contract_rows(left, right):
    return lax.dot_general(
        left, right, (((0,), (0,)), ((), ())), preferred_element_type=jnp.float32
    )


def contract_cols(left, right):
    return lax.dot_general(
        left, right, (((1,), (1,)), ((), ())), preferred_element_type=jnp.float32
    )


def dot(left, right):
    return lax.dot_general(left, right, (((1,), (0,)), ((), ())), preferred_element_type=F32)


def offsets_of(part, parts, strip, axis, shape):
    index = lax.broadcasted_iota(jnp.int32, shape, axis)
    return (index // strip) * (parts * strip) + part * strip + index % strip


def block_diag_cols(turned, half, lanes):
    row = lax.broadcasted_iota(jnp.int32, (turned.shape[0], lanes), 0)
    zero = jnp.zeros_like(turned)
    return jnp.concatenate(
        [jnp.where(row < half, turned, zero), jnp.where(row >= half, turned, zero)], axis=1
    )


def attend_kernel(dims, part_ref, lam_ref, q_ref, k_ref, v_ref, gain_ref,
                  grouped_ref, mixed_ref, second_ref, lse_ref, vt_ref, qbd_ref, acc_ref):
    slots, parts, heads, tile, width, strip = dims
    half = width // 2
    cols = 2 * tile

    def turn(slot, carry):
        for h in range(heads):
            for c in range(parts):
                vt_ref[h, slot, :, c * tile:(c + 1) * tile] = jnp.transpose(
                    v_ref[c, slot, :, h * width:(h + 1) * width])
        return carry

    lax.fori_loop(0, slots, turn, 0)
    query_off = offsets_of(part_ref[0], parts, strip, 1, (1, tile))
    query_off = jnp.concatenate([query_off, query_off], axis=1)

    def one_block(slot, diag, state):
        out = []
        for h in range(heads):
            peak, total = state[2 * h], state[2 * h + 1]
            scores = []
            for c in range(parts):
                s = dot(k_ref[c, slot, :, h * width:(h + 1) * width], qbd_ref[h])
                if diag:
                    key_off = offsets_of(c, parts, strip, 0, (tile, 1))
                    s = jnp.where(key_off <= query_off, s, NEGATIVE)
                scores.append(s)
            top = scores[0]
            for s in scores[1:]:
                top = jnp.maximum(top, s)
            higher = jnp.maximum(peak, jnp.max(top, axis=0, keepdims=True))
            keep = jnp.exp(peak - higher)
            weights = [jnp.exp(s - higher) for s in scores]
            added = weights[0]
            for w in weights[1:]:
                added = added + w
            total = total * keep + jnp.sum(added, axis=0, keepdims=True)
            low = jnp.concatenate([w.astype(BF16) for w in weights], axis=0)
            acc_ref[h] = acc_ref[h] * keep + dot(vt_ref[h, slot], low)
            out += [higher, total]
        return tuple(out)

    def one_place(place, carry):
        for h in range(heads):
            turned = jnp.transpose(q_ref[place, :, h * width:(h + 1) * width])
            turned = turned * jnp.asarray(half ** -0.5, turned.dtype)
            qbd_ref[h] = block_diag_cols(turned, half, tile)
            acc_ref[h] = jnp.zeros((width, cols), F32)
        state = (jnp.full((1, cols), NEGATIVE, F32), jnp.zeros((1, cols), F32)) * heads
        state = one_block(place, True, state)
        state = lax.fori_loop(
            0, place, lambda j, st: one_block(j, False, st), state)
        for h in range(heads):
            peak, total = state[2 * h], state[2 * h + 1]
            result = acc_ref[h] / total
            second = result[:, tile:]
            mixed = result[:, :tile] - lam_ref[h] * second
            scale = lax.rsqrt(jnp.mean(mixed * mixed, axis=0, keepdims=True) + EPSILON)
            gain = gain_ref[h * width:(h + 1) * width, :] * SHRINK
            grouped = (mixed * scale * gain).astype(BF16)
            grouped_ref[place, :, h * width:(h + 1) * width] = jnp.transpose(grouped)
            mixed_ref[place, h] = mixed
            second_ref[place, h] = second
            lse_ref[place, h] = peak + jnp.log(total)
        return carry

    lax.fori_loop(0, slots, one_place, 0)


def mesh_copy(src, dst, send_sem, recv_sem, device):
    return pltpu.make_async_remote_copy(
        src_ref=src, dst_ref=dst, send_sem=send_sem, recv_sem=recv_sem,
        device_id=device, device_id_type=pl.DeviceIdType.MESH)


def greet(devices):
    barrier = pltpu.get_barrier_semaphore()
    for device in devices:
        pl.semaphore_signal(
            barrier, inc=1, device_id=device, device_id_type=pl.DeviceIdType.MESH)
    pl.semaphore_wait(barrier, len(devices))


def swap_halves(rows, half):
    quarter = half // 2
    lane = lax.broadcasted_iota(jnp.int32, rows.shape, 1)
    back = pltpu.roll(rows, rows.shape[1] - quarter, 1)
    ahead = pltpu.roll(rows, quarter, 1)
    return jnp.where(lane % half < quarter, back, ahead)


def attend_back_kernel(dims, groups, lam_ref, q_ref, k_ref, v_ref, gg_ref, gain_ref,
                       mixed_ref, second_ref, lse_ref, cost_ref, sint_ref, cosn_ref, sinn_ref,
                       wg_ref,
                       gq_ref, gk_ref, gv_ref, gpart_ref, lpart_ref, wsum_ref,
                       kt_ref, qbdt_ref, qbd_ref, gt_ref, g_ref, delta_ref, dqt_ref,
                       dka_ref, dva_ref, sb_ref, r1_ref, s2_ref, r2_ref,
                       wown_ref, wr1_ref, wr2_ref,
                       s1_sem, r1_sem, s2_sem, r2_sem, w1_sem, w2s_sem, w2r_sem):
    slots, parts, heads, tile, width, strip = dims
    half = width // 2
    scale = half ** -0.5
    part = lax.axis_index("ctx")
    row = lax.axis_index("dp")
    core = part % 2
    y = part // 2
    other_core = 1 - core
    other_y = 1 - y
    me = row * 2 + y
    sibling = {"ctx": y * 2 + other_core}
    across = {"ctx": other_y * 2 + core}

    def group_device(index):
        return {"dp": index // 2, "ctx": (index % 2) * 2 + core}

    others = [lax.rem(me + step, groups) for step in range(1, groups)]
    greet([sibling] + [group_device(index) for index in others])

    weights_out = mesh_copy(
        wg_ref.at[:, :, other_core], wr1_ref, w1_sem.at[0], w1_sem.at[1], sibling)
    weights_out.start()
    weights_own = pltpu.make_async_copy(wg_ref.at[:, :, core], wown_ref, w1_sem.at[2])
    weights_own.start()

    def weights_send(step):
        index = others[step]
        return mesh_copy(wown_ref.at[:, index], wr2_ref.at[step], w2s_sem.at[step],
                         w2r_sem.at[step], group_device(index))

    def weights_cross():
        weights_out.wait()
        weights_own.wait()

        def add(index, carry):
            for t in range(wown_ref.shape[0]):
                wown_ref[t, index] = (
                    wown_ref[t, index].astype(F32) + wr1_ref[t, index].astype(F32)).astype(BF16)
            return carry

        lax.fori_loop(0, groups, add, 0)
        for step in range(groups - 1):
            weights_send(step).start()

    def weights_finish():
        for step in range(groups - 1):
            weights_send(step).wait()
        for t in range(wown_ref.shape[0]):
            total = wown_ref[t, me].astype(F32)
            for step in range(groups - 1):
                total = total + wr2_ref[step, t].astype(F32)
            wsum_ref[t] = total

    def first_copy(j):
        return mesh_copy(sb_ref.at[j, other_core], r1_ref.at[j], s1_sem.at[j], r1_sem.at[j],
                         sibling)

    def second_copy(j):
        return mesh_copy(s2_ref.at[j], r2_ref.at[j], s2_sem.at[j], r2_sem.at[j], across)

    def pass_on(j):
        first_copy(j).wait()
        s2_ref[j] = (
            sb_ref[j, core, other_y].astype(F32) + r1_ref[j, other_y].astype(F32)).astype(BF16)

    def finish(j):
        second_copy(j).wait()
        total = (sb_ref[j, core, y].astype(F32) + r1_ref[j, y].astype(F32)
                 + r2_ref[j].astype(F32))
        gv_ref[j] = total[1].astype(BF16)
        for h in range(heads):
            lanes = slice(h * width, (h + 1) * width)
            grad = total[0, :, lanes]
            gk_ref[j, :, lanes] = (
                grad * cosn_ref[j] + swap_halves(grad, half) * sinn_ref[j]).astype(BF16)

    gpart_ref[...] = jnp.zeros_like(gpart_ref)
    lpart_ref[...] = jnp.zeros_like(lpart_ref)
    query_off = offsets_of(part, parts, strip, 1, (1, tile))
    query_off = jnp.concatenate([query_off, query_off], axis=1)

    def prepare(place, carry):
        for h in range(heads):
            lanes = slice(h * width, (h + 1) * width)
            lam = lam_ref[h]
            grad = gg_ref[lanes, pl.ds(pl.multiple_of(place * tile, tile), tile)]
            mixed = mixed_ref[place, h]
            second = second_ref[place, h]
            rg = lax.rsqrt(jnp.mean(mixed * mixed, axis=0, keepdims=True) + EPSILON)
            gpart_ref[lanes, :] += grad * (mixed * rg)
            up = grad * (gain_ref[lanes, :] * SHRINK)
            gm = rg * up - mixed * (rg * rg * rg * jnp.mean(up * mixed, axis=0, keepdims=True))
            lpart_ref[h] -= gm * second
            along = jnp.sum(gm * second, axis=0, keepdims=True)
            first = jnp.sum(gm * mixed, axis=0, keepdims=True) + lam * along
            delta_ref[place, h] = jnp.concatenate([first, -lam * along], axis=1)
            both = jnp.concatenate([gm, -lam * gm], axis=1)
            gt_ref[place, h] = both.astype(BF16)
            g_ref[place, h] = jnp.transpose(both).astype(BF16)
            query = q_ref[place, :, lanes]
            query = query * jnp.asarray(scale, query.dtype)
            qbdt_ref[place, h] = block_diag_cols(jnp.transpose(query), half, tile)
            lane = lax.broadcasted_iota(jnp.int32, (tile, width), 1)
            zero = jnp.zeros_like(query)
            qbd_ref[place, h, :tile] = jnp.where(lane < half, query, zero)
            qbd_ref[place, h, tile:] = jnp.where(lane >= half, query, zero)
            dqt_ref[place, h] = jnp.zeros((width, tile), F32)
        return carry

    lax.fori_loop(0, slots, prepare, 0)

    def one_block(place, slot, diag):
        for h in range(heads):
            lse = lse_ref[place, h]
            delta = delta_ref[place, h]
            lanes = slice(h * width, (h + 1) * width)
            turned = []
            for c in range(parts):
                keys = k_ref[c, slot, :, lanes]
                s = dot(keys, qbdt_ref[place, h])
                if diag:
                    key_off = offsets_of(c, parts, strip, 0, (tile, 1))
                    s = jnp.where(key_off <= query_off, s, NEGATIVE)
                weights = jnp.exp(s - lse)
                probs = dot(v_ref[c, slot, :, lanes], gt_ref[place, h])
                ds = (weights * (probs - delta)).astype(BF16)
                dv = dot(weights.astype(BF16), g_ref[place, h])
                dk = dot(ds, qbd_ref[place, h])
                if diag:
                    dva_ref[h, c] = dv
                    dka_ref[h, c] = dk
                else:
                    dva_ref[h, c] += dv
                    dka_ref[h, c] += dk
                turned.append(ds)
            dq = dot(kt_ref[h], jnp.concatenate(turned, axis=0))
            dqt_ref[place, h, :half] += dq[:half, :tile]
            dqt_ref[place, h, half:] += dq[half:, tile:]

    def one_key_block(j, carry):
        slot = j
        for h in range(heads):
            for c in range(parts):
                kt_ref[h, :, c * tile:(c + 1) * tile] = jnp.transpose(
                    k_ref[c, slot, :, h * width:(h + 1) * width])
        one_block(j, slot, True)

        def rest(place, inner):
            one_block(place, slot, False)
            return inner

        lax.fori_loop(j + 1, slots, rest, 0)
        for h in range(heads):
            lanes = slice(h * width, (h + 1) * width)
            for c in range(parts):
                sb_ref[j, c % 2, c // 2, 0, :, lanes] = dka_ref[h, c].astype(BF16)
                sb_ref[j, c % 2, c // 2, 1, :, lanes] = dva_ref[h, c].astype(BF16)

        @pl.when(j >= 1)
        def _():
            pass_on(j - 1)

        @pl.when(j == 0)
        def _():
            weights_cross()

        @pl.when(j >= 2)
        def _():
            finish(j - 2)

        first_copy(j).start()

        @pl.when(j >= 1)
        def _():
            second_copy(j - 1).start()

        return carry

    lax.fori_loop(0, slots, one_key_block, 0)

    pass_on(slots - 1)

    def put(place, carry):
        quarter = half // 2
        for h in range(heads):
            pieces = []
            for m in range(2):
                lead = dqt_ref[place, h, m * half:m * half + quarter]
                trail = dqt_ref[place, h, m * half + quarter:(m + 1) * half]
                pieces.append(lead * cost_ref[place] + trail * sint_ref[place])
                pieces.append(trail * cost_ref[place] - lead * sint_ref[place])
            turned = jnp.concatenate(pieces, axis=0) * scale
            gq_ref[place, :, h * width:(h + 1) * width] = jnp.transpose(turned).astype(BF16)
        return carry

    lax.fori_loop(0, 1, put, 0)
    second_copy(slots - 1).start()
    lax.fori_loop(1, slots, put, 0)
    finish(slots - 2)
    weights_finish()
    finish(slots - 1)


def specs(count, smem):
    return [pl.BlockSpec(memory_space=pltpu.SMEM)] * smem + [
        pl.BlockSpec(memory_space=pltpu.VMEM)] * (count - smem)


def attend(dims, part, lam, queries, keys_all, values_all, gain):
    slots, parts, heads, tile, width, strip = dims
    return pl.pallas_call(
        partial(attend_kernel, dims),
        out_shape=(
            jax.ShapeDtypeStruct((slots, tile, heads * width), BF16),
            jax.ShapeDtypeStruct((slots, heads, width, tile), F32),
            jax.ShapeDtypeStruct((slots, heads, width, tile), F32),
            jax.ShapeDtypeStruct((slots, heads, 1, 2 * tile), F32),
        ),
        in_specs=specs(6, 2),
        out_specs=specs(4, 0),
        scratch_shapes=[
            pltpu.VMEM((heads, slots, width, parts * tile), BF16),
            pltpu.VMEM((heads, width, 2 * tile), BF16),
            pltpu.VMEM((heads, width, 2 * tile), F32),
        ],
        compiler_params=pltpu.CompilerParams(vmem_limit_bytes=48 << 20),
        cost_estimate=pl.CostEstimate(
            flops=20_000_000_000, bytes_accessed=12_000_000, transcendentals=14_000_000),
        name="attend",
    )(part, lam, queries, keys_all, values_all, gain)


def attend_back(dims, groups, lam, queries, keys_all, values_all, gg, gain, mixed, second,
                lse, tables, wgrads):
    slots, parts, heads, tile, width, strip = dims
    assert parts == 4
    full = heads * width
    kinds, rows, cols = wgrads.shape[0], wgrads.shape[-2], wgrads.shape[-1]
    rows_low = jax.ShapeDtypeStruct((slots, tile, full), BF16)
    return pl.pallas_call(
        partial(attend_back_kernel, dims, groups),
        out_shape=(
            rows_low,
            rows_low,
            rows_low,
            jax.ShapeDtypeStruct((full, tile), F32),
            jax.ShapeDtypeStruct((heads, width, tile), F32),
            jax.ShapeDtypeStruct((kinds, rows, cols), F32),
        ),
        in_specs=specs(13, 1) + [pl.BlockSpec(memory_space=pl.ANY)],
        out_specs=specs(6, 0),
        scratch_shapes=[
            pltpu.VMEM((heads, width, parts * tile), BF16),
            pltpu.VMEM((slots, heads, width, 2 * tile), BF16),
            pltpu.VMEM((slots, heads, 2 * tile, width), BF16),
            pltpu.VMEM((slots, heads, width, 2 * tile), BF16),
            pltpu.VMEM((slots, heads, 2 * tile, width), BF16),
            pltpu.VMEM((slots, heads, 1, 2 * tile), F32),
            pltpu.VMEM((slots, heads, width, tile), F32),
            pltpu.VMEM((heads, parts, tile, width), F32),
            pltpu.VMEM((heads, parts, tile, width), F32),
            pltpu.VMEM((slots, 2, 2, 2, tile, full), BF16),
            pltpu.VMEM((slots, 2, 2, tile, full), BF16),
            pltpu.VMEM((slots, 2, tile, full), BF16),
            pltpu.VMEM((slots, 2, tile, full), BF16),
            pltpu.VMEM((kinds, groups, rows, cols), BF16),
            pltpu.VMEM((kinds, groups, rows, cols), BF16),
            pltpu.VMEM((groups - 1, kinds, rows, cols), BF16),
            pltpu.SemaphoreType.DMA((slots,)),
            pltpu.SemaphoreType.DMA((slots,)),
            pltpu.SemaphoreType.DMA((slots,)),
            pltpu.SemaphoreType.DMA((slots,)),
            pltpu.SemaphoreType.DMA((3,)),
            pltpu.SemaphoreType.DMA((groups - 1,)),
            pltpu.SemaphoreType.DMA((groups - 1,)),
        ],
        compiler_params=pltpu.CompilerParams(
            vmem_limit_bytes=60 << 20, collective_id=1, has_side_effects=True),
        cost_estimate=pl.CostEstimate(
            flops=60_000_000_000, bytes_accessed=24_000_000, transcendentals=14_000_000),
        name="attend_back",
    )(lam, queries, keys_all, values_all, gg, gain, mixed, second, lse, *tables, wgrads)


def dot_turned(left, right):
    return lax.dot_general(left, right, (((1,), (1,)), ((), ())), preferred_element_type=F32)


def dot_rows(left, right):
    return lax.dot_general(left, right, (((0,), (0,)), ((), ())), preferred_element_type=F32)


class LineSum:
    def __init__(self, axis, size, own, from_left, from_right, sems):
        self.axis, self.size = axis, size
        self.me = lax.axis_index(axis)
        self.own, self.buffers, self.sems = own, (from_left, from_right), sems

    def copy(self, q, t, side):
        target = self.size - 1 - t + self.me if side == 0 else t - (self.size - 1) + self.me
        target = jnp.clip(target, 0, self.size - 1)
        neighbour = jnp.clip(self.me + (1 if side == 0 else -1), 0, self.size - 1)
        return target, mesh_copy(
            self.own.at[q, target], self.buffers[side].at[q, t], self.sems.at[0, side, q, t],
            self.sems.at[1, side, q, t], {self.axis: neighbour})

    def rank(self, side):
        return self.me if side == 0 else self.size - 1 - self.me

    def step(self, q, t):
        for side in range(2):
            rank = self.rank(side)
            target, copy = self.copy(q, t, side)

            if t > 0:
                @pl.when((rank <= t) & (rank > 0))
                def _():
                    self.copy(q, t - 1, side)[1].wait_recv()
                    self.own[q, target] = (
                        self.own[q, target].astype(F32)
                        + self.buffers[side][q, t - 1].astype(F32)).astype(BF16)

            @pl.when(rank <= t)
            def _():
                copy.start()

    def total(self, q, acc):
        acc[...] = self.own[q, self.me].astype(F32)
        for side in range(2):
            @pl.when(self.rank(side) > 0)
            def _():
                self.copy(q, self.size - 2, side)[1].wait_recv()
                acc[...] += self.buffers[side][q, self.size - 2].astype(F32)

    def drain(self, q):
        for t in range(self.size - 1):
            for side in range(2):
                @pl.when(self.rank(side) <= t)
                def _():
                    self.copy(q, t, side)[1].wait_send()


def line_scratch(chunks, size, rows, width):
    return [
        pltpu.VMEM((chunks, size, rows, width), BF16),
        pltpu.VMEM((chunks, size - 1, rows, width), BF16),
        pltpu.VMEM((chunks, size - 1, rows, width), BF16),
        pltpu.VMEM((rows, width), F32),
        pltpu.SemaphoreType.DMA((2, 2, chunks, size - 1)),
    ]


def finish_kernel(dims, groups, lines, gq_ref, gk_ref, gv_ref, wq_ref, wk_ref, wv_ref, normed_ref,
                  branch_ref, grouped_ref, inputs_ref, gh_ref, gain_ref, small_ref,
                  ig_ref, wsum_ref, vec_ref,
                  own_ref, left_ref, right_ref, acc_ref, line_sem,
                  wloc_ref, wr1_ref, wr2_ref, mixer_ref, va_ref, vb_ref, vc_ref, v2_ref,
                  w1_sem, w2_sem, va_sem, vb_sem, vc_sem):
    slots, parts, heads, tile, width, strip = dims
    full = heads * width
    model = normed_ref.shape[-1]
    chunks = own_ref.shape[0]
    per = slots // chunks
    part = lax.axis_index("ctx")
    row = lax.axis_index("dp")
    place = lax.axis_index("head")
    core = part % 2
    y = part // 2
    other_core = 1 - core
    me = row * 2 + y
    sibling = {"ctx": y * 2 + other_core}

    def group_device(index):
        return {"dp": index // 2, "ctx": (index % 2) * 2 + core}

    others = [lax.rem(me + step, groups) for step in range(1, groups)]
    line_others = [lax.rem(place + step, lines) for step in range(1, lines)]
    greet([sibling] + [group_device(index) for index in others]
          + [{"head": index} for index in line_others])
    line = LineSum("head", lines, own_ref, left_ref, right_ref, line_sem)
    mixer_ref[...] = jnp.zeros_like(mixer_ref)
    block = 256

    def product(q):
        grads = [ref[q * per:(q + 1) * per].reshape(per * tile, full)
                 for ref in (gq_ref, gk_ref, gv_ref)]

        def columns(index, carry):
            cols = pl.ds(pl.multiple_of(index * block, block), block)
            terms = dot_turned(grads[0], wq_ref[cols, :])
            terms += dot_turned(grads[1], wk_ref[cols, :])
            terms += dot_turned(grads[2], wv_ref[cols, :])
            terms = terms.astype(BF16)
            for p in range(per):
                for z in range(lines):
                    own_ref[q, z, p * strip:(p + 1) * strip, cols] = (
                        terms[p * tile + z * strip:p * tile + (z + 1) * strip])
            return carry

        lax.fori_loop(0, model // block, columns, 0)

    rows = wsum_ref.shape[1]
    narrow = 128

    def weight_term(kind):
        rows_ref = branch_ref if kind == 3 else normed_ref
        grad_ref = (gq_ref, gk_ref, gv_ref, grouped_ref)[kind]

        def columns(index, carry):
            cols = pl.ds(pl.multiple_of(index * narrow, narrow), narrow)
            term = jnp.zeros((narrow, full), F32)
            for s in range(0, slots, 2):
                left = rows_ref[s:s + 2, :, cols].reshape(2 * tile, narrow)
                grad = grad_ref[s:s + 2].reshape(2 * tile, full)
                term += dot(jnp.transpose(left), grad)
            wloc_ref[kind, cols] = term.astype(BF16)
            return carry

        lax.fori_loop(0, model // narrow, columns, 0)

    def share(index, which):
        return pl.ds(pl.multiple_of((index * 2 + which) * rows, 16), rows)

    def weights_out(index):
        return mesh_copy(wloc_ref.at[:, share(index, other_core)], wr1_ref.at[:, index],
                         w1_sem.at[0, index], w1_sem.at[1, index], sibling)

    def weights_send(step):
        index = others[step]
        return mesh_copy(wloc_ref.at[:, share(index, core)], wr2_ref.at[step], w2_sem.at[0, step],
                         w2_sem.at[1, step], group_device(index))

    def weights_cross():
        for index in range(groups):
            weights_out(index).wait()

        def add(index, carry):
            for k in range(4):
                wloc_ref[k, share(index, core)] = (
                    wloc_ref[k, share(index, core)].astype(F32) + wr1_ref[k, index].astype(F32)
                ).astype(BF16)
            return carry

        lax.fori_loop(0, groups, add, 0)

    def weights_finish():
        for step in range(groups - 1):
            weights_send(step).wait()
        for k in range(4):
            total = wloc_ref[k, share(me, core)].astype(F32)
            for step in range(groups - 1):
                total = total + wr2_ref[step, k].astype(F32)
            wsum_ref[k] = total

    def close(q):
        line.total(q, acc_ref)
        grad = acc_ref[...]
        x = inputs_ref[q * per:(q + 1) * per].reshape(per * strip, model).astype(F32)
        scale = lax.rsqrt(jnp.mean(x * x, axis=1, keepdims=True) + EPSILON)
        mixer_ref[...] += jnp.sum((grad * (x * scale)).reshape(per * strip // 8, 8, model), axis=0)
        up = grad * gain_ref[...]
        result = (gh_ref[q * per:(q + 1) * per].reshape(per * strip, model) + scale * up
                  - x * (scale * scale * scale * jnp.mean(up * x, axis=1, keepdims=True)))
        ig_ref[q * per:(q + 1) * per] = result.astype(BF16).reshape(per, strip, model)

    for slot in range(chunks + lines - 1):
        if slot < chunks:
            product(slot)
        for t in range(lines - 1):
            if 0 <= slot - t < chunks:
                line.step(slot - t, t)
        if slot < 4:
            weight_term(slot)
            if slot == 3:
                for index in range(groups):
                    weights_out(index).start()
        if slot == 4:
            weights_cross()
        if slot == 5:
            for step in range(groups - 1):
                weights_send(step).start()
        if slot - lines + 1 >= 0:
            close(slot - lines + 1)
    first_row = lax.broadcasted_iota(jnp.int32, small_ref.shape, 0) == 0
    mixer = jnp.broadcast_to(jnp.sum(mixer_ref[...], axis=0, keepdims=True), small_ref.shape)
    va_ref[0] = jnp.where(first_row, mixer, small_ref[...])
    for q in range(chunks):
        line.drain(q)
    swap = mesh_copy(va_ref.at[0], va_ref.at[1], va_sem.at[0], va_sem.at[1], sibling)
    swap.start()
    weights_finish()
    swap.wait()
    vb_ref[me] = va_ref[0] + va_ref[1]

    def group_copy(source, target, sem):
        return mesh_copy(vb_ref.at[source], vb_ref.at[source], vb_sem.at[0, sem],
                         vb_sem.at[1, source], group_device(target))

    for step, index in enumerate(others):
        group_copy(me, index, step).start()
    for step, index in enumerate(others):
        group_copy(index, index, step).wait_recv()
    total = vb_ref[0]
    for index in range(1, groups):
        total = total + vb_ref[index]
    vc_ref[place] = total
    v2_ref[...] = total

    def line_copy(source, target, sem):
        return mesh_copy(vc_ref.at[source], vc_ref.at[source], vc_sem.at[0, sem],
                         vc_sem.at[1, source], {"head": target})

    for step, index in enumerate(line_others):
        line_copy(place, index, step).start()
    for step, index in enumerate(line_others):
        line_copy(index, index, step).wait_recv()
    total = vc_ref[0]
    for index in range(1, lines):
        total = total + vc_ref[index]
    row_index = lax.broadcasted_iota(jnp.int32, total.shape, 0)
    vec_ref[...] = jnp.where(row_index < 2, total, v2_ref[...])
    for step, index in enumerate(others):
        group_copy(me, index, step).wait_send()
    for step, index in enumerate(line_others):
        line_copy(place, index, step).wait_send()


def finish(dims, groups, lines, chunks, rows, *operands):
    slots, parts, heads, tile, width, strip = dims
    full = heads * width
    model = operands[6].shape[-1]
    return pl.pallas_call(
        partial(finish_kernel, dims, groups, lines),
        out_shape=(
            jax.ShapeDtypeStruct((slots, strip, model), BF16),
            jax.ShapeDtypeStruct((4, rows, full), F32),
            jax.ShapeDtypeStruct((8, model), F32),
        ),
        in_specs=specs(13, 0),
        out_specs=specs(3, 0),
        scratch_shapes=line_scratch(chunks, lines, slots // chunks * strip, model) + [
            pltpu.VMEM((4, model, full), BF16),
            pltpu.VMEM((4, groups, rows, full), BF16),
            pltpu.VMEM((groups - 1, 4, rows, full), BF16),
            pltpu.VMEM((8, model), F32),
            pltpu.VMEM((2, 8, model), F32),
            pltpu.VMEM((groups, 8, model), F32),
            pltpu.VMEM((lines, 8, model), F32),
            pltpu.VMEM((8, model), F32),
            pltpu.SemaphoreType.DMA((2, groups)),
            pltpu.SemaphoreType.DMA((2, groups - 1)),
            pltpu.SemaphoreType.DMA((2,)),
            pltpu.SemaphoreType.DMA((2, groups)),
            pltpu.SemaphoreType.DMA((2, lines)),
        ],
        compiler_params=pltpu.CompilerParams(
            vmem_limit_bytes=60 << 20, collective_id=2, has_side_effects=True),
        cost_estimate=pl.CostEstimate(
            flops=8_000_000_000, bytes_accessed=24_000_000, transcendentals=0),
        name="finish",
    )(*operands)


def per_device(
    inputs,
    block_order,
    mixer_gain,
    query_weight,
    key_weight,
    value_weight,
    lambda_qone,
    lambda_kone,
    lambda_qtwo,
    lambda_ktwo,
    group_gain,
    output_weight,
    feed_gain,
    gate_weight,
    up_weight,
    down_weight,
    cotangent,
):
    seq_count, pair_count, short_rows, model_width = inputs.shape
    assert seq_count == 1
    parts = lax.axis_size("ctx")
    head_total = lax.axis_size("head")
    part = lax.axis_index("ctx")
    head_place = lax.axis_index("head")
    block_len = short_rows * head_total
    slots = block_order.shape[1]
    heads_here, head_dim = lambda_qone.shape
    qwidth = query_weight.shape[1]
    width = 2 * head_dim
    tile = block_len // parts
    strip = short_rows // parts
    dims = (slots, parts, heads_here, tile, width, strip)
    row_count = slots * tile
    order = block_order.reshape(slots)
    slot_of = jnp.argsort(order).astype(jnp.int32)
    index = jnp.arange(tile, dtype=jnp.int32)
    row_offsets = (index // strip) * short_rows + part * strip + index % strip
    own_places = jnp.arange(slots, dtype=jnp.int32)[:, None] * block_len + row_offsets[None, :]
    groups = lax.axis_size("dp") * parts // 2
    quarter = head_dim // 2
    frequency = THETA ** (-jnp.arange(quarter, dtype=jnp.float32) / quarter)
    angles = own_places.astype(F32)[:, None, :] * frequency[None, :, None]
    cos_turned, sin_turned = jnp.cos(angles), jnp.sin(angles)
    cos_rows = jnp.tile(cos_turned.transpose(0, 2, 1), (1, 1, 4))
    sin_rows = jnp.tile(sin_turned.transpose(0, 2, 1), (1, 1, 4))
    lane = jnp.arange(width)
    sin_rows = jnp.where(lane % head_dim < quarter, sin_rows, -sin_rows)
    tables = (cos_turned, sin_turned, cos_rows, sin_rows)
    lambda_one = jnp.exp(jnp.sum(lambda_qone * lambda_kone, axis=-1))
    lambda_two = jnp.exp(jnp.sum(lambda_qtwo * lambda_ktwo, axis=-1))
    lambda_head = lambda_one - lambda_two + LAMBDA_INIT
    split_shape = (slots, tile, heads_here, 2, head_dim)
    rows_shape = (slots, tile, model_width)

    def spread(rows):
        cut = rows.reshape(pair_count, parts, strip, model_width).transpose(1, 0, 2, 3)
        cut = lax.all_to_all(cut, "ctx", 0, 0, tiled=True)
        return jnp.take(cut.reshape(slots, strip, model_width), slot_of, axis=0)

    def unspread(rows):
        cut = jnp.take(rows, order, axis=0).reshape(parts, pair_count, strip, model_width)
        cut = lax.all_to_all(cut, "ctx", 0, 0, tiled=True)
        return cut.transpose(1, 0, 2, 3).reshape(1, pair_count, short_rows, model_width)

    inputs_here = spread(inputs)
    tokens = inputs_here.astype(jnp.float32)
    scale_one = rms_scale(tokens)
    normed = (tokens * scale_one * mixer_gain).astype(jnp.bfloat16)
    normed_rows = lax.all_gather(normed, "head", axis=1, tiled=True).reshape(row_count, model_width)
    query_lin = jnp.dot(normed_rows, query_weight, preferred_element_type=jnp.float32)
    key_lin = jnp.dot(normed_rows, key_weight, preferred_element_type=jnp.float32)
    value_lin = jnp.dot(normed_rows, value_weight, preferred_element_type=jnp.float32)
    queries = rotate(query_lin.reshape(split_shape), own_places, 1.0).astype(jnp.bfloat16)
    keys_own = rotate(key_lin.reshape(split_shape), own_places, 1.0).astype(jnp.bfloat16)
    values_own = value_lin.astype(jnp.bfloat16)
    part_shape = (slots, tile, qwidth)
    keys_all = lax.all_gather(keys_own.reshape(part_shape), "ctx", axis=0)
    values_all = lax.all_gather(values_own.reshape(part_shape), "ctx", axis=0)
    part_arr = part.reshape(1).astype(jnp.int32)
    gain_col = group_gain.reshape(qwidth, 1)
    grouped, mixed, second, lse = attend(
        dims, part_arr, lambda_head, queries.reshape(part_shape), keys_all, values_all,
        gain_col)
    grouped = grouped.reshape(row_count, qwidth)
    attn_terms = jnp.dot(grouped, output_weight, preferred_element_type=jnp.float32).reshape(
        rows_shape
    )
    hidden = tokens + lax.psum_scatter(
        attn_terms.astype(jnp.bfloat16), "head", scatter_dimension=1, tiled=True
    ).astype(jnp.float32)
    cotangent_here = spread(cotangent)
    scale_two = rms_scale(hidden)
    normed_two = (hidden * scale_two * feed_gain).astype(jnp.bfloat16)
    feed_rows = lax.all_gather(normed_two, "head", axis=1, tiled=True).reshape(
        row_count, model_width
    )
    gate_vals = jnp.dot(feed_rows, gate_weight, preferred_element_type=jnp.float32)
    up_vals = jnp.dot(feed_rows, up_weight, preferred_element_type=jnp.float32)
    gate_sigmoid = jax.nn.sigmoid(gate_vals)
    silu_gate = gate_vals * gate_sigmoid
    activation = (silu_gate * up_vals).astype(jnp.bfloat16)
    feed_terms = jnp.dot(activation, down_weight, preferred_element_type=jnp.float32).reshape(
        rows_shape
    )
    block_out = (
        hidden
        + lax.psum_scatter(
            feed_terms.astype(jnp.bfloat16), "head", scatter_dimension=1, tiled=True
        ).astype(jnp.float32)
    ).astype(jnp.bfloat16)
    grad_rows = lax.all_gather(cotangent_here, "head", axis=1, tiled=True).reshape(
        row_count, model_width
    )
    down_term = contract_rows(grad_rows, activation)
    grad_activ = contract_cols(grad_rows, down_weight)
    grad_gate = (
        grad_activ * up_vals * gate_sigmoid * (1.0 + gate_vals * (1.0 - gate_sigmoid))
    ).astype(jnp.bfloat16)
    grad_up = (grad_activ * silu_gate).astype(jnp.bfloat16)
    gate_term = contract_rows(feed_rows, grad_gate)
    up_term = contract_rows(feed_rows, grad_up)
    normed_two_terms = (
        contract_cols(grad_gate, gate_weight) + contract_cols(grad_up, up_weight)
    ).reshape(rows_shape)
    grad_normed_two = lax.psum_scatter(
        normed_two_terms.astype(jnp.bfloat16), "head", scatter_dimension=1, tiled=True
    ).astype(jnp.float32)
    feed_part = jnp.sum(grad_normed_two * hidden * scale_two, axis=(0, 1))
    grad_hidden = cotangent_here.astype(jnp.float32) + norm_back(
        grad_normed_two, hidden, scale_two, feed_gain
    )
    branch_rows = lax.all_gather(
        grad_hidden.astype(jnp.bfloat16), "head", axis=1, tiled=True
    ).reshape(row_count, model_width)
    grad_grouped = contract_cols(output_weight, branch_rows)
    shares = lax.axis_size("dp") * parts
    wgrads = jnp.stack([gate_term.astype(BF16), up_term.astype(BF16), down_term.astype(BF16)])
    wgrads = wgrads.reshape(3, groups, 2, model_width // shares, wgrads.shape[-1])
    grad_query, grad_key, grad_value, group_part, lambda_part, feed_sums = attend_back(
        dims, groups, lambda_head, queries.reshape(part_shape), keys_all, values_all,
        grad_grouped, gain_col, mixed, second, lse, tables, wgrads)
    group_part = jnp.sum(group_part, axis=1) * SHRINK
    lambda_part = jnp.sum(lambda_part, axis=(1, 2))
    third = jnp.pad(
        jnp.concatenate([group_part, lambda_part]), (0, model_width - qwidth - heads_here))
    small = jnp.pad(jnp.stack([jnp.zeros_like(feed_part), feed_part, third]), ((0, 5), (0, 0)))
    grad_rows_shape = (slots, tile, model_width)
    input_grad, attn_sums, vectors = finish(
        dims, groups, head_total, 4, model_width // shares, grad_query, grad_key, grad_value,
        query_weight, key_weight, value_weight, normed_rows.reshape(grad_rows_shape),
        branch_rows.reshape(grad_rows_shape), grouped.reshape(part_shape), inputs_here,
        grad_hidden, mixer_gain.reshape(1, model_width), small)
    block_out = unspread(block_out)
    input_grad = unspread(input_grad).astype(F32)
    group_grad = vectors[2, :qwidth]
    lambda_grad = vectors[2, qwidth:qwidth + heads_here]
    qone_grad = (lambda_grad * lambda_one)[:, None] * lambda_kone
    kone_grad = (lambda_grad * lambda_one)[:, None] * lambda_qone
    qtwo_grad = -(lambda_grad * lambda_two)[:, None] * lambda_ktwo
    ktwo_grad = -(lambda_grad * lambda_two)[:, None] * lambda_qtwo
    return (
        block_out,
        input_grad,
        vectors[0],
        attn_sums[0],
        attn_sums[1],
        attn_sums[2],
        qone_grad,
        kone_grad,
        qtwo_grad,
        ktwo_grad,
        group_grad,
        attn_sums[3].T,
        vectors[1],
        feed_sums[0],
        feed_sums[1],
        feed_sums[2].T,
    )


def solution(mesh):
    return jax.shard_map(
        per_device,
        mesh=mesh,
        in_specs=(
            P("dp", "ctx", "head", None),
            P("dp", None),
            P(),
            P(None, "head"),
            P(None, "head"),
            P(None, "head"),
            P("head", None),
            P("head", None),
            P("head", None),
            P("head", None),
            P("head"),
            P("head", None),
            P(),
            P(None, "head"),
            P(None, "head"),
            P("head", None),
            P("dp", "ctx", "head", None),
        ),
        out_specs=(
            P("dp", "ctx", "head", None),
            P("dp", "ctx", "head", None),
            P(),
            P(("dp", "ctx"), "head"),
            P(("dp", "ctx"), "head"),
            P(("dp", "ctx"), "head"),
            P("head", None),
            P("head", None),
            P("head", None),
            P("head", None),
            P("head"),
            P("head", ("dp", "ctx")),
            P(),
            P(("dp", "ctx"), "head"),
            P(("dp", "ctx"), "head"),
            P("head", ("dp", "ctx")),
        ),
        check_vma=False,
    )
```

```python
from functools import partial
import math

import jax
import jax.numpy as jnp
from jax import lax
from jax.experimental import pallas as pl
from jax.experimental.pallas import tpu as pltpu
from jax.sharding import PartitionSpec as P

EPSILON = 1e-05
LAMBDA_INIT = 0.8 - 0.6 * math.exp(-0.3 * 12)
SHRINK = 1.0 - LAMBDA_INIT
THETA = 10000.0
NEGATIVE = -1e30
F32 = jnp.float32
BF16 = jnp.bfloat16


def rms_scale(value_rows):
    return lax.rsqrt(jnp.mean(value_rows * value_rows, axis=-1, keepdims=True) + EPSILON)


def norm_back(grad_in, value_rows, scale, gain):
    upstream = grad_in * gain
    return scale * upstream - value_rows * scale**3 * jnp.mean(
        upstream * value_rows, axis=-1, keepdims=True
    )


def rotate(tensor, places, direction):
    half_dim = tensor.shape[-1] // 2
    frequency = THETA ** (-jnp.arange(half_dim, dtype=jnp.float32) / half_dim)
    angles = places.astype(jnp.float32)[..., None] * frequency
    angles = angles.reshape(places.shape + (1,) * (tensor.ndim - places.ndim - 1) + (half_dim,))
    cosine = jnp.cos(angles)
    sine_part = jnp.sin(angles) * direction
    leading = tensor[..., :half_dim]
    trailing = tensor[..., half_dim:]
    return jnp.concatenate(
        [leading * cosine - trailing * sine_part, leading * sine_part + trailing * cosine], axis=-1
    )


def contract_rows(left, right):
    return lax.dot_general(
        left, right, (((0,), (0,)), ((), ())), preferred_element_type=jnp.float32
    )


def contract_cols(left, right):
    return lax.dot_general(
        left, right, (((1,), (1,)), ((), ())), preferred_element_type=jnp.float32
    )


def dot(left, right):
    return lax.dot_general(left, right, (((1,), (0,)), ((), ())), preferred_element_type=F32)


def offsets_of(part, parts, strip, axis, shape):
    index = lax.broadcasted_iota(jnp.int32, shape, axis)
    return (index // strip) * (parts * strip) + part * strip + index % strip


def block_diag_cols(turned, half, lanes):
    row = lax.broadcasted_iota(jnp.int32, (turned.shape[0], lanes), 0)
    zero = jnp.zeros_like(turned)
    return jnp.concatenate(
        [jnp.where(row < half, turned, zero), jnp.where(row >= half, turned, zero)], axis=1
    )


def attend_kernel(dims, part_ref, lam_ref, q_ref, k_ref, v_ref, gain_ref,
                  grouped_ref, mixed_ref, second_ref, lse_ref, vt_ref, qbd_ref, acc_ref):
    slots, parts, heads, tile, width, strip = dims
    half = width // 2
    cols = 2 * tile

    def turn(slot, carry):
        for h in range(heads):
            for c in range(parts):
                vt_ref[h, slot, :, c * tile:(c + 1) * tile] = jnp.transpose(
                    v_ref[c, slot, :, h * width:(h + 1) * width])
        return carry

    lax.fori_loop(0, slots, turn, 0)
    query_off = offsets_of(part_ref[0], parts, strip, 1, (1, tile))
    query_off = jnp.concatenate([query_off, query_off], axis=1)

    def one_block(slot, diag, state):
        out = []
        for h in range(heads):
            peak, total = state[2 * h], state[2 * h + 1]
            scores = []
            for c in range(parts):
                s = dot(k_ref[c, slot, :, h * width:(h + 1) * width], qbd_ref[h])
                if diag:
                    key_off = offsets_of(c, parts, strip, 0, (tile, 1))
                    s = jnp.where(key_off <= query_off, s, NEGATIVE)
                scores.append(s)
            top = scores[0]
            for s in scores[1:]:
                top = jnp.maximum(top, s)
            higher = jnp.maximum(peak, jnp.max(top, axis=0, keepdims=True))
            keep = jnp.exp(peak - higher)
            weights = [jnp.exp(s - higher) for s in scores]
            added = weights[0]
            for w in weights[1:]:
                added = added + w
            total = total * keep + jnp.sum(added, axis=0, keepdims=True)
            low = jnp.concatenate([w.astype(BF16) for w in weights], axis=0)
            acc_ref[h] = acc_ref[h] * keep + dot(vt_ref[h, slot], low)
            out += [higher, total]
        return tuple(out)

    def one_place(place, carry):
        for h in range(heads):
            turned = jnp.transpose(q_ref[place, :, h * width:(h + 1) * width])
            turned = turned * jnp.asarray(half ** -0.5, turned.dtype)
            qbd_ref[h] = block_diag_cols(turned, half, tile)
            acc_ref[h] = jnp.zeros((width, cols), F32)
        state = (jnp.full((1, cols), NEGATIVE, F32), jnp.zeros((1, cols), F32)) * heads
        state = one_block(place, True, state)
        state = lax.fori_loop(
            0, place, lambda j, st: one_block(j, False, st), state)
        for h in range(heads):
            peak, total = state[2 * h], state[2 * h + 1]
            result = acc_ref[h] / total
            second = result[:, tile:]
            mixed = result[:, :tile] - lam_ref[h] * second
            scale = lax.rsqrt(jnp.mean(mixed * mixed, axis=0, keepdims=True) + EPSILON)
            gain = gain_ref[h * width:(h + 1) * width, :] * SHRINK
            grouped = (mixed * scale * gain).astype(BF16)
            grouped_ref[place, :, h * width:(h + 1) * width] = jnp.transpose(grouped)
            mixed_ref[place, h] = mixed
            second_ref[place, h] = second
            lse_ref[place, h] = peak + jnp.log(total)
        return carry

    lax.fori_loop(0, slots, one_place, 0)


def mesh_copy(src, dst, send_sem, recv_sem, device):
    return pltpu.make_async_remote_copy(
        src_ref=src, dst_ref=dst, send_sem=send_sem, recv_sem=recv_sem,
        device_id=device, device_id_type=pl.DeviceIdType.MESH)


def greet(devices):
    barrier = pltpu.get_barrier_semaphore()
    for device in devices:
        pl.semaphore_signal(
            barrier, inc=1, device_id=device, device_id_type=pl.DeviceIdType.MESH)
    pl.semaphore_wait(barrier, len(devices))


def swap_halves(rows, half):
    quarter = half // 2
    lane = lax.broadcasted_iota(jnp.int32, rows.shape, 1)
    back = pltpu.roll(rows, rows.shape[1] - quarter, 1)
    ahead = pltpu.roll(rows, quarter, 1)
    return jnp.where(lane % half < quarter, back, ahead)


def attend_back_kernel(dims, groups, lam_ref, q_ref, k_ref, v_ref, gg_ref, gain_ref,
                       mixed_ref, second_ref, lse_ref, cost_ref, sint_ref, cosn_ref, sinn_ref,
                       wg_ref,
                       gq_ref, gk_ref, gv_ref, gpart_ref, lpart_ref, wsum_ref,
                       kt_ref, qbdt_ref, qbd_ref, gt_ref, g_ref, delta_ref, dqt_ref,
                       dka_ref, dva_ref, sb_ref, r1_ref, s2_ref, r2_ref,
                       wown_ref, wr1_ref, wr2_ref,
                       s1_sem, r1_sem, s2_sem, r2_sem, w1_sem, w2s_sem, w2r_sem):
    slots, parts, heads, tile, width, strip = dims
    half = width // 2
    scale = half ** -0.5
    part = lax.axis_index("ctx")
    row = lax.axis_index("dp")
    core = part % 2
    y = part // 2
    other_core = 1 - core
    other_y = 1 - y
    me = row * 2 + y
    sibling = {"ctx": y * 2 + other_core}
    across = {"ctx": other_y * 2 + core}

    def group_device(index):
        return {"dp": index // 2, "ctx": (index % 2) * 2 + core}

    others = [lax.rem(me + step, groups) for step in range(1, groups)]
    greet([sibling] + [group_device(index) for index in others])

    weights_out = mesh_copy(
        wg_ref.at[:, :, other_core], wr1_ref, w1_sem.at[0], w1_sem.at[1], sibling)
    weights_out.start()
    weights_own = pltpu.make_async_copy(wg_ref.at[:, :, core], wown_ref, w1_sem.at[2])
    weights_own.start()

    def weights_send(step):
        index = others[step]
        return mesh_copy(wown_ref.at[:, index], wr2_ref.at[step], w2s_sem.at[step],
                         w2r_sem.at[step], group_device(index))

    def weights_cross():
        weights_out.wait()
        weights_own.wait()

        def add(index, carry):
            for t in range(wown_ref.shape[0]):
                wown_ref[t, index] = (
                    wown_ref[t, index].astype(F32) + wr1_ref[t, index].astype(F32)).astype(BF16)
            return carry

        lax.fori_loop(0, groups, add, 0)
        for step in range(groups - 1):
            weights_send(step).start()

    def weights_finish():
        for step in range(groups - 1):
            weights_send(step).wait()
        for t in range(wown_ref.shape[0]):
            total = wown_ref[t, me].astype(F32)
            for step in range(groups - 1):
                total = total + wr2_ref[step, t].astype(F32)
            wsum_ref[t] = total

    def first_copy(j):
        return mesh_copy(sb_ref.at[j, other_core], r1_ref.at[j], s1_sem.at[j], r1_sem.at[j],
                         sibling)

    def second_copy(j):
        return mesh_copy(s2_ref.at[j], r2_ref.at[j], s2_sem.at[j], r2_sem.at[j], across)

    def pass_on(j):
        first_copy(j).wait()
        s2_ref[j] = (
            sb_ref[j, core, other_y].astype(F32) + r1_ref[j, other_y].astype(F32)).astype(BF16)

    def finish(j):
        second_copy(j).wait()
        total = (sb_ref[j, core, y].astype(F32) + r1_ref[j, y].astype(F32)
                 + r2_ref[j].astype(F32))
        gv_ref[j] = total[1].astype(BF16)
        for h in range(heads):
            lanes = slice(h * width, (h + 1) * width)
            grad = total[0, :, lanes]
            gk_ref[j, :, lanes] = (
                grad * cosn_ref[j] + swap_halves(grad, half) * sinn_ref[j]).astype(BF16)

    gpart_ref[...] = jnp.zeros_like(gpart_ref)
    lpart_ref[...] = jnp.zeros_like(lpart_ref)
    query_off = offsets_of(part, parts, strip, 1, (1, tile))
    query_off = jnp.concatenate([query_off, query_off], axis=1)

    def prepare(place, carry):
        for h in range(heads):
            lanes = slice(h * width, (h + 1) * width)
            lam = lam_ref[h]
            grad = gg_ref[lanes, pl.ds(pl.multiple_of(place * tile, tile), tile)]
            mixed = mixed_ref[place, h]
            second = second_ref[place, h]
            rg = lax.rsqrt(jnp.mean(mixed * mixed, axis=0, keepdims=True) + EPSILON)
            gpart_ref[lanes, :] += grad * (mixed * rg)
            up = grad * (gain_ref[lanes, :] * SHRINK)
            gm = rg * up - mixed * (rg * rg * rg * jnp.mean(up * mixed, axis=0, keepdims=True))
            lpart_ref[h] -= gm * second
            along = jnp.sum(gm * second, axis=0, keepdims=True)
            first = jnp.sum(gm * mixed, axis=0, keepdims=True) + lam * along
            delta_ref[place, h] = jnp.concatenate([first, -lam * along], axis=1)
            both = jnp.concatenate([gm, -lam * gm], axis=1)
            gt_ref[place, h] = both.astype(BF16)
            g_ref[place, h] = jnp.transpose(both).astype(BF16)
            query = q_ref[place, :, lanes]
            query = query * jnp.asarray(scale, query.dtype)
            qbdt_ref[place, h] = block_diag_cols(jnp.transpose(query), half, tile)
            lane = lax.broadcasted_iota(jnp.int32, (tile, width), 1)
            zero = jnp.zeros_like(query)
            qbd_ref[place, h, :tile] = jnp.where(lane < half, query, zero)
            qbd_ref[place, h, tile:] = jnp.where(lane >= half, query, zero)
            dqt_ref[place, h] = jnp.zeros((width, tile), F32)
        return carry

    lax.fori_loop(0, slots, prepare, 0)

    def one_block(place, slot, diag):
        for h in range(heads):
            lse = lse_ref[place, h]
            delta = delta_ref[place, h]
            lanes = slice(h * width, (h + 1) * width)
            turned = []
            for c in range(parts):
                keys = k_ref[c, slot, :, lanes]
                s = dot(keys, qbdt_ref[place, h])
                if diag:
                    key_off = offsets_of(c, parts, strip, 0, (tile, 1))
                    s = jnp.where(key_off <= query_off, s, NEGATIVE)
                weights = jnp.exp(s - lse)
                probs = dot(v_ref[c, slot, :, lanes], gt_ref[place, h])
                ds = (weights * (probs - delta)).astype(BF16)
                dv = dot(weights.astype(BF16), g_ref[place, h])
                dk = dot(ds, qbd_ref[place, h])
                if diag:
                    dva_ref[h, c] = dv
                    dka_ref[h, c] = dk
                else:
                    dva_ref[h, c] += dv
                    dka_ref[h, c] += dk
                turned.append(ds)
            dq = dot(kt_ref[h], jnp.concatenate(turned, axis=0))
            dqt_ref[place, h, :half] += dq[:half, :tile]
            dqt_ref[place, h, half:] += dq[half:, tile:]

    def one_key_block(j, carry):
        slot = j
        for h in range(heads):
            for c in range(parts):
                kt_ref[h, :, c * tile:(c + 1) * tile] = jnp.transpose(
                    k_ref[c, slot, :, h * width:(h + 1) * width])
        one_block(j, slot, True)

        def rest(place, inner):
            one_block(place, slot, False)
            return inner

        lax.fori_loop(j + 1, slots, rest, 0)
        for h in range(heads):
            lanes = slice(h * width, (h + 1) * width)
            for c in range(parts):
                sb_ref[j, c % 2, c // 2, 0, :, lanes] = dka_ref[h, c].astype(BF16)
                sb_ref[j, c % 2, c // 2, 1, :, lanes] = dva_ref[h, c].astype(BF16)

        @pl.when(j >= 1)
        def _():
            pass_on(j - 1)

        @pl.when(j == 0)
        def _():
            weights_cross()

        @pl.when(j >= 2)
        def _():
            finish(j - 2)

        first_copy(j).start()

        @pl.when(j >= 1)
        def _():
            second_copy(j - 1).start()

        return carry

    lax.fori_loop(0, slots, one_key_block, 0)

    pass_on(slots - 1)

    def put(place, carry):
        quarter = half // 2
        for h in range(heads):
            pieces = []
            for m in range(2):
                lead = dqt_ref[place, h, m * half:m * half + quarter]
                trail = dqt_ref[place, h, m * half + quarter:(m + 1) * half]
                pieces.append(lead * cost_ref[place] + trail * sint_ref[place])
                pieces.append(trail * cost_ref[place] - lead * sint_ref[place])
            turned = jnp.concatenate(pieces, axis=0) * scale
            gq_ref[place, :, h * width:(h + 1) * width] = jnp.transpose(turned).astype(BF16)
        return carry

    lax.fori_loop(0, 1, put, 0)
    second_copy(slots - 1).start()
    lax.fori_loop(1, slots, put, 0)
    finish(slots - 2)
    weights_finish()
    finish(slots - 1)


def specs(count, smem):
    return [pl.BlockSpec(memory_space=pltpu.SMEM)] * smem + [
        pl.BlockSpec(memory_space=pltpu.VMEM)] * (count - smem)


def attend(dims, part, lam, queries, keys_all, values_all, gain):
    slots, parts, heads, tile, width, strip = dims
    return pl.pallas_call(
        partial(attend_kernel, dims),
        out_shape=(
            jax.ShapeDtypeStruct((slots, tile, heads * width), BF16),
            jax.ShapeDtypeStruct((slots, heads, width, tile), F32),
            jax.ShapeDtypeStruct((slots, heads, width, tile), F32),
            jax.ShapeDtypeStruct((slots, heads, 1, 2 * tile), F32),
        ),
        in_specs=specs(6, 2),
        out_specs=specs(4, 0),
        scratch_shapes=[
            pltpu.VMEM((heads, slots, width, parts * tile), BF16),
            pltpu.VMEM((heads, width, 2 * tile), BF16),
            pltpu.VMEM((heads, width, 2 * tile), F32),
        ],
        compiler_params=pltpu.CompilerParams(vmem_limit_bytes=48 << 20),
        cost_estimate=pl.CostEstimate(
            flops=20_000_000_000, bytes_accessed=12_000_000, transcendentals=14_000_000),
        name="attend",
    )(part, lam, queries, keys_all, values_all, gain)


def attend_back(dims, groups, lam, queries, keys_all, values_all, gg, gain, mixed, second,
                lse, tables, wgrads):
    slots, parts, heads, tile, width, strip = dims
    assert parts == 4
    full = heads * width
    kinds, rows, cols = wgrads.shape[0], wgrads.shape[-2], wgrads.shape[-1]
    rows_low = jax.ShapeDtypeStruct((slots, tile, full), BF16)
    return pl.pallas_call(
        partial(attend_back_kernel, dims, groups),
        out_shape=(
            rows_low,
            rows_low,
            rows_low,
            jax.ShapeDtypeStruct((full, tile), F32),
            jax.ShapeDtypeStruct((heads, width, tile), F32),
            jax.ShapeDtypeStruct((kinds, rows, cols), F32),
        ),
        in_specs=specs(13, 1) + [pl.BlockSpec(memory_space=pl.ANY)],
        out_specs=specs(6, 0),
        scratch_shapes=[
            pltpu.VMEM((heads, width, parts * tile), BF16),
            pltpu.VMEM((slots, heads, width, 2 * tile), BF16),
            pltpu.VMEM((slots, heads, 2 * tile, width), BF16),
            pltpu.VMEM((slots, heads, width, 2 * tile), BF16),
            pltpu.VMEM((slots, heads, 2 * tile, width), BF16),
            pltpu.VMEM((slots, heads, 1, 2 * tile), F32),
            pltpu.VMEM((slots, heads, width, tile), F32),
            pltpu.VMEM((heads, parts, tile, width), F32),
            pltpu.VMEM((heads, parts, tile, width), F32),
            pltpu.VMEM((slots, 2, 2, 2, tile, full), BF16),
            pltpu.VMEM((slots, 2, 2, tile, full), BF16),
            pltpu.VMEM((slots, 2, tile, full), BF16),
            pltpu.VMEM((slots, 2, tile, full), BF16),
            pltpu.VMEM((kinds, groups, rows, cols), BF16),
            pltpu.VMEM((kinds, groups, rows, cols), BF16),
            pltpu.VMEM((groups - 1, kinds, rows, cols), BF16),
            pltpu.SemaphoreType.DMA((slots,)),
            pltpu.SemaphoreType.DMA((slots,)),
            pltpu.SemaphoreType.DMA((slots,)),
            pltpu.SemaphoreType.DMA((slots,)),
            pltpu.SemaphoreType.DMA((3,)),
            pltpu.SemaphoreType.DMA((groups - 1,)),
            pltpu.SemaphoreType.DMA((groups - 1,)),
        ],
        compiler_params=pltpu.CompilerParams(
            vmem_limit_bytes=60 << 20, collective_id=1, has_side_effects=True),
        cost_estimate=pl.CostEstimate(
            flops=60_000_000_000, bytes_accessed=24_000_000, transcendentals=14_000_000),
        name="attend_back",
    )(lam, queries, keys_all, values_all, gg, gain, mixed, second, lse, *tables, wgrads)


def dot_turned(left, right):
    return lax.dot_general(left, right, (((1,), (1,)), ((), ())), preferred_element_type=F32)


def dot_rows(left, right):
    return lax.dot_general(left, right, (((0,), (0,)), ((), ())), preferred_element_type=F32)


class LineSum:
    def __init__(self, axis, size, own, from_left, from_right, sems):
        self.axis, self.size = axis, size
        self.me = lax.axis_index(axis)
        self.own, self.buffers, self.sems = own, (from_left, from_right), sems

    def copy(self, q, t, side):
        target = self.size - 1 - t + self.me if side == 0 else t - (self.size - 1) + self.me
        target = jnp.clip(target, 0, self.size - 1)
        neighbour = jnp.clip(self.me + (1 if side == 0 else -1), 0, self.size - 1)
        return target, mesh_copy(
            self.own.at[q, target], self.buffers[side].at[q, t], self.sems.at[0, side, q, t],
            self.sems.at[1, side, q, t], {self.axis: neighbour})

    def rank(self, side):
        return self.me if side == 0 else self.size - 1 - self.me

    def step(self, q, t):
        for side in range(2):
            rank = self.rank(side)
            target, copy = self.copy(q, t, side)

            if t > 0:
                @pl.when((rank <= t) & (rank > 0))
                def _():
                    self.copy(q, t - 1, side)[1].wait_recv()
                    self.own[q, target] = (
                        self.own[q, target].astype(F32)
                        + self.buffers[side][q, t - 1].astype(F32)).astype(BF16)

            @pl.when(rank <= t)
            def _():
                copy.start()

    def total(self, q, acc):
        acc[...] = self.own[q, self.me].astype(F32)
        for side in range(2):
            @pl.when(self.rank(side) > 0)
            def _():
                self.copy(q, self.size - 2, side)[1].wait_recv()
                acc[...] += self.buffers[side][q, self.size - 2].astype(F32)

    def drain(self, q):
        for t in range(self.size - 1):
            for side in range(2):
                @pl.when(self.rank(side) <= t)
                def _():
                    self.copy(q, t, side)[1].wait_send()


def line_scratch(chunks, size, rows, width):
    return [
        pltpu.VMEM((chunks, size, rows, width), BF16),
        pltpu.VMEM((chunks, size - 1, rows, width), BF16),
        pltpu.VMEM((chunks, size - 1, rows, width), BF16),
        pltpu.VMEM((rows, width), F32),
        pltpu.SemaphoreType.DMA((2, 2, chunks, size - 1)),
    ]


def finish_kernel(dims, groups, lines, gq_ref, gk_ref, gv_ref, wq_ref, wk_ref, wv_ref, normed_ref,
                  branch_ref, grouped_ref, inputs_ref, gh_ref, gain_ref, small_ref,
                  ig_ref, wsum_ref, vec_ref,
                  own_ref, left_ref, right_ref, acc_ref, line_sem,
                  wloc_ref, wr1_ref, wr2_ref, mixer_ref, va_ref, vb_ref, vc_ref, v2_ref,
                  w1_sem, w2_sem, va_sem, vb_sem, vc_sem):
    slots, parts, heads, tile, width, strip = dims
    full = heads * width
    model = normed_ref.shape[-1]
    chunks = own_ref.shape[0]
    per = slots // chunks
    part = lax.axis_index("ctx")
    row = lax.axis_index("dp")
    place = lax.axis_index("head")
    core = part % 2
    y = part // 2
    other_core = 1 - core
    me = row * 2 + y
    sibling = {"ctx": y * 2 + other_core}

    def group_device(index):
        return {"dp": index // 2, "ctx": (index % 2) * 2 + core}

    others = [lax.rem(me + step, groups) for step in range(1, groups)]
    line_others = [lax.rem(place + step, lines) for step in range(1, lines)]
    greet([sibling] + [group_device(index) for index in others]
          + [{"head": index} for index in line_others])
    line = LineSum("head", lines, own_ref, left_ref, right_ref, line_sem)
    mixer_ref[...] = jnp.zeros_like(mixer_ref)
    block = 256

    def product(q):
        grads = [ref[q * per:(q + 1) * per].reshape(per * tile, full)
                 for ref in (gq_ref, gk_ref, gv_ref)]

        def columns(index, carry):
            cols = pl.ds(pl.multiple_of(index * block, block), block)
            terms = dot_turned(grads[0], wq_ref[cols, :])
            terms += dot_turned(grads[1], wk_ref[cols, :])
            terms += dot_turned(grads[2], wv_ref[cols, :])
            terms = terms.astype(BF16)
            for p in range(per):
                for z in range(lines):
                    own_ref[q, z, p * strip:(p + 1) * strip, cols] = (
                        terms[p * tile + z * strip:p * tile + (z + 1) * strip])
            return carry

        lax.fori_loop(0, model // block, columns, 0)

    rows = wsum_ref.shape[1]
    narrow = 128

    def weight_term(kind):
        rows_ref = branch_ref if kind == 3 else normed_ref
        grad_ref = (gq_ref, gk_ref, gv_ref, grouped_ref)[kind]

        def columns(index, carry):
            cols = pl.ds(pl.multiple_of(index * narrow, narrow), narrow)
            term = jnp.zeros((narrow, full), F32)
            for s in range(0, slots, 2):
                left = rows_ref[s:s + 2, :, cols].reshape(2 * tile, narrow)
                grad = grad_ref[s:s + 2].reshape(2 * tile, full)
                term += dot(jnp.transpose(left), grad)
            wloc_ref[kind, cols] = term.astype(BF16)
            return carry

        lax.fori_loop(0, model // narrow, columns, 0)

    def share(index, which):
        return pl.ds(pl.multiple_of((index * 2 + which) * rows, 16), rows)

    def weights_out(index):
        return mesh_copy(wloc_ref.at[:, share(index, other_core)], wr1_ref.at[:, index],
                         w1_sem.at[0, index], w1_sem.at[1, index], sibling)

    def weights_send(step):
        index = others[step]
        return mesh_copy(wloc_ref.at[:, share(index, core)], wr2_ref.at[step], w2_sem.at[0, step],
                         w2_sem.at[1, step], group_device(index))

    def weights_cross():
        for index in range(groups):
            weights_out(index).wait()

        def add(index, carry):
            for k in range(4):
                wloc_ref[k, share(index, core)] = (
                    wloc_ref[k, share(index, core)].astype(F32) + wr1_ref[k, index].astype(F32)
                ).astype(BF16)
            return carry

        lax.fori_loop(0, groups, add, 0)

    def weights_finish():
        for step in range(groups - 1):
            weights_send(step).wait()
        for k in range(4):
            total = wloc_ref[k, share(me, core)].astype(F32)
            for step in range(groups - 1):
                total = total + wr2_ref[step, k].astype(F32)
            wsum_ref[k] = total

    def close(q):
        line.total(q, acc_ref)
        grad = acc_ref[...]
        x = inputs_ref[q * per:(q + 1) * per].reshape(per * strip, model).astype(F32)
        scale = lax.rsqrt(jnp.mean(x * x, axis=1, keepdims=True) + EPSILON)
        mixer_ref[...] += jnp.sum((grad * (x * scale)).reshape(per * strip // 8, 8, model), axis=0)
        up = grad * gain_ref[...]
        result = (gh_ref[q * per:(q + 1) * per].reshape(per * strip, model) + scale * up
                  - x * (scale * scale * scale * jnp.mean(up * x, axis=1, keepdims=True)))
        ig_ref[q * per:(q + 1) * per] = result.astype(BF16).reshape(per, strip, model)

    for slot in range(chunks + lines - 1):
        if slot < chunks:
            product(slot)
        for t in range(lines - 1):
            if 0 <= slot - t < chunks:
                line.step(slot - t, t)
        if slot < 4:
            weight_term(slot)
            if slot == 3:
                for index in range(groups):
                    weights_out(index).start()
        if slot == 4:
            weights_cross()
        if slot == 5:
            for step in range(groups - 1):
                weights_send(step).start()
        if slot - lines + 1 >= 0:
            close(slot - lines + 1)
    first_row = lax.broadcasted_iota(jnp.int32, small_ref.shape, 0) == 0
    mixer = jnp.broadcast_to(jnp.sum(mixer_ref[...], axis=0, keepdims=True), small_ref.shape)
    va_ref[0] = jnp.where(first_row, mixer, small_ref[...])
    for q in range(chunks):
        line.drain(q)
    swap = mesh_copy(va_ref.at[0], va_ref.at[1], va_sem.at[0], va_sem.at[1], sibling)
    swap.start()
    weights_finish()
    swap.wait()
    vb_ref[me] = va_ref[0] + va_ref[1]

    def group_copy(source, target, sem):
        return mesh_copy(vb_ref.at[source], vb_ref.at[source], vb_sem.at[0, sem],
                         vb_sem.at[1, source], group_device(target))

    for step, index in enumerate(others):
        group_copy(me, index, step).start()
    for step, index in enumerate(others):
        group_copy(index, index, step).wait_recv()
    total = vb_ref[0]
    for index in range(1, groups):
        total = total + vb_ref[index]
    vc_ref[place] = total
    v2_ref[...] = total

    def line_copy(source, target, sem):
        return mesh_copy(vc_ref.at[source], vc_ref.at[source], vc_sem.at[0, sem],
                         vc_sem.at[1, source], {"head": target})

    for step, index in enumerate(line_others):
        line_copy(place, index, step).start()
    for step, index in enumerate(line_others):
        line_copy(index, index, step).wait_recv()
    total = vc_ref[0]
    for index in range(1, lines):
        total = total + vc_ref[index]
    row_index = lax.broadcasted_iota(jnp.int32, total.shape, 0)
    vec_ref[...] = jnp.where(row_index < 2, total, v2_ref[...])
    for step, index in enumerate(others):
        group_copy(me, index, step).wait_send()
    for step, index in enumerate(line_others):
        line_copy(place, index, step).wait_send()


def finish(dims, groups, lines, chunks, rows, *operands):
    slots, parts, heads, tile, width, strip = dims
    full = heads * width
    model = operands[6].shape[-1]
    return pl.pallas_call(
        partial(finish_kernel, dims, groups, lines),
        out_shape=(
            jax.ShapeDtypeStruct((slots, strip, model), BF16),
            jax.ShapeDtypeStruct((4, rows, full), F32),
            jax.ShapeDtypeStruct((8, model), F32),
        ),
        in_specs=specs(13, 0),
        out_specs=specs(3, 0),
        scratch_shapes=line_scratch(chunks, lines, slots // chunks * strip, model) + [
            pltpu.VMEM((4, model, full), BF16),
            pltpu.VMEM((4, groups, rows, full), BF16),
            pltpu.VMEM((groups - 1, 4, rows, full), BF16),
            pltpu.VMEM((8, model), F32),
            pltpu.VMEM((2, 8, model), F32),
            pltpu.VMEM((groups, 8, model), F32),
            pltpu.VMEM((lines, 8, model), F32),
            pltpu.VMEM((8, model), F32),
            pltpu.SemaphoreType.DMA((2, groups)),
            pltpu.SemaphoreType.DMA((2, groups - 1)),
            pltpu.SemaphoreType.DMA((2,)),
            pltpu.SemaphoreType.DMA((2, groups)),
            pltpu.SemaphoreType.DMA((2, lines)),
        ],
        compiler_params=pltpu.CompilerParams(
            vmem_limit_bytes=60 << 20, collective_id=2, has_side_effects=True),
        cost_estimate=pl.CostEstimate(
            flops=8_000_000_000, bytes_accessed=24_000_000, transcendentals=0),
        name="finish",
    )(*operands)


def per_device(
    inputs,
    block_order,
    mixer_gain,
    query_weight,
    key_weight,
    value_weight,
    lambda_qone,
    lambda_kone,
    lambda_qtwo,
    lambda_ktwo,
    group_gain,
    output_weight,
    feed_gain,
    gate_weight,
    up_weight,
    down_weight,
    cotangent,
):
    seq_count, pair_count, short_rows, model_width = inputs.shape
    assert seq_count == 1
    parts = lax.axis_size("ctx")
    head_total = lax.axis_size("head")
    part = lax.axis_index("ctx")
    head_place = lax.axis_index("head")
    block_len = short_rows * head_total
    slots = block_order.shape[1]
    heads_here, head_dim = lambda_qone.shape
    qwidth = query_weight.shape[1]
    width = 2 * head_dim
    tile = block_len // parts
    strip = short_rows // parts
    dims = (slots, parts, heads_here, tile, width, strip)
    row_count = slots * tile
    order = block_order.reshape(slots)
    slot_of = jnp.argsort(order).astype(jnp.int32)
    index = jnp.arange(tile, dtype=jnp.int32)
    row_offsets = (index // strip) * short_rows + part * strip + index % strip
    own_places = jnp.arange(slots, dtype=jnp.int32)[:, None] * block_len + row_offsets[None, :]
    groups = lax.axis_size("dp") * parts // 2
    quarter = head_dim // 2
    frequency = THETA ** (-jnp.arange(quarter, dtype=jnp.float32) / quarter)
    angles = own_places.astype(F32)[:, None, :] * frequency[None, :, None]
    cos_turned, sin_turned = jnp.cos(angles), jnp.sin(angles)
    cos_rows = jnp.tile(cos_turned.transpose(0, 2, 1), (1, 1, 4))
    sin_rows = jnp.tile(sin_turned.transpose(0, 2, 1), (1, 1, 4))
    lane = jnp.arange(width)
    sin_rows = jnp.where(lane % head_dim < quarter, sin_rows, -sin_rows)
    tables = (cos_turned, sin_turned, cos_rows, sin_rows)
    lambda_one = jnp.exp(jnp.sum(lambda_qone * lambda_kone, axis=-1))
    lambda_two = jnp.exp(jnp.sum(lambda_qtwo * lambda_ktwo, axis=-1))
    lambda_head = lambda_one - lambda_two + LAMBDA_INIT
    split_shape = (slots, tile, heads_here, 2, head_dim)
    rows_shape = (slots, tile, model_width)

    def spread(rows):
        cut = rows.reshape(pair_count, parts, strip, model_width).transpose(1, 0, 2, 3)
        cut = lax.all_to_all(cut, "ctx", 0, 0, tiled=True)
        return jnp.take(cut.reshape(slots, strip, model_width), slot_of, axis=0)

    def unspread(rows):
        cut = jnp.take(rows, order, axis=0).reshape(parts, pair_count, strip, model_width)
        cut = lax.all_to_all(cut, "ctx", 0, 0, tiled=True)
        return cut.transpose(1, 0, 2, 3).reshape(1, pair_count, short_rows, model_width)

    inputs_here = spread(inputs)
    tokens = inputs_here.astype(jnp.float32)
    scale_one = rms_scale(tokens)
    normed = (tokens * scale_one * mixer_gain).astype(jnp.bfloat16)
    normed_rows = lax.all_gather(normed, "head", axis=1, tiled=True).reshape(row_count, model_width)
    cotangent_here = spread(cotangent)
    normed_rows, cotangent_here = lax.optimization_barrier((normed_rows, cotangent_here))
    query_lin = jnp.dot(normed_rows, query_weight, preferred_element_type=jnp.float32)
    key_lin = jnp.dot(normed_rows, key_weight, preferred_element_type=jnp.float32)
    value_lin = jnp.dot(normed_rows, value_weight, preferred_element_type=jnp.float32)
    queries = rotate(query_lin.reshape(split_shape), own_places, 1.0).astype(jnp.bfloat16)
    keys_own = rotate(key_lin.reshape(split_shape), own_places, 1.0).astype(jnp.bfloat16)
    values_own = value_lin.astype(jnp.bfloat16)
    part_shape = (slots, tile, qwidth)
    keys_all = lax.all_gather(keys_own.reshape(part_shape), "ctx", axis=0)
    values_all = lax.all_gather(values_own.reshape(part_shape), "ctx", axis=0)
    keys_all, values_all, late = lax.optimization_barrier((keys_all, values_all, cotangent_here))
    grad_rows = lax.all_gather(late, "head", axis=1, tiled=True)
    part_arr = part.reshape(1).astype(jnp.int32)
    gain_col = group_gain.reshape(qwidth, 1)
    grouped, mixed, second, lse = attend(
        dims, part_arr, lambda_head, queries.reshape(part_shape), keys_all, values_all,
        gain_col)
    grouped, grad_rows = lax.optimization_barrier((grouped, grad_rows))
    grouped = grouped.reshape(row_count, qwidth)
    grad_rows = grad_rows.reshape(row_count, model_width)
    attn_terms = jnp.dot(grouped, output_weight, preferred_element_type=jnp.float32).reshape(
        rows_shape
    )
    hidden = tokens + lax.psum_scatter(
        attn_terms.astype(jnp.bfloat16), "head", scatter_dimension=1, tiled=True
    ).astype(jnp.float32)
    scale_two = rms_scale(hidden)
    normed_two = (hidden * scale_two * feed_gain).astype(jnp.bfloat16)
    feed_rows = lax.all_gather(normed_two, "head", axis=1, tiled=True).reshape(
        row_count, model_width
    )
    gate_vals = jnp.dot(feed_rows, gate_weight, preferred_element_type=jnp.float32)
    up_vals = jnp.dot(feed_rows, up_weight, preferred_element_type=jnp.float32)
    gate_sigmoid = jax.nn.sigmoid(gate_vals)
    silu_gate = gate_vals * gate_sigmoid
    activation = (silu_gate * up_vals).astype(jnp.bfloat16)
    feed_terms = jnp.dot(activation, down_weight, preferred_element_type=jnp.float32).reshape(
        rows_shape
    )
    down_term = contract_rows(grad_rows, activation)
    grad_activ = contract_cols(grad_rows, down_weight)
    grad_gate = (
        grad_activ * up_vals * gate_sigmoid * (1.0 + gate_vals * (1.0 - gate_sigmoid))
    ).astype(jnp.bfloat16)
    grad_up = (grad_activ * silu_gate).astype(jnp.bfloat16)
    gate_term = contract_rows(feed_rows, grad_gate)
    up_term = contract_rows(feed_rows, grad_up)
    normed_two_terms = (
        contract_cols(grad_gate, gate_weight) + contract_cols(grad_up, up_weight)
    ).reshape(rows_shape)
    grad_normed_two = lax.psum_scatter(
        normed_two_terms.astype(jnp.bfloat16), "head", scatter_dimension=1, tiled=True
    ).astype(jnp.float32)
    feed_part = jnp.sum(grad_normed_two * hidden * scale_two, axis=(0, 1))
    grad_hidden = cotangent_here.astype(jnp.float32) + norm_back(
        grad_normed_two, hidden, scale_two, feed_gain
    )
    branch_rows = lax.all_gather(
        grad_hidden.astype(jnp.bfloat16), "head", axis=1, tiled=True
    ).reshape(row_count, model_width)
    branch_rows, feed_terms = lax.optimization_barrier((branch_rows, feed_terms.astype(BF16)))
    feed_sum = lax.psum_scatter(feed_terms, "head", scatter_dimension=1, tiled=True)
    grad_grouped = contract_cols(output_weight, branch_rows)
    shares = lax.axis_size("dp") * parts
    wgrads = jnp.stack([gate_term.astype(BF16), up_term.astype(BF16), down_term.astype(BF16)])
    wgrads = wgrads.reshape(3, groups, 2, model_width // shares, wgrads.shape[-1])
    grad_query, grad_key, grad_value, group_part, lambda_part, feed_sums = attend_back(
        dims, groups, lambda_head, queries.reshape(part_shape), keys_all, values_all,
        grad_grouped, gain_col, mixed, second, lse, tables, wgrads)
    feed_sum, grad_query = lax.optimization_barrier((feed_sum, grad_query))
    block_out = (hidden + feed_sum.astype(F32)).astype(BF16)
    group_part = jnp.sum(group_part, axis=1) * SHRINK
    lambda_part = jnp.sum(lambda_part, axis=(1, 2))
    third = jnp.pad(
        jnp.concatenate([group_part, lambda_part]), (0, model_width - qwidth - heads_here))
    small = jnp.pad(jnp.stack([jnp.zeros_like(feed_part), feed_part, third]), ((0, 5), (0, 0)))
    grad_rows_shape = (slots, tile, model_width)
    input_grad, attn_sums, vectors = finish(
        dims, groups, head_total, 4, model_width // shares, grad_query, grad_key, grad_value,
        query_weight, key_weight, value_weight, normed_rows.reshape(grad_rows_shape),
        branch_rows.reshape(grad_rows_shape), grouped.reshape(part_shape), inputs_here,
        grad_hidden, mixer_gain.reshape(1, model_width), small)
    block_out = unspread(block_out)
    input_grad = unspread(input_grad).astype(F32)
    group_grad = vectors[2, :qwidth]
    lambda_grad = vectors[2, qwidth:qwidth + heads_here]
    qone_grad = (lambda_grad * lambda_one)[:, None] * lambda_kone
    kone_grad = (lambda_grad * lambda_one)[:, None] * lambda_qone
    qtwo_grad = -(lambda_grad * lambda_two)[:, None] * lambda_ktwo
    ktwo_grad = -(lambda_grad * lambda_two)[:, None] * lambda_qtwo
    return (
        block_out,
        input_grad,
        vectors[0],
        attn_sums[0],
        attn_sums[1],
        attn_sums[2],
        qone_grad,
        kone_grad,
        qtwo_grad,
        ktwo_grad,
        group_grad,
        attn_sums[3].T,
        vectors[1],
        feed_sums[0],
        feed_sums[1],
        feed_sums[2].T,
    )


def solution(mesh):
    return jax.shard_map(
        per_device,
        mesh=mesh,
        in_specs=(
            P("dp", "ctx", "head", None),
            P("dp", None),
            P(),
            P(None, "head"),
            P(None, "head"),
            P(None, "head"),
            P("head", None),
            P("head", None),
            P("head", None),
            P("head", None),
            P("head"),
            P("head", None),
            P(),
            P(None, "head"),
            P(None, "head"),
            P("head", None),
            P("dp", "ctx", "head", None),
        ),
        out_specs=(
            P("dp", "ctx", "head", None),
            P("dp", "ctx", "head", None),
            P(),
            P(("dp", "ctx"), "head"),
            P(("dp", "ctx"), "head"),
            P(("dp", "ctx"), "head"),
            P("head", None),
            P("head", None),
            P("head", None),
            P("head", None),
            P("head"),
            P("head", ("dp", "ctx")),
            P(),
            P(("dp", "ctx"), "head"),
            P(("dp", "ctx"), "head"),
            P("head", ("dp", "ctx")),
        ),
        check_vma=False,
    )
```

```python
from functools import partial
import math

import jax
import jax.numpy as jnp
from jax import lax
from jax.experimental import pallas as pl
from jax.experimental.pallas import tpu as pltpu
from jax.sharding import PartitionSpec as P

EPSILON = 1e-05
LAMBDA_INIT = 0.8 - 0.6 * math.exp(-0.3 * 12)
SHRINK = 1.0 - LAMBDA_INIT
THETA = 10000.0
NEGATIVE = -1e30
F32 = jnp.float32
BF16 = jnp.bfloat16


def rms_scale(value_rows):
    return lax.rsqrt(jnp.mean(value_rows * value_rows, axis=-1, keepdims=True) + EPSILON)


def norm_back(grad_in, value_rows, scale, gain):
    upstream = grad_in * gain
    return scale * upstream - value_rows * scale**3 * jnp.mean(
        upstream * value_rows, axis=-1, keepdims=True
    )


def rotate(tensor, places, direction):
    half_dim = tensor.shape[-1] // 2
    frequency = THETA ** (-jnp.arange(half_dim, dtype=jnp.float32) / half_dim)
    angles = places.astype(jnp.float32)[..., None] * frequency
    angles = angles.reshape(places.shape + (1,) * (tensor.ndim - places.ndim - 1) + (half_dim,))
    cosine = jnp.cos(angles)
    sine_part = jnp.sin(angles) * direction
    leading = tensor[..., :half_dim]
    trailing = tensor[..., half_dim:]
    return jnp.concatenate(
        [leading * cosine - trailing * sine_part, leading * sine_part + trailing * cosine], axis=-1
    )


def contract_rows(left, right):
    return lax.dot_general(
        left, right, (((0,), (0,)), ((), ())), preferred_element_type=jnp.float32
    )


def contract_cols(left, right):
    return lax.dot_general(
        left, right, (((1,), (1,)), ((), ())), preferred_element_type=jnp.float32
    )


def dot(left, right):
    return lax.dot_general(left, right, (((1,), (0,)), ((), ())), preferred_element_type=F32)


def offsets_of(part, parts, strip, axis, shape):
    index = lax.broadcasted_iota(jnp.int32, shape, axis)
    return (index // strip) * (parts * strip) + part * strip + index % strip


def block_diag_cols(turned, half, lanes):
    row = lax.broadcasted_iota(jnp.int32, (turned.shape[0], lanes), 0)
    zero = jnp.zeros_like(turned)
    return jnp.concatenate(
        [jnp.where(row < half, turned, zero), jnp.where(row >= half, turned, zero)], axis=1
    )


def attend_kernel(dims, part_ref, lam_ref, q_ref, kv_ref, gain_ref,
                  grouped_ref, mixed_ref, second_ref, lse_ref, vt_ref, qbd_ref, acc_ref):
    slots, parts, heads, tile, width, strip = dims
    half = width // 2
    cols = 2 * tile

    def turn(slot, carry):
        for h in range(heads):
            for c in range(parts):
                vt_ref[h, slot, :, c * tile:(c + 1) * tile] = jnp.transpose(
                    kv_ref[c, slot, 1, :, h * width:(h + 1) * width])
        return carry

    lax.fori_loop(0, slots, turn, 0)
    query_off = offsets_of(part_ref[0], parts, strip, 1, (1, tile))
    query_off = jnp.concatenate([query_off, query_off], axis=1)

    def one_block(slot, diag, state):
        out = []
        for h in range(heads):
            peak, total = state[2 * h], state[2 * h + 1]
            scores = []
            for c in range(parts):
                s = dot(kv_ref[c, slot, 0, :, h * width:(h + 1) * width], qbd_ref[h])
                if diag:
                    key_off = offsets_of(c, parts, strip, 0, (tile, 1))
                    s = jnp.where(key_off <= query_off, s, NEGATIVE)
                scores.append(s)
            top = scores[0]
            for s in scores[1:]:
                top = jnp.maximum(top, s)
            higher = jnp.maximum(peak, jnp.max(top, axis=0, keepdims=True))
            keep = jnp.exp(peak - higher)
            weights = [jnp.exp(s - higher) for s in scores]
            added = weights[0]
            for w in weights[1:]:
                added = added + w
            total = total * keep + jnp.sum(added, axis=0, keepdims=True)
            low = jnp.concatenate([w.astype(BF16) for w in weights], axis=0)
            acc_ref[h] = acc_ref[h] * keep + dot(vt_ref[h, slot], low)
            out += [higher, total]
        return tuple(out)

    def one_place(place, carry):
        for h in range(heads):
            turned = jnp.transpose(q_ref[place, :, h * width:(h + 1) * width])
            turned = turned * jnp.asarray(half ** -0.5, turned.dtype)
            qbd_ref[h] = block_diag_cols(turned, half, tile)
            acc_ref[h] = jnp.zeros((width, cols), F32)
        state = (jnp.full((1, cols), NEGATIVE, F32), jnp.zeros((1, cols), F32)) * heads
        state = one_block(place, True, state)
        state = lax.fori_loop(
            0, place, lambda j, st: one_block(j, False, st), state)
        for h in range(heads):
            peak, total = state[2 * h], state[2 * h + 1]
            result = acc_ref[h] / total
            second = result[:, tile:]
            mixed = result[:, :tile] - lam_ref[h] * second
            scale = lax.rsqrt(jnp.mean(mixed * mixed, axis=0, keepdims=True) + EPSILON)
            gain = gain_ref[h * width:(h + 1) * width, :] * SHRINK
            grouped = (mixed * scale * gain).astype(BF16)
            grouped_ref[place, :, h * width:(h + 1) * width] = jnp.transpose(grouped)
            mixed_ref[place, h] = mixed
            second_ref[place, h] = second
            lse_ref[place, h] = peak + jnp.log(total)
        return carry

    lax.fori_loop(0, slots, one_place, 0)


def mesh_copy(src, dst, send_sem, recv_sem, device):
    return pltpu.make_async_remote_copy(
        src_ref=src, dst_ref=dst, send_sem=send_sem, recv_sem=recv_sem,
        device_id=device, device_id_type=pl.DeviceIdType.MESH)


def greet(devices):
    barrier = pltpu.get_barrier_semaphore()
    for device in devices:
        pl.semaphore_signal(
            barrier, inc=1, device_id=device, device_id_type=pl.DeviceIdType.MESH)
    pl.semaphore_wait(barrier, len(devices))


def swap_halves(rows, half):
    quarter = half // 2
    lane = lax.broadcasted_iota(jnp.int32, rows.shape, 1)
    back = pltpu.roll(rows, rows.shape[1] - quarter, 1)
    ahead = pltpu.roll(rows, quarter, 1)
    return jnp.where(lane % half < quarter, back, ahead)


def attend_back_kernel(dims, groups, lam_ref, q_ref, kv_ref, gg_ref, gain_ref,
                       mixed_ref, second_ref, lse_ref, cost_ref, sint_ref, cosn_ref, sinn_ref,
                       wg_ref,
                       gq_ref, gk_ref, gv_ref, gpart_ref, lpart_ref, wsum_ref,
                       kt_ref, qbdt_ref, qbd_ref, gt_ref, g_ref, delta_ref, dqt_ref,
                       dka_ref, dva_ref, sb_ref, r1_ref, s2_ref, r2_ref,
                       wown_ref, wr1_ref, wr2_ref,
                       s1_sem, r1_sem, s2_sem, r2_sem, w1_sem, w2s_sem, w2r_sem):
    slots, parts, heads, tile, width, strip = dims
    half = width // 2
    scale = half ** -0.5
    part = lax.axis_index("ctx")
    row = lax.axis_index("dp")
    core = part % 2
    y = part // 2
    other_core = 1 - core
    other_y = 1 - y
    me = row * 2 + y
    sibling = {"ctx": y * 2 + other_core}
    across = {"ctx": other_y * 2 + core}

    def group_device(index):
        return {"dp": index // 2, "ctx": (index % 2) * 2 + core}

    others = [lax.rem(me + step, groups) for step in range(1, groups)]
    greet([sibling] + [group_device(index) for index in others])

    weights_out = mesh_copy(
        wg_ref.at[:, :, other_core], wr1_ref, w1_sem.at[0], w1_sem.at[1], sibling)
    weights_out.start()
    weights_own = pltpu.make_async_copy(wg_ref.at[:, :, core], wown_ref, w1_sem.at[2])
    weights_own.start()

    def weights_send(step):
        index = others[step]
        return mesh_copy(wown_ref.at[:, index], wr2_ref.at[step], w2s_sem.at[step],
                         w2r_sem.at[step], group_device(index))

    def weights_cross():
        weights_out.wait()
        weights_own.wait()

        def add(index, carry):
            for t in range(wown_ref.shape[0]):
                wown_ref[t, index] = (
                    wown_ref[t, index].astype(F32) + wr1_ref[t, index].astype(F32)).astype(BF16)
            return carry

        lax.fori_loop(0, groups, add, 0)
        for step in range(groups - 1):
            weights_send(step).start()

    def weights_finish():
        for step in range(groups - 1):
            weights_send(step).wait()
        for t in range(wown_ref.shape[0]):
            total = wown_ref[t, me].astype(F32)
            for step in range(groups - 1):
                total = total + wr2_ref[step, t].astype(F32)
            wsum_ref[t] = total

    def first_copy(j):
        return mesh_copy(sb_ref.at[j, other_core], r1_ref.at[j], s1_sem.at[j], r1_sem.at[j],
                         sibling)

    def second_copy(j):
        return mesh_copy(s2_ref.at[j], r2_ref.at[j], s2_sem.at[j], r2_sem.at[j], across)

    def pass_on(j):
        first_copy(j).wait()
        s2_ref[j] = (
            sb_ref[j, core, other_y].astype(F32) + r1_ref[j, other_y].astype(F32)).astype(BF16)

    def finish(j):
        second_copy(j).wait()
        total = (sb_ref[j, core, y].astype(F32) + r1_ref[j, y].astype(F32)
                 + r2_ref[j].astype(F32))
        gv_ref[j] = total[1].astype(BF16)
        for h in range(heads):
            lanes = slice(h * width, (h + 1) * width)
            grad = total[0, :, lanes]
            gk_ref[j, :, lanes] = (
                grad * cosn_ref[j] + swap_halves(grad, half) * sinn_ref[j]).astype(BF16)

    gpart_ref[...] = jnp.zeros_like(gpart_ref)
    lpart_ref[...] = jnp.zeros_like(lpart_ref)
    query_off = offsets_of(part, parts, strip, 1, (1, tile))
    query_off = jnp.concatenate([query_off, query_off], axis=1)

    def prepare(place, carry):
        for h in range(heads):
            lanes = slice(h * width, (h + 1) * width)
            lam = lam_ref[h]
            grad = gg_ref[lanes, pl.ds(pl.multiple_of(place * tile, tile), tile)]
            mixed = mixed_ref[place, h]
            second = second_ref[place, h]
            rg = lax.rsqrt(jnp.mean(mixed * mixed, axis=0, keepdims=True) + EPSILON)
            gpart_ref[lanes, :] += grad * (mixed * rg)
            up = grad * (gain_ref[lanes, :] * SHRINK)
            gm = rg * up - mixed * (rg * rg * rg * jnp.mean(up * mixed, axis=0, keepdims=True))
            lpart_ref[h] -= gm * second
            along = jnp.sum(gm * second, axis=0, keepdims=True)
            first = jnp.sum(gm * mixed, axis=0, keepdims=True) + lam * along
            delta_ref[place, h] = jnp.concatenate([first, -lam * along], axis=1)
            both = jnp.concatenate([gm, -lam * gm], axis=1)
            gt_ref[place, h] = both.astype(BF16)
            g_ref[place, h] = jnp.transpose(both).astype(BF16)
            query = q_ref[place, :, lanes]
            query = query * jnp.asarray(scale, query.dtype)
            qbdt_ref[place, h] = block_diag_cols(jnp.transpose(query), half, tile)
            lane = lax.broadcasted_iota(jnp.int32, (tile, width), 1)
            zero = jnp.zeros_like(query)
            qbd_ref[place, h, :tile] = jnp.where(lane < half, query, zero)
            qbd_ref[place, h, tile:] = jnp.where(lane >= half, query, zero)
            dqt_ref[place, h] = jnp.zeros((width, tile), F32)
        return carry

    lax.fori_loop(0, slots, prepare, 0)

    def one_block(place, slot, diag):
        for h in range(heads):
            lse = lse_ref[place, h]
            delta = delta_ref[place, h]
            lanes = slice(h * width, (h + 1) * width)
            turned = []
            for c in range(parts):
                keys = kv_ref[c, slot, 0, :, lanes]
                s = dot(keys, qbdt_ref[place, h])
                if diag:
                    key_off = offsets_of(c, parts, strip, 0, (tile, 1))
                    s = jnp.where(key_off <= query_off, s, NEGATIVE)
                weights = jnp.exp(s - lse)
                probs = dot(kv_ref[c, slot, 1, :, lanes], gt_ref[place, h])
                ds = (weights * (probs - delta)).astype(BF16)
                dv = dot(weights.astype(BF16), g_ref[place, h])
                dk = dot(ds, qbd_ref[place, h])
                if diag:
                    dva_ref[h, c] = dv
                    dka_ref[h, c] = dk
                else:
                    dva_ref[h, c] += dv
                    dka_ref[h, c] += dk
                turned.append(ds)
            dq = dot(kt_ref[h], jnp.concatenate(turned, axis=0))
            dqt_ref[place, h, :half] += dq[:half, :tile]
            dqt_ref[place, h, half:] += dq[half:, tile:]

    def one_key_block(j, carry):
        slot = j
        for h in range(heads):
            for c in range(parts):
                kt_ref[h, :, c * tile:(c + 1) * tile] = jnp.transpose(
                    kv_ref[c, slot, 0, :, h * width:(h + 1) * width])
        one_block(j, slot, True)

        def rest(place, inner):
            one_block(place, slot, False)
            return inner

        lax.fori_loop(j + 1, slots, rest, 0)
        for h in range(heads):
            lanes = slice(h * width, (h + 1) * width)
            for c in range(parts):
                sb_ref[j, c % 2, c // 2, 0, :, lanes] = dka_ref[h, c].astype(BF16)
                sb_ref[j, c % 2, c // 2, 1, :, lanes] = dva_ref[h, c].astype(BF16)

        @pl.when(j >= 1)
        def _():
            pass_on(j - 1)

        @pl.when(j == 0)
        def _():
            weights_cross()

        @pl.when(j >= 2)
        def _():
            finish(j - 2)

        first_copy(j).start()

        @pl.when(j >= 1)
        def _():
            second_copy(j - 1).start()

        return carry

    lax.fori_loop(0, slots, one_key_block, 0)

    pass_on(slots - 1)

    def put(place, carry):
        quarter = half // 2
        for h in range(heads):
            pieces = []
            for m in range(2):
                lead = dqt_ref[place, h, m * half:m * half + quarter]
                trail = dqt_ref[place, h, m * half + quarter:(m + 1) * half]
                pieces.append(lead * cost_ref[place] + trail * sint_ref[place])
                pieces.append(trail * cost_ref[place] - lead * sint_ref[place])
            turned = jnp.concatenate(pieces, axis=0) * scale
            gq_ref[place, :, h * width:(h + 1) * width] = jnp.transpose(turned).astype(BF16)
        return carry

    lax.fori_loop(0, 1, put, 0)
    second_copy(slots - 1).start()
    lax.fori_loop(1, slots, put, 0)
    finish(slots - 2)
    weights_finish()
    finish(slots - 1)


def specs(count, smem):
    return [pl.BlockSpec(memory_space=pltpu.SMEM)] * smem + [
        pl.BlockSpec(memory_space=pltpu.VMEM)] * (count - smem)


def attend(dims, part, lam, queries, kv_all, gain):
    slots, parts, heads, tile, width, strip = dims
    return pl.pallas_call(
        partial(attend_kernel, dims),
        out_shape=(
            jax.ShapeDtypeStruct((slots, tile, heads * width), BF16),
            jax.ShapeDtypeStruct((slots, heads, width, tile), F32),
            jax.ShapeDtypeStruct((slots, heads, width, tile), F32),
            jax.ShapeDtypeStruct((slots, heads, 1, 2 * tile), F32),
        ),
        in_specs=specs(5, 2),
        out_specs=specs(4, 0),
        scratch_shapes=[
            pltpu.VMEM((heads, slots, width, parts * tile), BF16),
            pltpu.VMEM((heads, width, 2 * tile), BF16),
            pltpu.VMEM((heads, width, 2 * tile), F32),
        ],
        compiler_params=pltpu.CompilerParams(vmem_limit_bytes=48 << 20),
        cost_estimate=pl.CostEstimate(
            flops=20_000_000_000, bytes_accessed=12_000_000, transcendentals=14_000_000),
        name="attend",
    )(part, lam, queries, kv_all, gain)


def attend_back(dims, groups, lam, queries, kv_all, gg, gain, mixed, second,
                lse, tables, wgrads):
    slots, parts, heads, tile, width, strip = dims
    assert parts == 4
    full = heads * width
    kinds, rows, cols = wgrads.shape[0], wgrads.shape[-2], wgrads.shape[-1]
    rows_low = jax.ShapeDtypeStruct((slots, tile, full), BF16)
    return pl.pallas_call(
        partial(attend_back_kernel, dims, groups),
        out_shape=(
            rows_low,
            rows_low,
            rows_low,
            jax.ShapeDtypeStruct((full, tile), F32),
            jax.ShapeDtypeStruct((heads, width, tile), F32),
            jax.ShapeDtypeStruct((kinds, rows, cols), F32),
        ),
        in_specs=specs(12, 1) + [pl.BlockSpec(memory_space=pl.ANY)],
        out_specs=specs(6, 0),
        scratch_shapes=[
            pltpu.VMEM((heads, width, parts * tile), BF16),
            pltpu.VMEM((slots, heads, width, 2 * tile), BF16),
            pltpu.VMEM((slots, heads, 2 * tile, width), BF16),
            pltpu.VMEM((slots, heads, width, 2 * tile), BF16),
            pltpu.VMEM((slots, heads, 2 * tile, width), BF16),
            pltpu.VMEM((slots, heads, 1, 2 * tile), F32),
            pltpu.VMEM((slots, heads, width, tile), F32),
            pltpu.VMEM((heads, parts, tile, width), F32),
            pltpu.VMEM((heads, parts, tile, width), F32),
            pltpu.VMEM((slots, 2, 2, 2, tile, full), BF16),
            pltpu.VMEM((slots, 2, 2, tile, full), BF16),
            pltpu.VMEM((slots, 2, tile, full), BF16),
            pltpu.VMEM((slots, 2, tile, full), BF16),
            pltpu.VMEM((kinds, groups, rows, cols), BF16),
            pltpu.VMEM((kinds, groups, rows, cols), BF16),
            pltpu.VMEM((groups - 1, kinds, rows, cols), BF16),
            pltpu.SemaphoreType.DMA((slots,)),
            pltpu.SemaphoreType.DMA((slots,)),
            pltpu.SemaphoreType.DMA((slots,)),
            pltpu.SemaphoreType.DMA((slots,)),
            pltpu.SemaphoreType.DMA((3,)),
            pltpu.SemaphoreType.DMA((groups - 1,)),
            pltpu.SemaphoreType.DMA((groups - 1,)),
        ],
        compiler_params=pltpu.CompilerParams(
            vmem_limit_bytes=60 << 20, collective_id=1, has_side_effects=True),
        cost_estimate=pl.CostEstimate(
            flops=60_000_000_000, bytes_accessed=24_000_000, transcendentals=14_000_000),
        name="attend_back",
    )(lam, queries, kv_all, gg, gain, mixed, second, lse, *tables, wgrads)


def dot_turned(left, right):
    return lax.dot_general(left, right, (((1,), (1,)), ((), ())), preferred_element_type=F32)


def dot_rows(left, right):
    return lax.dot_general(left, right, (((0,), (0,)), ((), ())), preferred_element_type=F32)


class LineSum:
    def __init__(self, axis, size, own, from_left, from_right, sems):
        self.axis, self.size = axis, size
        self.me = lax.axis_index(axis)
        self.own, self.buffers, self.sems = own, (from_left, from_right), sems

    def copy(self, q, t, side):
        target = self.size - 1 - t + self.me if side == 0 else t - (self.size - 1) + self.me
        target = jnp.clip(target, 0, self.size - 1)
        neighbour = jnp.clip(self.me + (1 if side == 0 else -1), 0, self.size - 1)
        return target, mesh_copy(
            self.own.at[q, target], self.buffers[side].at[q, t], self.sems.at[0, side, q, t],
            self.sems.at[1, side, q, t], {self.axis: neighbour})

    def rank(self, side):
        return self.me if side == 0 else self.size - 1 - self.me

    def step(self, q, t):
        for side in range(2):
            rank = self.rank(side)
            target, copy = self.copy(q, t, side)

            if t > 0:
                @pl.when((rank <= t) & (rank > 0))
                def _():
                    self.copy(q, t - 1, side)[1].wait_recv()
                    self.own[q, target] = (
                        self.own[q, target].astype(F32)
                        + self.buffers[side][q, t - 1].astype(F32)).astype(BF16)

            @pl.when(rank <= t)
            def _():
                copy.start()

    def total(self, q, acc):
        acc[...] = self.own[q, self.me].astype(F32)
        for side in range(2):
            @pl.when(self.rank(side) > 0)
            def _():
                self.copy(q, self.size - 2, side)[1].wait_recv()
                acc[...] += self.buffers[side][q, self.size - 2].astype(F32)

    def drain(self, q):
        for t in range(self.size - 1):
            for side in range(2):
                @pl.when(self.rank(side) <= t)
                def _():
                    self.copy(q, t, side)[1].wait_send()


def line_scratch(chunks, size, rows, width):
    return [
        pltpu.VMEM((chunks, size, rows, width), BF16),
        pltpu.VMEM((chunks, size - 1, rows, width), BF16),
        pltpu.VMEM((chunks, size - 1, rows, width), BF16),
        pltpu.VMEM((rows, width), F32),
        pltpu.SemaphoreType.DMA((2, 2, chunks, size - 1)),
    ]


def finish_kernel(dims, groups, lines, gq_ref, gk_ref, gv_ref, wq_ref, wk_ref, wv_ref, normed_ref,
                  branch_ref, grouped_ref, inputs_ref, gh_ref, gain_ref, small_ref, bo_ref,
                  ig_ref, wsum_ref, vec_ref, bout_ref,
                  own_ref, left_ref, right_ref, acc_ref, line_sem,
                  wloc_ref, wr1_ref, wr2_ref, mixer_ref, va_ref, vb_ref, vc_ref, v2_ref,
                  w1_sem, w2_sem, va_sem, vb_sem, vc_sem, bo_sem):
    slots, parts, heads, tile, width, strip = dims
    full = heads * width
    model = normed_ref.shape[-1]
    chunks = own_ref.shape[0]
    per = slots // chunks
    part = lax.axis_index("ctx")
    row = lax.axis_index("dp")
    place = lax.axis_index("head")
    core = part % 2
    y = part // 2
    other_core = 1 - core
    me = row * 2 + y
    sibling = {"ctx": y * 2 + other_core}

    def group_device(index):
        return {"dp": index // 2, "ctx": (index % 2) * 2 + core}

    others = [lax.rem(me + step, groups) for step in range(1, groups)]
    line_others = [lax.rem(place + step, lines) for step in range(1, lines)]
    targets = [lax.rem(part + step, parts) for step in range(1, parts)]
    greet([sibling, {"ctx": (1 - y) * 2 + other_core}]
          + [group_device(index) for index in others]
          + [{"head": index} for index in line_others])
    line = LineSum("head", lines, own_ref, left_ref, right_ref, line_sem)
    mixer_ref[...] = jnp.zeros_like(mixer_ref)

    def out_copy(step):
        return mesh_copy(bo_ref.at[targets[step]], bout_ref.at[:, part], bo_sem.at[0, step],
                         bo_sem.at[1, step], {"ctx": targets[step]})

    block = 256

    def product(q):
        grads = [ref[q * per:(q + 1) * per].reshape(per * tile, full)
                 for ref in (gq_ref, gk_ref, gv_ref)]

        def columns(index, carry):
            cols = pl.ds(pl.multiple_of(index * block, block), block)
            terms = dot_turned(grads[0], wq_ref[cols, :])
            terms += dot_turned(grads[1], wk_ref[cols, :])
            terms += dot_turned(grads[2], wv_ref[cols, :])
            terms = terms.astype(BF16)
            for p in range(per):
                for z in range(lines):
                    own_ref[q, z, p * strip:(p + 1) * strip, cols] = (
                        terms[p * tile + z * strip:p * tile + (z + 1) * strip])
            return carry

        lax.fori_loop(0, model // block, columns, 0)

    rows = wsum_ref.shape[1]
    narrow = 128

    def weight_term(kind):
        rows_ref = branch_ref if kind == 3 else normed_ref
        grad_ref = (gq_ref, gk_ref, gv_ref, grouped_ref)[kind]

        def columns(index, carry):
            cols = pl.ds(pl.multiple_of(index * narrow, narrow), narrow)
            term = jnp.zeros((narrow, full), F32)
            for s in range(0, slots, 2):
                left = rows_ref[s:s + 2, :, cols].reshape(2 * tile, narrow)
                grad = grad_ref[s:s + 2].reshape(2 * tile, full)
                term += dot(jnp.transpose(left), grad)
            wloc_ref[kind, cols] = term.astype(BF16)
            return carry

        lax.fori_loop(0, model // narrow, columns, 0)

    def share(index, which):
        return pl.ds(pl.multiple_of((index * 2 + which) * rows, 16), rows)

    def weights_out(index):
        return mesh_copy(wloc_ref.at[:, share(index, other_core)], wr1_ref.at[:, index],
                         w1_sem.at[0, index], w1_sem.at[1, index], sibling)

    def weights_send(step):
        index = others[step]
        return mesh_copy(wloc_ref.at[:, share(index, core)], wr2_ref.at[step], w2_sem.at[0, step],
                         w2_sem.at[1, step], group_device(index))

    def weights_cross():
        for index in range(groups):
            weights_out(index).wait()

        def add(index, carry):
            for k in range(4):
                wloc_ref[k, share(index, core)] = (
                    wloc_ref[k, share(index, core)].astype(F32) + wr1_ref[k, index].astype(F32)
                ).astype(BF16)
            return carry

        lax.fori_loop(0, groups, add, 0)

    def weights_finish():
        for step in range(groups - 1):
            weights_send(step).wait()
        for k in range(4):
            total = wloc_ref[k, share(me, core)].astype(F32)
            for step in range(groups - 1):
                total = total + wr2_ref[step, k].astype(F32)
            wsum_ref[k] = total

    def close(q):
        line.total(q, acc_ref)
        grad = acc_ref[...]
        x = inputs_ref[q * per:(q + 1) * per].reshape(per * strip, model).astype(F32)
        scale = lax.rsqrt(jnp.mean(x * x, axis=1, keepdims=True) + EPSILON)
        mixer_ref[...] += jnp.sum((grad * (x * scale)).reshape(per * strip // 8, 8, model), axis=0)
        up = grad * gain_ref[...]
        result = (gh_ref[q * per:(q + 1) * per].reshape(per * strip, model) + scale * up
                  - x * (scale * scale * scale * jnp.mean(up * x, axis=1, keepdims=True)))
        ig_ref[q * per:(q + 1) * per] = result.astype(BF16).reshape(per, strip, model)

    for slot in range(chunks + lines - 1):
        if slot < chunks:
            product(slot)
        for t in range(lines - 1):
            if 0 <= slot - t < chunks:
                line.step(slot - t, t)
        if slot == 0:
            for step in range(parts - 1):
                out_copy(step).start()
            bout_ref[:, part] = bo_ref[part]
        if slot < 4:
            weight_term(slot)
            if slot == 3:
                for index in range(groups):
                    weights_out(index).start()
        if slot == 4:
            weights_cross()
        if slot == 5:
            for step in range(groups - 1):
                weights_send(step).start()
        if slot - lines + 1 >= 0:
            close(slot - lines + 1)
    first_row = lax.broadcasted_iota(jnp.int32, small_ref.shape, 0) == 0
    mixer = jnp.broadcast_to(jnp.sum(mixer_ref[...], axis=0, keepdims=True), small_ref.shape)
    va_ref[0] = jnp.where(first_row, mixer, small_ref[...])
    for q in range(chunks):
        line.drain(q)
    for step in range(parts - 1):
        out_copy(step).wait()
    swap = mesh_copy(va_ref.at[0], va_ref.at[1], va_sem.at[0], va_sem.at[1], sibling)
    swap.start()
    weights_finish()
    swap.wait()
    vb_ref[me] = va_ref[0] + va_ref[1]

    def group_copy(source, target, sem):
        return mesh_copy(vb_ref.at[source], vb_ref.at[source], vb_sem.at[0, sem],
                         vb_sem.at[1, source], group_device(target))

    for step, index in enumerate(others):
        group_copy(me, index, step).start()
    for step, index in enumerate(others):
        group_copy(index, index, step).wait_recv()
    total = vb_ref[0]
    for index in range(1, groups):
        total = total + vb_ref[index]
    vc_ref[place] = total
    v2_ref[...] = total

    def line_copy(source, target, sem):
        return mesh_copy(vc_ref.at[source], vc_ref.at[source], vc_sem.at[0, sem],
                         vc_sem.at[1, source], {"head": target})

    for step, index in enumerate(line_others):
        line_copy(place, index, step).start()
    for step, index in enumerate(line_others):
        line_copy(index, index, step).wait_recv()
    total = vc_ref[0]
    for index in range(1, lines):
        total = total + vc_ref[index]
    row_index = lax.broadcasted_iota(jnp.int32, total.shape, 0)
    vec_ref[...] = jnp.where(row_index < 2, total, v2_ref[...])
    for step, index in enumerate(others):
        group_copy(me, index, step).wait_send()
    for step, index in enumerate(line_others):
        line_copy(place, index, step).wait_send()


def finish(dims, groups, lines, chunks, rows, *operands):
    slots, parts, heads, tile, width, strip = dims
    full = heads * width
    model = operands[6].shape[-1]
    pairs = operands[-1].shape[1]
    return pl.pallas_call(
        partial(finish_kernel, dims, groups, lines),
        out_shape=(
            jax.ShapeDtypeStruct((slots, strip, model), BF16),
            jax.ShapeDtypeStruct((4, rows, full), F32),
            jax.ShapeDtypeStruct((8, model), F32),
            jax.ShapeDtypeStruct((pairs, parts, strip, model), BF16),
        ),
        in_specs=specs(14, 0),
        out_specs=specs(4, 0),
        scratch_shapes=line_scratch(chunks, lines, slots // chunks * strip, model) + [
            pltpu.VMEM((4, model, full), BF16),
            pltpu.VMEM((4, groups, rows, full), BF16),
            pltpu.VMEM((groups - 1, 4, rows, full), BF16),
            pltpu.VMEM((8, model), F32),
            pltpu.VMEM((2, 8, model), F32),
            pltpu.VMEM((groups, 8, model), F32),
            pltpu.VMEM((lines, 8, model), F32),
            pltpu.VMEM((8, model), F32),
            pltpu.SemaphoreType.DMA((2, groups)),
            pltpu.SemaphoreType.DMA((2, groups - 1)),
            pltpu.SemaphoreType.DMA((2,)),
            pltpu.SemaphoreType.DMA((2, groups)),
            pltpu.SemaphoreType.DMA((2, lines)),
            pltpu.SemaphoreType.DMA((2, parts - 1)),
        ],
        compiler_params=pltpu.CompilerParams(
            vmem_limit_bytes=60 << 20, collective_id=2, has_side_effects=True),
        cost_estimate=pl.CostEstimate(
            flops=8_000_000_000, bytes_accessed=24_000_000, transcendentals=0),
        name="finish",
    )(*operands)


class LineGather:
    def __init__(self, axis, size, view, sems):
        self.axis, self.size, self.view, self.sems = axis, size, view, sems
        self.me = lax.axis_index(axis)

    def copy(self, q, t, side):
        source = jnp.clip(self.me - t if side == 0 else self.me + t, 0, self.size - 1)
        neighbour = jnp.clip(self.me + (1 if side == 0 else -1), 0, self.size - 1)
        return mesh_copy(
            self.view(q, source), self.view(q, source), self.sems.at[0, side, q, t],
            self.sems.at[1, side, q, source], {self.axis: neighbour})

    def rank(self, side):
        return self.me if side == 0 else self.size - 1 - self.me

    def step(self, q, t):
        for side in range(2):
            rank = self.rank(side)

            if t > 0:
                @pl.when(rank >= t)
                def _():
                    self.copy(q, t, side).wait_recv()

            if t < self.size - 1:
                @pl.when((rank >= t) & (rank < self.size - 1))
                def _():
                    self.copy(q, t, side).start()

    def drain(self, q):
        for t in range(self.size - 1):
            for side in range(2):
                rank = self.rank(side)

                @pl.when((rank >= t) & (rank < self.size - 1))
                def _():
                    self.copy(q, t, side).wait_send()


def open_kernel(dims, lines, chunks, x_ref, gain_ref, wq_ref, wk_ref, wv_ref, cosn_ref, sinn_ref,
                cot_ref, normed_ref, q_ref, kv_ref, cout_ref,
                line_sem, c_sem, sib_sem, far_sem, fwd_sem):
    slots, parts, heads, tile, width, strip = dims
    half = width // 2
    per = slots // chunks
    model = x_ref.shape[-1]
    part = lax.axis_index("ctx")
    place = lax.axis_index("head")
    core = part % 2
    y = part // 2
    sibling = {"ctx": y * 2 + 1 - core}
    across = {"ctx": (1 - y) * 2 + core}
    far = (1 - y) * 2 + core
    far_other = (1 - y) * 2 + 1 - core
    near = y * 2 + 1 - core
    targets = [lax.rem(part + step, parts) for step in range(1, parts)]
    greet([{"ctx": target} for target in targets]
          + [{"head": lax.rem(place + step, lines)} for step in range(1, lines)])
    line = LineGather(
        "head", lines, lambda q, s: normed_ref.at[pl.ds(q * per, per), s], line_sem)

    def norm(q):
        x = x_ref[q * per:(q + 1) * per].reshape(per * strip, model).astype(F32)
        scale = lax.rsqrt(jnp.mean(x * x, axis=1, keepdims=True) + EPSILON)
        low = (x * scale * gain_ref[...]).astype(BF16).reshape(per, strip, model)
        for p in range(per):
            normed_ref[q * per + p, place] = low[p]

    def cot_copy(step):
        return mesh_copy(cot_ref.at[:, targets[step]], cout_ref.at[part], c_sem.at[0, step],
                         c_sem.at[1, step], {"ctx": targets[step]})

    def chunk_view(source, q):
        return kv_ref.at[source, pl.ds(q * per, per)]

    def to_sibling(q):
        return mesh_copy(chunk_view(part, q), chunk_view(part, q), sib_sem.at[0, q],
                         sib_sem.at[1, q], sibling)

    def from_sibling(q):
        return mesh_copy(chunk_view(near, q), chunk_view(near, q), sib_sem.at[0, q],
                         sib_sem.at[1, q], sibling)

    def to_far(q):
        return mesh_copy(chunk_view(part, q), chunk_view(part, q), far_sem.at[0, q],
                         far_sem.at[1, q], across)

    def from_far(q):
        return mesh_copy(chunk_view(far, q), chunk_view(far, q), far_sem.at[0, q],
                         far_sem.at[1, q], across)

    def forward(q):
        return mesh_copy(chunk_view(far, q), chunk_view(far, q), fwd_sem.at[0, q],
                         fwd_sem.at[1, q], sibling)

    def forwarded(q):
        return mesh_copy(chunk_view(far_other, q), chunk_view(far_other, q), fwd_sem.at[0, q],
                         fwd_sem.at[1, q], sibling)

    def project(q):
        rows = normed_ref[q * per:(q + 1) * per].reshape(per * tile, model)
        for kind, weight_ref in ((1, wv_ref), (0, wk_ref), (2, wq_ref)):
            result = dot(rows, weight_ref[...])
            for p in range(per):
                at = q * per + p
                for h in range(heads):
                    lanes = slice(h * width, (h + 1) * width)
                    piece = result[p * tile:(p + 1) * tile, lanes]
                    if kind != 1:
                        piece = piece * cosn_ref[at] - swap_halves(piece, half) * sinn_ref[at]
                    if kind == 2:
                        q_ref[at, :, lanes] = piece.astype(BF16)
                    else:
                        kv_ref[part, at, kind, :, lanes] = piece.astype(BF16)

    for slot in range(chunks + lines - 1):
        if slot < chunks:
            norm(slot)
        for t in range(lines):
            if 0 <= slot - t < chunks:
                line.step(slot - t, t)
        if slot == 0:
            for step in range(parts - 1):
                cot_copy(step).start()
            cout_ref[part] = cot_ref[:, part]
        q = slot - lines + 1
        if q >= 0:
            project(q)
            to_far(q).start()
            to_sibling(q).start()
        if q >= 1:
            from_far(q - 1).wait_recv()
            forward(q - 1).start()
    from_far(chunks - 1).wait_recv()
    forward(chunks - 1).start()
    for step in range(parts - 1):
        cot_copy(step).wait()
    for q in range(chunks):
        line.drain(q)
        from_sibling(q).wait_recv()
        to_sibling(q).wait_send()
        to_far(q).wait_send()
    for q in range(chunks):
        forwarded(q).wait_recv()
        forward(q).wait_send()


def open_rows(dims, lines, chunks, *operands):
    slots, parts, heads, tile, width, strip = dims
    full = heads * width
    model = operands[0].shape[-1]
    pairs = operands[-1].shape[0]
    return pl.pallas_call(
        partial(open_kernel, dims, lines, chunks),
        out_shape=(
            jax.ShapeDtypeStruct((slots, lines, strip, model), BF16),
            jax.ShapeDtypeStruct((slots, tile, full), BF16),
            jax.ShapeDtypeStruct((parts, slots, 2, tile, full), BF16),
            jax.ShapeDtypeStruct((parts, pairs, strip, model), BF16),
        ),
        in_specs=specs(8, 0),
        out_specs=specs(4, 0),
        scratch_shapes=[
            pltpu.SemaphoreType.DMA((2, 2, chunks, lines)),
            pltpu.SemaphoreType.DMA((2, parts - 1)),
            pltpu.SemaphoreType.DMA((2, chunks)),
            pltpu.SemaphoreType.DMA((2, chunks)),
            pltpu.SemaphoreType.DMA((2, chunks)),
        ],
        compiler_params=pltpu.CompilerParams(
            vmem_limit_bytes=60 << 20, collective_id=3, has_side_effects=True),
        cost_estimate=pl.CostEstimate(
            flops=4_000_000_000, bytes_accessed=16_000_000, transcendentals=0),
        name="open_rows",
    )(*operands)


def per_device(
    inputs,
    block_order,
    mixer_gain,
    query_weight,
    key_weight,
    value_weight,
    lambda_qone,
    lambda_kone,
    lambda_qtwo,
    lambda_ktwo,
    group_gain,
    output_weight,
    feed_gain,
    gate_weight,
    up_weight,
    down_weight,
    cotangent,
):
    seq_count, pair_count, short_rows, model_width = inputs.shape
    assert seq_count == 1
    parts = lax.axis_size("ctx")
    head_total = lax.axis_size("head")
    part = lax.axis_index("ctx")
    head_place = lax.axis_index("head")
    block_len = short_rows * head_total
    slots = block_order.shape[1]
    heads_here, head_dim = lambda_qone.shape
    qwidth = query_weight.shape[1]
    width = 2 * head_dim
    tile = block_len // parts
    strip = short_rows // parts
    dims = (slots, parts, heads_here, tile, width, strip)
    row_count = slots * tile
    order = block_order.reshape(slots)
    slot_of = jnp.argsort(order).astype(jnp.int32)
    index = jnp.arange(tile, dtype=jnp.int32)
    row_offsets = (index // strip) * short_rows + part * strip + index % strip
    own_places = jnp.arange(slots, dtype=jnp.int32)[:, None] * block_len + row_offsets[None, :]
    groups = lax.axis_size("dp") * parts // 2
    quarter = head_dim // 2
    frequency = THETA ** (-jnp.arange(quarter, dtype=jnp.float32) / quarter)
    angles = own_places.astype(F32)[:, None, :] * frequency[None, :, None]
    cos_turned, sin_turned = jnp.cos(angles), jnp.sin(angles)
    cos_rows = jnp.tile(cos_turned.transpose(0, 2, 1), (1, 1, 4))
    sin_rows = jnp.tile(sin_turned.transpose(0, 2, 1), (1, 1, 4))
    lane = jnp.arange(width)
    sin_rows = jnp.where(lane % head_dim < quarter, sin_rows, -sin_rows)
    tables = (cos_turned, sin_turned, cos_rows, sin_rows)
    lambda_one = jnp.exp(jnp.sum(lambda_qone * lambda_kone, axis=-1))
    lambda_two = jnp.exp(jnp.sum(lambda_qtwo * lambda_ktwo, axis=-1))
    lambda_head = lambda_one - lambda_two + LAMBDA_INIT
    split_shape = (slots, tile, heads_here, 2, head_dim)
    rows_shape = (slots, tile, model_width)

    def spread(rows):
        cut = rows.reshape(pair_count, parts, strip, model_width).transpose(1, 0, 2, 3)
        cut = lax.all_to_all(cut, "ctx", 0, 0, tiled=True)
        return jnp.take(cut.reshape(slots, strip, model_width), slot_of, axis=0)

    def unspread(rows):
        cut = jnp.take(rows, order, axis=0).reshape(parts, pair_count, strip, model_width)
        cut = lax.all_to_all(cut, "ctx", 0, 0, tiled=True)
        return cut.transpose(1, 0, 2, 3).reshape(1, pair_count, short_rows, model_width)

    inputs_here = spread(inputs)
    tokens = inputs_here.astype(jnp.float32)
    part_shape = (slots, tile, qwidth)
    cut_shape = (pair_count, parts, strip, model_width)
    normed_rows, queries, kv_all, cotangent_slots = open_rows(
        dims, head_total, 4, inputs_here, mixer_gain.reshape(1, model_width), query_weight,
        key_weight, value_weight, cos_rows, sin_rows, cotangent.reshape(cut_shape))
    cotangent_here = jnp.take(
        cotangent_slots.reshape(slots, strip, model_width), slot_of, axis=0)
    grad_rows = lax.all_gather(cotangent_here, "head", axis=1, tiled=True)
    part_arr = part.reshape(1).astype(jnp.int32)
    gain_col = group_gain.reshape(qwidth, 1)
    grouped, mixed, second, lse = attend(
        dims, part_arr, lambda_head, queries, kv_all,
        gain_col)
    grouped, grad_rows = lax.optimization_barrier((grouped, grad_rows))
    grouped = grouped.reshape(row_count, qwidth)
    grad_rows = grad_rows.reshape(row_count, model_width)
    attn_terms = jnp.dot(grouped, output_weight, preferred_element_type=jnp.float32).reshape(
        rows_shape
    )
    hidden = tokens + lax.psum_scatter(
        attn_terms.astype(jnp.bfloat16), "head", scatter_dimension=1, tiled=True
    ).astype(jnp.float32)
    scale_two = rms_scale(hidden)
    normed_two = (hidden * scale_two * feed_gain).astype(jnp.bfloat16)
    feed_rows = lax.all_gather(normed_two, "head", axis=1, tiled=True).reshape(
        row_count, model_width
    )
    gate_vals = jnp.dot(feed_rows, gate_weight, preferred_element_type=jnp.float32)
    up_vals = jnp.dot(feed_rows, up_weight, preferred_element_type=jnp.float32)
    gate_sigmoid = jax.nn.sigmoid(gate_vals)
    silu_gate = gate_vals * gate_sigmoid
    activation = (silu_gate * up_vals).astype(jnp.bfloat16)
    feed_terms = jnp.dot(activation, down_weight, preferred_element_type=jnp.float32).reshape(
        rows_shape
    )
    down_term = contract_rows(grad_rows, activation)
    grad_activ = contract_cols(grad_rows, down_weight)
    grad_gate = (
        grad_activ * up_vals * gate_sigmoid * (1.0 + gate_vals * (1.0 - gate_sigmoid))
    ).astype(jnp.bfloat16)
    grad_up = (grad_activ * silu_gate).astype(jnp.bfloat16)
    gate_term = contract_rows(feed_rows, grad_gate)
    up_term = contract_rows(feed_rows, grad_up)
    normed_two_terms = (
        contract_cols(grad_gate, gate_weight) + contract_cols(grad_up, up_weight)
    ).reshape(rows_shape)
    grad_normed_two = lax.psum_scatter(
        normed_two_terms.astype(jnp.bfloat16), "head", scatter_dimension=1, tiled=True
    ).astype(jnp.float32)
    feed_part = jnp.sum(grad_normed_two * hidden * scale_two, axis=(0, 1))
    grad_hidden = cotangent_here.astype(jnp.float32) + norm_back(
        grad_normed_two, hidden, scale_two, feed_gain
    )
    branch_rows = lax.all_gather(
        grad_hidden.astype(jnp.bfloat16), "head", axis=1, tiled=True
    ).reshape(row_count, model_width)
    branch_rows, feed_terms = lax.optimization_barrier((branch_rows, feed_terms.astype(BF16)))
    feed_sum = lax.psum_scatter(feed_terms, "head", scatter_dimension=1, tiled=True)
    grad_grouped = contract_cols(output_weight, branch_rows)
    shares = lax.axis_size("dp") * parts
    wgrads = jnp.stack([gate_term.astype(BF16), up_term.astype(BF16), down_term.astype(BF16)])
    wgrads = wgrads.reshape(3, groups, 2, model_width // shares, wgrads.shape[-1])
    grad_query, grad_key, grad_value, group_part, lambda_part, feed_sums = attend_back(
        dims, groups, lambda_head, queries, kv_all,
        grad_grouped, gain_col, mixed, second, lse, tables, wgrads)
    feed_sum, grad_query = lax.optimization_barrier((feed_sum, grad_query))
    block_out = (hidden + feed_sum.astype(F32)).astype(BF16)
    group_part = jnp.sum(group_part, axis=1) * SHRINK
    lambda_part = jnp.sum(lambda_part, axis=(1, 2))
    third = jnp.pad(
        jnp.concatenate([group_part, lambda_part]), (0, model_width - qwidth - heads_here))
    small = jnp.pad(jnp.stack([jnp.zeros_like(feed_part), feed_part, third]), ((0, 5), (0, 0)))
    grad_rows_shape = (slots, tile, model_width)
    block_slots = jnp.take(block_out, order, axis=0).reshape(
        parts, pair_count, strip, model_width)
    input_grad, attn_sums, vectors, block_out = finish(
        dims, groups, head_total, 4, model_width // shares, grad_query, grad_key, grad_value,
        query_weight, key_weight, value_weight, normed_rows.reshape(grad_rows_shape),
        branch_rows.reshape(grad_rows_shape), grouped.reshape(part_shape), inputs_here,
        grad_hidden, mixer_gain.reshape(1, model_width), small, block_slots)
    block_out = block_out.reshape(inputs.shape)
    input_grad = unspread(input_grad).astype(F32)
    group_grad = vectors[2, :qwidth]
    lambda_grad = vectors[2, qwidth:qwidth + heads_here]
    qone_grad = (lambda_grad * lambda_one)[:, None] * lambda_kone
    kone_grad = (lambda_grad * lambda_one)[:, None] * lambda_qone
    qtwo_grad = -(lambda_grad * lambda_two)[:, None] * lambda_ktwo
    ktwo_grad = -(lambda_grad * lambda_two)[:, None] * lambda_qtwo
    return (
        block_out,
        input_grad,
        vectors[0],
        attn_sums[0],
        attn_sums[1],
        attn_sums[2],
        qone_grad,
        kone_grad,
        qtwo_grad,
        ktwo_grad,
        group_grad,
        attn_sums[3].T,
        vectors[1],
        feed_sums[0],
        feed_sums[1],
        feed_sums[2].T,
    )


def solution(mesh):
    return jax.shard_map(
        per_device,
        mesh=mesh,
        in_specs=(
            P("dp", "ctx", "head", None),
            P("dp", None),
            P(),
            P(None, "head"),
            P(None, "head"),
            P(None, "head"),
            P("head", None),
            P("head", None),
            P("head", None),
            P("head", None),
            P("head"),
            P("head", None),
            P(),
            P(None, "head"),
            P(None, "head"),
            P("head", None),
            P("dp", "ctx", "head", None),
        ),
        out_specs=(
            P("dp", "ctx", "head", None),
            P("dp", "ctx", "head", None),
            P(),
            P(("dp", "ctx"), "head"),
            P(("dp", "ctx"), "head"),
            P(("dp", "ctx"), "head"),
            P("head", None),
            P("head", None),
            P("head", None),
            P("head", None),
            P("head"),
            P("head", ("dp", "ctx")),
            P(),
            P(("dp", "ctx"), "head"),
            P(("dp", "ctx"), "head"),
            P("head", ("dp", "ctx")),
        ),
        check_vma=False,
    )
```

```python
from functools import partial
import math

import jax
import jax.numpy as jnp
from jax import lax
from jax.experimental import pallas as pl
from jax.experimental.pallas import tpu as pltpu
from jax.sharding import PartitionSpec as P

EPSILON = 1e-05
LAMBDA_INIT = 0.8 - 0.6 * math.exp(-0.3 * 12)
SHRINK = 1.0 - LAMBDA_INIT
THETA = 10000.0
NEGATIVE = -1e30
F32 = jnp.float32
BF16 = jnp.bfloat16


def rms_scale(value_rows):
    return lax.rsqrt(jnp.mean(value_rows * value_rows, axis=-1, keepdims=True) + EPSILON)


def norm_back(grad_in, value_rows, scale, gain):
    upstream = grad_in * gain
    return scale * upstream - value_rows * scale**3 * jnp.mean(
        upstream * value_rows, axis=-1, keepdims=True
    )


def rotate(tensor, places, direction):
    half_dim = tensor.shape[-1] // 2
    frequency = THETA ** (-jnp.arange(half_dim, dtype=jnp.float32) / half_dim)
    angles = places.astype(jnp.float32)[..., None] * frequency
    angles = angles.reshape(places.shape + (1,) * (tensor.ndim - places.ndim - 1) + (half_dim,))
    cosine = jnp.cos(angles)
    sine_part = jnp.sin(angles) * direction
    leading = tensor[..., :half_dim]
    trailing = tensor[..., half_dim:]
    return jnp.concatenate(
        [leading * cosine - trailing * sine_part, leading * sine_part + trailing * cosine], axis=-1
    )


def contract_rows(left, right):
    return lax.dot_general(
        left, right, (((0,), (0,)), ((), ())), preferred_element_type=jnp.float32
    )


def contract_cols(left, right):
    return lax.dot_general(
        left, right, (((1,), (1,)), ((), ())), preferred_element_type=jnp.float32
    )


def dot(left, right):
    return lax.dot_general(left, right, (((1,), (0,)), ((), ())), preferred_element_type=F32)


def offsets_of(part, parts, strip, axis, shape):
    index = lax.broadcasted_iota(jnp.int32, shape, axis)
    return (index // strip) * (parts * strip) + part * strip + index % strip


def block_diag_cols(turned, half, lanes):
    row = lax.broadcasted_iota(jnp.int32, (turned.shape[0], lanes), 0)
    zero = jnp.zeros_like(turned)
    return jnp.concatenate(
        [jnp.where(row < half, turned, zero), jnp.where(row >= half, turned, zero)], axis=1
    )


def attend_kernel(dims, part_ref, lam_ref, q_ref, kv_ref, gain_ref,
                  grouped_ref, mixed_ref, second_ref, lse_ref, vt_ref, qbd_ref, acc_ref):
    slots, parts, heads, tile, width, strip = dims
    half = width // 2
    cols = 2 * tile

    def turn(slot, carry):
        for h in range(heads):
            for c in range(parts):
                vt_ref[h, slot, :, c * tile:(c + 1) * tile] = jnp.transpose(
                    kv_ref[c, slot, 1, :, h * width:(h + 1) * width])
        return carry

    lax.fori_loop(0, slots, turn, 0)
    query_off = offsets_of(part_ref[0], parts, strip, 1, (1, tile))
    query_off = jnp.concatenate([query_off, query_off], axis=1)

    def one_block(slot, diag, state):
        out = []
        for h in range(heads):
            peak, total = state[2 * h], state[2 * h + 1]
            scores = []
            for c in range(parts):
                s = dot(kv_ref[c, slot, 0, :, h * width:(h + 1) * width], qbd_ref[h])
                if diag:
                    key_off = offsets_of(c, parts, strip, 0, (tile, 1))
                    s = jnp.where(key_off <= query_off, s, NEGATIVE)
                scores.append(s)
            top = scores[0]
            for s in scores[1:]:
                top = jnp.maximum(top, s)
            higher = jnp.maximum(peak, jnp.max(top, axis=0, keepdims=True))
            keep = jnp.exp(peak - higher)
            weights = [jnp.exp(s - higher) for s in scores]
            added = weights[0]
            for w in weights[1:]:
                added = added + w
            total = total * keep + jnp.sum(added, axis=0, keepdims=True)
            low = jnp.concatenate([w.astype(BF16) for w in weights], axis=0)
            acc_ref[h] = acc_ref[h] * keep + dot(vt_ref[h, slot], low)
            out += [higher, total]
        return tuple(out)

    def one_place(place, carry):
        for h in range(heads):
            turned = jnp.transpose(q_ref[place, :, h * width:(h + 1) * width])
            turned = turned * jnp.asarray(half ** -0.5, turned.dtype)
            qbd_ref[h] = block_diag_cols(turned, half, tile)
            acc_ref[h] = jnp.zeros((width, cols), F32)
        state = (jnp.full((1, cols), NEGATIVE, F32), jnp.zeros((1, cols), F32)) * heads
        state = one_block(place, True, state)
        state = lax.fori_loop(
            0, place, lambda j, st: one_block(j, False, st), state)
        for h in range(heads):
            peak, total = state[2 * h], state[2 * h + 1]
            result = acc_ref[h] / total
            second = result[:, tile:]
            mixed = result[:, :tile] - lam_ref[h] * second
            scale = lax.rsqrt(jnp.mean(mixed * mixed, axis=0, keepdims=True) + EPSILON)
            gain = gain_ref[h * width:(h + 1) * width, :] * SHRINK
            grouped = (mixed * scale * gain).astype(BF16)
            grouped_ref[place, :, h * width:(h + 1) * width] = jnp.transpose(grouped)
            mixed_ref[place, h] = mixed
            second_ref[place, h] = second
            lse_ref[place, h] = peak + jnp.log(total)
        return carry

    lax.fori_loop(0, slots, one_place, 0)


def mesh_copy(src, dst, send_sem, recv_sem, device):
    return pltpu.make_async_remote_copy(
        src_ref=src, dst_ref=dst, send_sem=send_sem, recv_sem=recv_sem,
        device_id=device, device_id_type=pl.DeviceIdType.MESH)


def greet(devices):
    barrier = pltpu.get_barrier_semaphore()
    for device in devices:
        pl.semaphore_signal(
            barrier, inc=1, device_id=device, device_id_type=pl.DeviceIdType.MESH)
    pl.semaphore_wait(barrier, len(devices))


def swap_halves(rows, half):
    quarter = half // 2
    lane = lax.broadcasted_iota(jnp.int32, rows.shape, 1)
    back = pltpu.roll(rows, rows.shape[1] - quarter, 1)
    ahead = pltpu.roll(rows, quarter, 1)
    return jnp.where(lane % half < quarter, back, ahead)


def attend_back_kernel(dims, groups, lam_ref, q_ref, kv_ref, gg_ref, gain_ref,
                       mixed_ref, second_ref, lse_ref, cost_ref, sint_ref, cosn_ref, sinn_ref,
                       wg_ref,
                       gq_ref, gk_ref, gv_ref, gpart_ref, lpart_ref, wsum_ref,
                       kt_ref, qbdt_ref, qbd_ref, gt_ref, g_ref, delta_ref, dqt_ref,
                       dka_ref, dva_ref, sb_ref, r1_ref, s2_ref, r2_ref,
                       wown_ref, wr1_ref, wr2_ref,
                       s1_sem, r1_sem, s2_sem, r2_sem, w1_sem, w2s_sem, w2r_sem):
    slots, parts, heads, tile, width, strip = dims
    half = width // 2
    scale = half ** -0.5
    part = lax.axis_index("ctx")
    row = lax.axis_index("dp")
    core = part % 2
    y = part // 2
    other_core = 1 - core
    other_y = 1 - y
    me = row * 2 + y
    sibling = {"ctx": y * 2 + other_core}
    across = {"ctx": other_y * 2 + core}

    def group_device(index):
        return {"dp": index // 2, "ctx": (index % 2) * 2 + core}

    others = [lax.rem(me + step, groups) for step in range(1, groups)]
    greet([sibling] + [group_device(index) for index in others])

    weights_out = mesh_copy(
        wg_ref.at[:, :, other_core], wr1_ref, w1_sem.at[0], w1_sem.at[1], sibling)
    weights_out.start()
    weights_own = pltpu.make_async_copy(wg_ref.at[:, :, core], wown_ref, w1_sem.at[2])
    weights_own.start()

    def weights_send(step):
        index = others[step]
        return mesh_copy(wown_ref.at[:, index], wr2_ref.at[step], w2s_sem.at[step],
                         w2r_sem.at[step], group_device(index))

    def weights_cross():
        weights_out.wait()
        weights_own.wait()

        def add(index, carry):
            for t in range(wown_ref.shape[0]):
                wown_ref[t, index] = (
                    wown_ref[t, index].astype(F32) + wr1_ref[t, index].astype(F32)).astype(BF16)
            return carry

        lax.fori_loop(0, groups, add, 0)
        for step in range(groups - 1):
            weights_send(step).start()

    def weights_finish():
        for step in range(groups - 1):
            weights_send(step).wait()
        for t in range(wown_ref.shape[0]):
            total = wown_ref[t, me].astype(F32)
            for step in range(groups - 1):
                total = total + wr2_ref[step, t].astype(F32)
            wsum_ref[t] = total

    def first_copy(j):
        return mesh_copy(sb_ref.at[j, other_core], r1_ref.at[j], s1_sem.at[j], r1_sem.at[j],
                         sibling)

    def second_copy(j):
        return mesh_copy(s2_ref.at[j], r2_ref.at[j], s2_sem.at[j], r2_sem.at[j], across)

    def pass_on(j):
        first_copy(j).wait()
        s2_ref[j] = (
            sb_ref[j, core, other_y].astype(F32) + r1_ref[j, other_y].astype(F32)).astype(BF16)

    def finish(j):
        second_copy(j).wait()
        total = (sb_ref[j, core, y].astype(F32) + r1_ref[j, y].astype(F32)
                 + r2_ref[j].astype(F32))
        gv_ref[j] = total[1].astype(BF16)
        for h in range(heads):
            lanes = slice(h * width, (h + 1) * width)
            grad = total[0, :, lanes]
            gk_ref[j, :, lanes] = (
                grad * cosn_ref[j] + swap_halves(grad, half) * sinn_ref[j]).astype(BF16)

    gpart_ref[...] = jnp.zeros_like(gpart_ref)
    lpart_ref[...] = jnp.zeros_like(lpart_ref)
    query_off = offsets_of(part, parts, strip, 1, (1, tile))
    query_off = jnp.concatenate([query_off, query_off], axis=1)

    def prepare(place, carry):
        for h in range(heads):
            lanes = slice(h * width, (h + 1) * width)
            lam = lam_ref[h]
            grad = gg_ref[lanes, pl.ds(pl.multiple_of(place * tile, tile), tile)]
            mixed = mixed_ref[place, h]
            second = second_ref[place, h]
            rg = lax.rsqrt(jnp.mean(mixed * mixed, axis=0, keepdims=True) + EPSILON)
            gpart_ref[lanes, :] += grad * (mixed * rg)
            up = grad * (gain_ref[lanes, :] * SHRINK)
            gm = rg * up - mixed * (rg * rg * rg * jnp.mean(up * mixed, axis=0, keepdims=True))
            lpart_ref[h] -= gm * second
            along = jnp.sum(gm * second, axis=0, keepdims=True)
            first = jnp.sum(gm * mixed, axis=0, keepdims=True) + lam * along
            delta_ref[place, h] = jnp.concatenate([first, -lam * along], axis=1)
            both = jnp.concatenate([gm, -lam * gm], axis=1)
            gt_ref[place, h] = both.astype(BF16)
            g_ref[place, h] = jnp.transpose(both).astype(BF16)
            query = q_ref[place, :, lanes]
            query = query * jnp.asarray(scale, query.dtype)
            qbdt_ref[place, h] = block_diag_cols(jnp.transpose(query), half, tile)
            lane = lax.broadcasted_iota(jnp.int32, (tile, width), 1)
            zero = jnp.zeros_like(query)
            qbd_ref[place, h, :tile] = jnp.where(lane < half, query, zero)
            qbd_ref[place, h, tile:] = jnp.where(lane >= half, query, zero)
            dqt_ref[place, h] = jnp.zeros((width, tile), F32)
        return carry

    lax.fori_loop(0, slots, prepare, 0)

    def one_block(place, slot, diag):
        for h in range(heads):
            lse = lse_ref[place, h]
            delta = delta_ref[place, h]
            lanes = slice(h * width, (h + 1) * width)
            turned = []
            for c in range(parts):
                keys = kv_ref[c, slot, 0, :, lanes]
                s = dot(keys, qbdt_ref[place, h])
                if diag:
                    key_off = offsets_of(c, parts, strip, 0, (tile, 1))
                    s = jnp.where(key_off <= query_off, s, NEGATIVE)
                weights = jnp.exp(s - lse)
                probs = dot(kv_ref[c, slot, 1, :, lanes], gt_ref[place, h])
                ds = (weights * (probs - delta)).astype(BF16)
                dv = dot(weights.astype(BF16), g_ref[place, h])
                dk = dot(ds, qbd_ref[place, h])
                if diag:
                    dva_ref[h, c] = dv
                    dka_ref[h, c] = dk
                else:
                    dva_ref[h, c] += dv
                    dka_ref[h, c] += dk
                turned.append(ds)
            dq = dot(kt_ref[h], jnp.concatenate(turned, axis=0))
            dqt_ref[place, h, :half] += dq[:half, :tile]
            dqt_ref[place, h, half:] += dq[half:, tile:]

    def one_key_block(j, carry):
        slot = j
        for h in range(heads):
            for c in range(parts):
                kt_ref[h, :, c * tile:(c + 1) * tile] = jnp.transpose(
                    kv_ref[c, slot, 0, :, h * width:(h + 1) * width])
        one_block(j, slot, True)

        def rest(place, inner):
            one_block(place, slot, False)
            return inner

        lax.fori_loop(j + 1, slots, rest, 0)
        for h in range(heads):
            lanes = slice(h * width, (h + 1) * width)
            for c in range(parts):
                sb_ref[j, c % 2, c // 2, 0, :, lanes] = dka_ref[h, c].astype(BF16)
                sb_ref[j, c % 2, c // 2, 1, :, lanes] = dva_ref[h, c].astype(BF16)

        @pl.when(j >= 1)
        def _():
            pass_on(j - 1)

        @pl.when(j == 0)
        def _():
            weights_cross()

        @pl.when(j >= 2)
        def _():
            finish(j - 2)

        first_copy(j).start()

        @pl.when(j >= 1)
        def _():
            second_copy(j - 1).start()

        return carry

    lax.fori_loop(0, slots, one_key_block, 0)

    pass_on(slots - 1)

    def put(place, carry):
        quarter = half // 2
        for h in range(heads):
            pieces = []
            for m in range(2):
                lead = dqt_ref[place, h, m * half:m * half + quarter]
                trail = dqt_ref[place, h, m * half + quarter:(m + 1) * half]
                pieces.append(lead * cost_ref[place] + trail * sint_ref[place])
                pieces.append(trail * cost_ref[place] - lead * sint_ref[place])
            turned = jnp.concatenate(pieces, axis=0) * scale
            gq_ref[place, :, h * width:(h + 1) * width] = jnp.transpose(turned).astype(BF16)
        return carry

    lax.fori_loop(0, 1, put, 0)
    second_copy(slots - 1).start()
    lax.fori_loop(1, slots, put, 0)
    finish(slots - 2)
    weights_finish()
    finish(slots - 1)


def specs(count, smem):
    return [pl.BlockSpec(memory_space=pltpu.SMEM)] * smem + [
        pl.BlockSpec(memory_space=pltpu.VMEM)] * (count - smem)


def attend(dims, part, lam, queries, kv_all, gain):
    slots, parts, heads, tile, width, strip = dims
    return pl.pallas_call(
        partial(attend_kernel, dims),
        out_shape=(
            jax.ShapeDtypeStruct((slots, tile, heads * width), BF16),
            jax.ShapeDtypeStruct((slots, heads, width, tile), F32),
            jax.ShapeDtypeStruct((slots, heads, width, tile), F32),
            jax.ShapeDtypeStruct((slots, heads, 1, 2 * tile), F32),
        ),
        in_specs=specs(5, 2),
        out_specs=specs(4, 0),
        scratch_shapes=[
            pltpu.VMEM((heads, slots, width, parts * tile), BF16),
            pltpu.VMEM((heads, width, 2 * tile), BF16),
            pltpu.VMEM((heads, width, 2 * tile), F32),
        ],
        compiler_params=pltpu.CompilerParams(vmem_limit_bytes=48 << 20),
        cost_estimate=pl.CostEstimate(
            flops=20_000_000_000, bytes_accessed=12_000_000, transcendentals=14_000_000),
        name="attend",
    )(part, lam, queries, kv_all, gain)


def attend_back(dims, groups, lam, queries, kv_all, gg, gain, mixed, second,
                lse, tables, wgrads):
    slots, parts, heads, tile, width, strip = dims
    assert parts == 4
    full = heads * width
    kinds, rows, cols = wgrads.shape[0], wgrads.shape[-2], wgrads.shape[-1]
    rows_low = jax.ShapeDtypeStruct((slots, tile, full), BF16)
    return pl.pallas_call(
        partial(attend_back_kernel, dims, groups),
        out_shape=(
            rows_low,
            rows_low,
            rows_low,
            jax.ShapeDtypeStruct((full, tile), F32),
            jax.ShapeDtypeStruct((heads, width, tile), F32),
            jax.ShapeDtypeStruct((kinds, rows, cols), F32),
        ),
        in_specs=specs(12, 1) + [pl.BlockSpec(memory_space=pl.ANY)],
        out_specs=specs(6, 0),
        scratch_shapes=[
            pltpu.VMEM((heads, width, parts * tile), BF16),
            pltpu.VMEM((slots, heads, width, 2 * tile), BF16),
            pltpu.VMEM((slots, heads, 2 * tile, width), BF16),
            pltpu.VMEM((slots, heads, width, 2 * tile), BF16),
            pltpu.VMEM((slots, heads, 2 * tile, width), BF16),
            pltpu.VMEM((slots, heads, 1, 2 * tile), F32),
            pltpu.VMEM((slots, heads, width, tile), F32),
            pltpu.VMEM((heads, parts, tile, width), F32),
            pltpu.VMEM((heads, parts, tile, width), F32),
            pltpu.VMEM((slots, 2, 2, 2, tile, full), BF16),
            pltpu.VMEM((slots, 2, 2, tile, full), BF16),
            pltpu.VMEM((slots, 2, tile, full), BF16),
            pltpu.VMEM((slots, 2, tile, full), BF16),
            pltpu.VMEM((kinds, groups, rows, cols), BF16),
            pltpu.VMEM((kinds, groups, rows, cols), BF16),
            pltpu.VMEM((groups - 1, kinds, rows, cols), BF16),
            pltpu.SemaphoreType.DMA((slots,)),
            pltpu.SemaphoreType.DMA((slots,)),
            pltpu.SemaphoreType.DMA((slots,)),
            pltpu.SemaphoreType.DMA((slots,)),
            pltpu.SemaphoreType.DMA((3,)),
            pltpu.SemaphoreType.DMA((groups - 1,)),
            pltpu.SemaphoreType.DMA((groups - 1,)),
        ],
        compiler_params=pltpu.CompilerParams(
            vmem_limit_bytes=60 << 20, collective_id=1, has_side_effects=True),
        cost_estimate=pl.CostEstimate(
            flops=60_000_000_000, bytes_accessed=24_000_000, transcendentals=14_000_000),
        name="attend_back",
    )(lam, queries, kv_all, gg, gain, mixed, second, lse, *tables, wgrads)


def dot_turned(left, right):
    return lax.dot_general(left, right, (((1,), (1,)), ((), ())), preferred_element_type=F32)


def dot_rows(left, right):
    return lax.dot_general(left, right, (((0,), (0,)), ((), ())), preferred_element_type=F32)


class LineSum:
    def __init__(self, axis, size, own, from_left, from_right, sems):
        self.axis, self.size = axis, size
        self.me = lax.axis_index(axis)
        self.own, self.buffers, self.sems = own, (from_left, from_right), sems

    def copy(self, q, t, side):
        target = self.size - 1 - t + self.me if side == 0 else t - (self.size - 1) + self.me
        target = jnp.clip(target, 0, self.size - 1)
        neighbour = jnp.clip(self.me + (1 if side == 0 else -1), 0, self.size - 1)
        return target, mesh_copy(
            self.own.at[q, target], self.buffers[side].at[q, t], self.sems.at[0, side, q, t],
            self.sems.at[1, side, q, t], {self.axis: neighbour})

    def rank(self, side):
        return self.me if side == 0 else self.size - 1 - self.me

    def step(self, q, t):
        for side in range(2):
            rank = self.rank(side)
            target, copy = self.copy(q, t, side)

            if t > 0:
                @pl.when((rank <= t) & (rank > 0))
                def _():
                    self.copy(q, t - 1, side)[1].wait_recv()
                    self.own[q, target] = (
                        self.own[q, target].astype(F32)
                        + self.buffers[side][q, t - 1].astype(F32)).astype(BF16)

            @pl.when(rank <= t)
            def _():
                copy.start()

    def total(self, q, acc):
        acc[...] = self.own[q, self.me].astype(F32)
        for side in range(2):
            @pl.when(self.rank(side) > 0)
            def _():
                self.copy(q, self.size - 2, side)[1].wait_recv()
                acc[...] += self.buffers[side][q, self.size - 2].astype(F32)

    def drain(self, q):
        for t in range(self.size - 1):
            for side in range(2):
                @pl.when(self.rank(side) <= t)
                def _():
                    self.copy(q, t, side)[1].wait_send()


def line_scratch(chunks, size, rows, width):
    return [
        pltpu.VMEM((chunks, size, rows, width), BF16),
        pltpu.VMEM((chunks, size - 1, rows, width), BF16),
        pltpu.VMEM((chunks, size - 1, rows, width), BF16),
        pltpu.VMEM((rows, width), F32),
        pltpu.SemaphoreType.DMA((2, 2, chunks, size - 1)),
    ]


def finish_kernel(dims, groups, lines, gq_ref, gk_ref, gv_ref, wq_ref, wk_ref, wv_ref, normed_ref,
                  branch_ref, grouped_ref, inputs_ref, gh_ref, gain_ref, small_ref, bo_ref,
                  ig_ref, wsum_ref, vec_ref, bout_ref,
                  own_ref, left_ref, right_ref, acc_ref, line_sem,
                  wloc_ref, wr1_ref, wr2_ref, mixer_ref, va_ref, vb_ref, vc_ref, v2_ref,
                  w1_sem, w2_sem, va_sem, vb_sem, vc_sem, bo_sem):
    slots, parts, heads, tile, width, strip = dims
    full = heads * width
    model = normed_ref.shape[-1]
    chunks = own_ref.shape[0]
    per = slots // chunks
    part = lax.axis_index("ctx")
    row = lax.axis_index("dp")
    place = lax.axis_index("head")
    core = part % 2
    y = part // 2
    other_core = 1 - core
    me = row * 2 + y
    sibling = {"ctx": y * 2 + other_core}

    def group_device(index):
        return {"dp": index // 2, "ctx": (index % 2) * 2 + core}

    others = [lax.rem(me + step, groups) for step in range(1, groups)]
    line_others = [lax.rem(place + step, lines) for step in range(1, lines)]
    targets = [lax.rem(part + step, parts) for step in range(1, parts)]
    greet([sibling, {"ctx": (1 - y) * 2 + other_core}]
          + [group_device(index) for index in others]
          + [{"head": index} for index in line_others])
    line = LineSum("head", lines, own_ref, left_ref, right_ref, line_sem)
    mixer_ref[...] = jnp.zeros_like(mixer_ref)

    def out_copy(step):
        return mesh_copy(bo_ref.at[targets[step]], bout_ref.at[:, part], bo_sem.at[0, step],
                         bo_sem.at[1, step], {"ctx": targets[step]})

    block = 256

    def product(q):
        grads = [ref[q * per:(q + 1) * per].reshape(per * tile, full)
                 for ref in (gq_ref, gk_ref, gv_ref)]

        def columns(index, carry):
            cols = pl.ds(pl.multiple_of(index * block, block), block)
            terms = dot_turned(grads[0], wq_ref[cols, :])
            terms += dot_turned(grads[1], wk_ref[cols, :])
            terms += dot_turned(grads[2], wv_ref[cols, :])
            terms = terms.astype(BF16)
            for p in range(per):
                for z in range(lines):
                    own_ref[q, z, p * strip:(p + 1) * strip, cols] = (
                        terms[p * tile + z * strip:p * tile + (z + 1) * strip])
            return carry

        lax.fori_loop(0, model // block, columns, 0)

    rows = wsum_ref.shape[1]
    narrow = 128

    def weight_term(kind):
        rows_ref = branch_ref if kind == 3 else normed_ref
        grad_ref = (gq_ref, gk_ref, gv_ref, grouped_ref)[kind]

        def columns(index, carry):
            cols = pl.ds(pl.multiple_of(index * narrow, narrow), narrow)
            term = jnp.zeros((narrow, full), F32)
            for s in range(0, slots, 2):
                left = rows_ref[s:s + 2, :, cols].reshape(2 * tile, narrow)
                grad = grad_ref[s:s + 2].reshape(2 * tile, full)
                term += dot(jnp.transpose(left), grad)
            wloc_ref[kind, cols] = term.astype(BF16)
            return carry

        lax.fori_loop(0, model // narrow, columns, 0)

    def share(index, which):
        return pl.ds(pl.multiple_of((index * 2 + which) * rows, 16), rows)

    def weights_out(index):
        return mesh_copy(wloc_ref.at[:, share(index, other_core)], wr1_ref.at[:, index],
                         w1_sem.at[0, index], w1_sem.at[1, index], sibling)

    def weights_send(step):
        index = others[step]
        return mesh_copy(wloc_ref.at[:, share(index, core)], wr2_ref.at[step], w2_sem.at[0, step],
                         w2_sem.at[1, step], group_device(index))

    def weights_cross():
        for index in range(groups):
            weights_out(index).wait()

        def add(index, carry):
            for k in range(4):
                wloc_ref[k, share(index, core)] = (
                    wloc_ref[k, share(index, core)].astype(F32) + wr1_ref[k, index].astype(F32)
                ).astype(BF16)
            return carry

        lax.fori_loop(0, groups, add, 0)

    def weights_finish():
        for step in range(groups - 1):
            weights_send(step).wait()
        for k in range(4):
            total = wloc_ref[k, share(me, core)].astype(F32)
            for step in range(groups - 1):
                total = total + wr2_ref[step, k].astype(F32)
            wsum_ref[k] = total

    def close(q):
        line.total(q, acc_ref)
        grad = acc_ref[...]
        x = inputs_ref[q * per:(q + 1) * per].reshape(per * strip, model).astype(F32)
        scale = lax.rsqrt(jnp.mean(x * x, axis=1, keepdims=True) + EPSILON)
        mixer_ref[...] += jnp.sum((grad * (x * scale)).reshape(per * strip // 8, 8, model), axis=0)
        up = grad * gain_ref[...]
        result = (gh_ref[q * per:(q + 1) * per].reshape(per * strip, model) + scale * up
                  - x * (scale * scale * scale * jnp.mean(up * x, axis=1, keepdims=True)))
        ig_ref[q * per:(q + 1) * per] = result.astype(BF16).reshape(per, strip, model)

    for slot in range(chunks + lines - 1):
        if slot < chunks:
            product(slot)
        for t in range(lines - 1):
            if 0 <= slot - t < chunks:
                line.step(slot - t, t)
        if slot == 0:
            for step in range(parts - 1):
                out_copy(step).start()
            bout_ref[:, part] = bo_ref[part]
        if slot < 4:
            weight_term(slot)
            if slot == 3:
                for index in range(groups):
                    weights_out(index).start()
        if slot == 4:
            weights_cross()
        if slot == 5:
            for step in range(groups - 1):
                weights_send(step).start()
        if slot - lines + 1 >= 0:
            close(slot - lines + 1)
    first_row = lax.broadcasted_iota(jnp.int32, small_ref.shape, 0) == 0
    mixer = jnp.broadcast_to(jnp.sum(mixer_ref[...], axis=0, keepdims=True), small_ref.shape)
    va_ref[0] = jnp.where(first_row, mixer, small_ref[...])
    for q in range(chunks):
        line.drain(q)
    for step in range(parts - 1):
        out_copy(step).wait()
    swap = mesh_copy(va_ref.at[0], va_ref.at[1], va_sem.at[0], va_sem.at[1], sibling)
    swap.start()
    weights_finish()
    swap.wait()
    vb_ref[me] = va_ref[0] + va_ref[1]

    def group_copy(source, target, sem):
        return mesh_copy(vb_ref.at[source], vb_ref.at[source], vb_sem.at[0, sem],
                         vb_sem.at[1, source], group_device(target))

    for step, index in enumerate(others):
        group_copy(me, index, step).start()
    for step, index in enumerate(others):
        group_copy(index, index, step).wait_recv()
    total = vb_ref[0]
    for index in range(1, groups):
        total = total + vb_ref[index]
    vc_ref[place] = total
    v2_ref[...] = total

    def line_copy(source, target, sem):
        return mesh_copy(vc_ref.at[source], vc_ref.at[source], vc_sem.at[0, sem],
                         vc_sem.at[1, source], {"head": target})

    for step, index in enumerate(line_others):
        line_copy(place, index, step).start()
    for step, index in enumerate(line_others):
        line_copy(index, index, step).wait_recv()
    total = vc_ref[0]
    for index in range(1, lines):
        total = total + vc_ref[index]
    row_index = lax.broadcasted_iota(jnp.int32, total.shape, 0)
    vec_ref[...] = jnp.where(row_index < 2, total, v2_ref[...])
    for step, index in enumerate(others):
        group_copy(me, index, step).wait_send()
    for step, index in enumerate(line_others):
        line_copy(place, index, step).wait_send()


def finish(dims, groups, lines, chunks, rows, *operands):
    slots, parts, heads, tile, width, strip = dims
    full = heads * width
    model = operands[6].shape[-1]
    pairs = operands[-1].shape[1]
    return pl.pallas_call(
        partial(finish_kernel, dims, groups, lines),
        out_shape=(
            jax.ShapeDtypeStruct((slots, strip, model), BF16),
            jax.ShapeDtypeStruct((4, rows, full), F32),
            jax.ShapeDtypeStruct((8, model), F32),
            jax.ShapeDtypeStruct((pairs, parts, strip, model), BF16),
        ),
        in_specs=specs(14, 0),
        out_specs=specs(4, 0),
        scratch_shapes=line_scratch(chunks, lines, slots // chunks * strip, model) + [
            pltpu.VMEM((4, model, full), BF16),
            pltpu.VMEM((4, groups, rows, full), BF16),
            pltpu.VMEM((groups - 1, 4, rows, full), BF16),
            pltpu.VMEM((8, model), F32),
            pltpu.VMEM((2, 8, model), F32),
            pltpu.VMEM((groups, 8, model), F32),
            pltpu.VMEM((lines, 8, model), F32),
            pltpu.VMEM((8, model), F32),
            pltpu.SemaphoreType.DMA((2, groups)),
            pltpu.SemaphoreType.DMA((2, groups - 1)),
            pltpu.SemaphoreType.DMA((2,)),
            pltpu.SemaphoreType.DMA((2, groups)),
            pltpu.SemaphoreType.DMA((2, lines)),
            pltpu.SemaphoreType.DMA((2, parts - 1)),
        ],
        compiler_params=pltpu.CompilerParams(
            vmem_limit_bytes=60 << 20, collective_id=2, has_side_effects=True),
        cost_estimate=pl.CostEstimate(
            flops=8_000_000_000, bytes_accessed=24_000_000, transcendentals=0),
        name="finish",
    )(*operands)


class LineGather:
    def __init__(self, axis, size, view, sems):
        self.axis, self.size, self.view, self.sems = axis, size, view, sems
        self.me = lax.axis_index(axis)

    def copy(self, q, t, side):
        source = jnp.clip(self.me - t if side == 0 else self.me + t, 0, self.size - 1)
        neighbour = jnp.clip(self.me + (1 if side == 0 else -1), 0, self.size - 1)
        return mesh_copy(
            self.view(q, source), self.view(q, source), self.sems.at[0, side, q, t],
            self.sems.at[1, side, q, source], {self.axis: neighbour})

    def rank(self, side):
        return self.me if side == 0 else self.size - 1 - self.me

    def step(self, q, t):
        for side in range(2):
            rank = self.rank(side)

            if t > 0:
                @pl.when(rank >= t)
                def _():
                    self.copy(q, t, side).wait_recv()

            if t < self.size - 1:
                @pl.when((rank >= t) & (rank < self.size - 1))
                def _():
                    self.copy(q, t, side).start()

    def drain(self, q):
        for t in range(self.size - 1):
            for side in range(2):
                rank = self.rank(side)

                @pl.when((rank >= t) & (rank < self.size - 1))
                def _():
                    self.copy(q, t, side).wait_send()


def open_kernel(dims, lines, chunks, x_ref, gain_ref, wq_ref, wk_ref, wv_ref, cosn_ref, sinn_ref,
                cot_ref, normed_ref, q_ref, kv_ref, cout_ref,
                line_sem, c_sem, sib_sem, far_sem, fwd_sem):
    slots, parts, heads, tile, width, strip = dims
    half = width // 2
    per = slots // chunks
    model = x_ref.shape[-1]
    part = lax.axis_index("ctx")
    place = lax.axis_index("head")
    core = part % 2
    y = part // 2
    sibling = {"ctx": y * 2 + 1 - core}
    across = {"ctx": (1 - y) * 2 + core}
    far = (1 - y) * 2 + core
    far_other = (1 - y) * 2 + 1 - core
    near = y * 2 + 1 - core
    targets = [lax.rem(part + step, parts) for step in range(1, parts)]
    greet([{"ctx": target} for target in targets]
          + [{"head": lax.rem(place + step, lines)} for step in range(1, lines)])
    line = LineGather(
        "head", lines, lambda q, s: normed_ref.at[pl.ds(q * per, per), s], line_sem)

    def norm(q):
        x = x_ref[q * per:(q + 1) * per].reshape(per * strip, model).astype(F32)
        scale = lax.rsqrt(jnp.mean(x * x, axis=1, keepdims=True) + EPSILON)
        low = (x * scale * gain_ref[...]).astype(BF16).reshape(per, strip, model)
        for p in range(per):
            normed_ref[q * per + p, place] = low[p]

    def cot_copy(step):
        return mesh_copy(cot_ref.at[:, targets[step]], cout_ref.at[part], c_sem.at[0, step],
                         c_sem.at[1, step], {"ctx": targets[step]})

    def chunk_view(source, q):
        return kv_ref.at[source, pl.ds(q * per, per)]

    def to_sibling(q):
        return mesh_copy(chunk_view(part, q), chunk_view(part, q), sib_sem.at[0, q],
                         sib_sem.at[1, q], sibling)

    def from_sibling(q):
        return mesh_copy(chunk_view(near, q), chunk_view(near, q), sib_sem.at[0, q],
                         sib_sem.at[1, q], sibling)

    def to_far(q):
        return mesh_copy(chunk_view(part, q), chunk_view(part, q), far_sem.at[0, q],
                         far_sem.at[1, q], across)

    def from_far(q):
        return mesh_copy(chunk_view(far, q), chunk_view(far, q), far_sem.at[0, q],
                         far_sem.at[1, q], across)

    def forward(q):
        return mesh_copy(chunk_view(far, q), chunk_view(far, q), fwd_sem.at[0, q],
                         fwd_sem.at[1, q], sibling)

    def forwarded(q):
        return mesh_copy(chunk_view(far_other, q), chunk_view(far_other, q), fwd_sem.at[0, q],
                         fwd_sem.at[1, q], sibling)

    def project(q):
        rows = normed_ref[q * per:(q + 1) * per].reshape(per * tile, model)
        for kind, weight_ref in ((1, wv_ref), (0, wk_ref), (2, wq_ref)):
            result = dot(rows, weight_ref[...])
            for p in range(per):
                at = q * per + p
                for h in range(heads):
                    lanes = slice(h * width, (h + 1) * width)
                    piece = result[p * tile:(p + 1) * tile, lanes]
                    if kind != 1:
                        piece = piece * cosn_ref[at] - swap_halves(piece, half) * sinn_ref[at]
                    if kind == 2:
                        q_ref[at, :, lanes] = piece.astype(BF16)
                    else:
                        kv_ref[part, at, kind, :, lanes] = piece.astype(BF16)

    for slot in range(chunks + lines - 1):
        if slot < chunks:
            norm(slot)
        for t in range(lines):
            if 0 <= slot - t < chunks:
                line.step(slot - t, t)
        if slot == 0:
            for step in range(parts - 1):
                cot_copy(step).start()
            cout_ref[part] = cot_ref[:, part]
        q = slot - lines + 1
        if q >= 0:
            project(q)
            to_far(q).start()
            to_sibling(q).start()
        if q >= 1:
            from_far(q - 1).wait_recv()
            forward(q - 1).start()
    from_far(chunks - 1).wait_recv()
    forward(chunks - 1).start()
    for step in range(parts - 1):
        cot_copy(step).wait()
    for q in range(chunks):
        line.drain(q)
        from_sibling(q).wait_recv()
        to_sibling(q).wait_send()
        to_far(q).wait_send()
    for q in range(chunks):
        forwarded(q).wait_recv()
        forward(q).wait_send()


def open_rows(dims, lines, chunks, *operands):
    slots, parts, heads, tile, width, strip = dims
    full = heads * width
    model = operands[0].shape[-1]
    pairs = operands[-1].shape[0]
    return pl.pallas_call(
        partial(open_kernel, dims, lines, chunks),
        out_shape=(
            jax.ShapeDtypeStruct((slots, lines, strip, model), BF16),
            jax.ShapeDtypeStruct((slots, tile, full), BF16),
            jax.ShapeDtypeStruct((parts, slots, 2, tile, full), BF16),
            jax.ShapeDtypeStruct((parts, pairs, strip, model), BF16),
        ),
        in_specs=specs(8, 0),
        out_specs=specs(4, 0),
        scratch_shapes=[
            pltpu.SemaphoreType.DMA((2, 2, chunks, lines)),
            pltpu.SemaphoreType.DMA((2, parts - 1)),
            pltpu.SemaphoreType.DMA((2, chunks)),
            pltpu.SemaphoreType.DMA((2, chunks)),
            pltpu.SemaphoreType.DMA((2, chunks)),
        ],
        compiler_params=pltpu.CompilerParams(
            vmem_limit_bytes=60 << 20, collective_id=3, has_side_effects=True),
        cost_estimate=pl.CostEstimate(
            flops=4_000_000_000, bytes_accessed=16_000_000, transcendentals=0),
        name="open_rows",
    )(*operands)


def greet_line(axis, size):
    place = lax.axis_index(axis)
    greet([{axis: lax.rem(place + step, size)} for step in range(1, size)])


def scatter_terms(own_ref, q, cols, terms, dims, lines):
    slots, parts, heads, tile, width, strip = dims
    for p in range(terms.shape[0] // tile):
        for z in range(lines):
            own_ref[q, z, p * strip:(p + 1) * strip, cols] = (
                terms[p * tile + z * strip:p * tile + (z + 1) * strip])


def line_turn(lines, chunks, summed, gathered, before, between):
    for slot in range(chunks + 2 * (lines - 1)):
        if slot < chunks:
            before(slot)
        for t in range(lines - 1):
            if 0 <= slot - t < chunks:
                summed.step(slot - t, t)
        q = slot - lines + 1
        if 0 <= q < chunks:
            between(q)
        for t in range(lines):
            if 0 <= q - t < chunks:
                gathered.step(q - t, t)
    for q in range(chunks):
        summed.drain(q)
        gathered.drain(q)


def feed_open_kernel(dims, lines, chunks, grouped_ref, wo_ref, inputs_ref, gain_ref, grad_ref,
                     down_ref, hidden_ref, rows_ref, gact_ref,
                     own_ref, left_ref, right_ref, acc_ref, line_sem, gather_sem):
    slots, parts, heads, tile, width, strip = dims
    full = heads * width
    per = slots // chunks
    model = inputs_ref.shape[-1]
    units = down_ref.shape[0]
    block = 256
    place = lax.axis_index("head")
    greet_line("head", lines)
    summed = LineSum("head", lines, own_ref, left_ref, right_ref, line_sem)
    gathered = LineGather(
        "head", lines, lambda q, s: rows_ref.at[pl.ds(q * per, per), s], gather_sem)

    def before(q):
        left = grouped_ref[q * per:(q + 1) * per].reshape(per * tile, full)

        def columns(index, carry):
            cols = pl.ds(pl.multiple_of(index * block, block), block)
            scatter_terms(own_ref, q, cols, dot(left, wo_ref[:, cols]).astype(BF16), dims, lines)
            return carry

        lax.fori_loop(0, model // block, columns, 0)

    def between(q):
        summed.total(q, acc_ref)
        hidden = inputs_ref[q * per:(q + 1) * per].reshape(per * strip, model).astype(F32)
        hidden = hidden + acc_ref[...]
        hidden_ref[q * per:(q + 1) * per] = hidden.reshape(per, strip, model)
        scale = lax.rsqrt(jnp.mean(hidden * hidden, axis=1, keepdims=True) + EPSILON)
        low = (hidden * scale * gain_ref[...]).astype(BF16).reshape(per, strip, model)
        for p in range(per):
            rows_ref[q * per + p, place] = low[p]

    def extra(q):
        grads = grad_ref[q * per:(q + 1) * per].reshape(per * tile, model)

        def columns(index, carry):
            cols = pl.ds(pl.multiple_of(index * block, block), block)
            result = dot_turned(grads, down_ref[cols, :])
            gact_ref[q * per:(q + 1) * per, :, cols] = result.reshape(per, tile, block)
            return carry

        lax.fori_loop(0, units // block, columns, 0)

    def before_all(q):
        before(q)
        if q > 0:
            extra(q - 1)
        if q == chunks - 1:
            extra(q)

    line_turn(lines, chunks, summed, gathered, before_all, between)


def feed_open(dims, lines, chunks, *operands):
    slots, parts, heads, tile, width, strip = dims
    model, units = operands[1].shape[1], operands[5].shape[0]
    return pl.pallas_call(
        partial(feed_open_kernel, dims, lines, chunks),
        out_shape=(
            jax.ShapeDtypeStruct((slots, strip, model), F32),
            jax.ShapeDtypeStruct((slots, lines, strip, model), BF16),
            jax.ShapeDtypeStruct((slots, tile, units), F32),
        ),
        in_specs=specs(6, 0),
        out_specs=specs(3, 0),
        scratch_shapes=line_scratch(chunks, lines, slots // chunks * strip, model) + [
            pltpu.SemaphoreType.DMA((2, 2, chunks, lines)),
        ],
        compiler_params=pltpu.CompilerParams(
            vmem_limit_bytes=60 << 20, collective_id=4, has_side_effects=True),
        cost_estimate=pl.CostEstimate(
            flops=4_000_000_000, bytes_accessed=20_000_000, transcendentals=0),
        name="feed_open",
    )(*operands)


def feed_close_kernel(dims, lines, chunks, gg_ref, gu_ref, wg_ref, wu_ref, rows_ref, grad_ref,
                      act_ref, hidden_ref, cot_ref, gain_ref,
                      gh_ref, branch_ref, terms_ref, part_ref,
                      own_ref, left_ref, right_ref, acc_ref, line_sem, gather_sem):
    slots, parts, heads, tile, width, strip = dims
    per = slots // chunks
    model = cot_ref.shape[-1]
    units = act_ref.shape[-1]
    block, narrow = 256, 128
    place = lax.axis_index("head")
    greet_line("head", lines)
    summed = LineSum("head", lines, own_ref, left_ref, right_ref, line_sem)
    gathered = LineGather(
        "head", lines, lambda q, s: branch_ref.at[pl.ds(q * per, per), s], gather_sem)
    part_ref[...] = jnp.zeros_like(part_ref)

    def weight_term(kind):
        left_rows = grad_ref if kind == 2 else rows_ref
        right_rows = (gg_ref, gu_ref, act_ref)[kind]

        def columns(index, carry):
            cols = pl.ds(pl.multiple_of(index * narrow, narrow), narrow)
            term = jnp.zeros((narrow, units), F32)
            for s in range(0, slots, 2):
                left = left_rows[s:s + 2, :, cols].reshape(2 * tile, narrow)
                term += dot(jnp.transpose(left), right_rows[s:s + 2].reshape(2 * tile, units))
            terms_ref[kind, cols] = term.astype(BF16)
            return carry

        lax.fori_loop(0, model // narrow, columns, 0)

    def before(q):
        gate = gg_ref[q * per:(q + 1) * per].reshape(per * tile, units)
        up = gu_ref[q * per:(q + 1) * per].reshape(per * tile, units)

        def columns(index, carry):
            cols = pl.ds(pl.multiple_of(index * block, block), block)
            terms = dot_turned(gate, wg_ref[cols, :]) + dot_turned(up, wu_ref[cols, :])
            scatter_terms(own_ref, q, cols, terms.astype(BF16), dims, lines)
            return carry

        lax.fori_loop(0, model // block, columns, 0)
        if q > 0:
            weight_term(q - 1)

    def between(q):
        summed.total(q, acc_ref)
        grad = acc_ref[...]
        hidden = hidden_ref[q * per:(q + 1) * per].reshape(per * strip, model)
        scale = lax.rsqrt(jnp.mean(hidden * hidden, axis=1, keepdims=True) + EPSILON)
        part_ref[...] += jnp.sum(
            (grad * (hidden * scale)).reshape(per * strip // 8, 8, model), axis=0)
        up = grad * gain_ref[...]
        result = (cot_ref[q * per:(q + 1) * per].reshape(per * strip, model).astype(F32)
                  + scale * up
                  - hidden * (scale * scale * scale * jnp.mean(up * hidden, axis=1, keepdims=True)))
        gh_ref[q * per:(q + 1) * per] = result.reshape(per, strip, model)
        low = result.astype(BF16).reshape(per, strip, model)
        for p in range(per):
            branch_ref[q * per + p, place] = low[p]

    line_turn(lines, chunks, summed, gathered, before, between)


def feed_close(dims, lines, chunks, *operands):
    slots, parts, heads, tile, width, strip = dims
    model, units = operands[8].shape[-1], operands[6].shape[-1]
    return pl.pallas_call(
        partial(feed_close_kernel, dims, lines, chunks),
        out_shape=(
            jax.ShapeDtypeStruct((slots, strip, model), F32),
            jax.ShapeDtypeStruct((slots, lines, strip, model), BF16),
            jax.ShapeDtypeStruct((3, model, units), BF16),
            jax.ShapeDtypeStruct((8, model), F32),
        ),
        in_specs=specs(10, 0),
        out_specs=specs(4, 0),
        scratch_shapes=line_scratch(chunks, lines, slots // chunks * strip, model) + [
            pltpu.SemaphoreType.DMA((2, 2, chunks, lines)),
        ],
        compiler_params=pltpu.CompilerParams(
            vmem_limit_bytes=60 << 20, collective_id=5, has_side_effects=True),
        cost_estimate=pl.CostEstimate(
            flops=16_000_000_000, bytes_accessed=40_000_000, transcendentals=0),
        name="feed_close",
    )(*operands)


def per_device(
    inputs,
    block_order,
    mixer_gain,
    query_weight,
    key_weight,
    value_weight,
    lambda_qone,
    lambda_kone,
    lambda_qtwo,
    lambda_ktwo,
    group_gain,
    output_weight,
    feed_gain,
    gate_weight,
    up_weight,
    down_weight,
    cotangent,
):
    seq_count, pair_count, short_rows, model_width = inputs.shape
    assert seq_count == 1
    parts = lax.axis_size("ctx")
    head_total = lax.axis_size("head")
    part = lax.axis_index("ctx")
    head_place = lax.axis_index("head")
    block_len = short_rows * head_total
    slots = block_order.shape[1]
    heads_here, head_dim = lambda_qone.shape
    qwidth = query_weight.shape[1]
    width = 2 * head_dim
    tile = block_len // parts
    strip = short_rows // parts
    dims = (slots, parts, heads_here, tile, width, strip)
    row_count = slots * tile
    order = block_order.reshape(slots)
    slot_of = jnp.argsort(order).astype(jnp.int32)
    index = jnp.arange(tile, dtype=jnp.int32)
    row_offsets = (index // strip) * short_rows + part * strip + index % strip
    own_places = jnp.arange(slots, dtype=jnp.int32)[:, None] * block_len + row_offsets[None, :]
    groups = lax.axis_size("dp") * parts // 2
    quarter = head_dim // 2
    frequency = THETA ** (-jnp.arange(quarter, dtype=jnp.float32) / quarter)
    angles = own_places.astype(F32)[:, None, :] * frequency[None, :, None]
    cos_turned, sin_turned = jnp.cos(angles), jnp.sin(angles)
    cos_rows = jnp.tile(cos_turned.transpose(0, 2, 1), (1, 1, 4))
    sin_rows = jnp.tile(sin_turned.transpose(0, 2, 1), (1, 1, 4))
    lane = jnp.arange(width)
    sin_rows = jnp.where(lane % head_dim < quarter, sin_rows, -sin_rows)
    tables = (cos_turned, sin_turned, cos_rows, sin_rows)
    lambda_one = jnp.exp(jnp.sum(lambda_qone * lambda_kone, axis=-1))
    lambda_two = jnp.exp(jnp.sum(lambda_qtwo * lambda_ktwo, axis=-1))
    lambda_head = lambda_one - lambda_two + LAMBDA_INIT
    split_shape = (slots, tile, heads_here, 2, head_dim)
    rows_shape = (slots, tile, model_width)

    def spread(rows):
        cut = rows.reshape(pair_count, parts, strip, model_width).transpose(1, 0, 2, 3)
        cut = lax.all_to_all(cut, "ctx", 0, 0, tiled=True)
        return jnp.take(cut.reshape(slots, strip, model_width), slot_of, axis=0)

    def unspread(rows):
        cut = jnp.take(rows, order, axis=0).reshape(parts, pair_count, strip, model_width)
        cut = lax.all_to_all(cut, "ctx", 0, 0, tiled=True)
        return cut.transpose(1, 0, 2, 3).reshape(1, pair_count, short_rows, model_width)

    inputs_here = spread(inputs)
    tokens = inputs_here.astype(jnp.float32)
    part_shape = (slots, tile, qwidth)
    cut_shape = (pair_count, parts, strip, model_width)
    normed_rows, queries, kv_all, cotangent_slots = open_rows(
        dims, head_total, 4, inputs_here, mixer_gain.reshape(1, model_width), query_weight,
        key_weight, value_weight, cos_rows, sin_rows, cotangent.reshape(cut_shape))
    cotangent_here = jnp.take(
        cotangent_slots.reshape(slots, strip, model_width), slot_of, axis=0)
    grad_rows = lax.all_gather(cotangent_here, "head", axis=1, tiled=True)
    part_arr = part.reshape(1).astype(jnp.int32)
    gain_col = group_gain.reshape(qwidth, 1)
    grouped, mixed, second, lse = attend(
        dims, part_arr, lambda_head, queries, kv_all,
        gain_col)
    grouped, grad_rows = lax.optimization_barrier((grouped, grad_rows))
    hidden, feed_rows, grad_activ = feed_open(
        dims, head_total, 4, grouped, output_weight, inputs_here,
        feed_gain.reshape(1, model_width), grad_rows, down_weight)
    feed_rows = feed_rows.reshape(row_count, model_width)
    grad_activ = grad_activ.reshape(row_count, grad_activ.shape[-1])
    gate_vals = jnp.dot(feed_rows, gate_weight, preferred_element_type=jnp.float32)
    up_vals = jnp.dot(feed_rows, up_weight, preferred_element_type=jnp.float32)
    gate_sigmoid = jax.nn.sigmoid(gate_vals)
    silu_gate = gate_vals * gate_sigmoid
    activation = (silu_gate * up_vals).astype(jnp.bfloat16)
    grad_gate = (
        grad_activ * up_vals * gate_sigmoid * (1.0 + gate_vals * (1.0 - gate_sigmoid))
    ).astype(jnp.bfloat16)
    grad_up = (grad_activ * silu_gate).astype(jnp.bfloat16)
    unit_shape = (slots, tile, activation.shape[-1])
    grad_hidden, branch_rows, wgrads, feed_part = feed_close(
        dims, head_total, 4, grad_gate.reshape(unit_shape), grad_up.reshape(unit_shape),
        gate_weight, up_weight, feed_rows.reshape(slots, tile, model_width), grad_rows,
        activation.reshape(unit_shape), hidden, cotangent_here, feed_gain.reshape(1, model_width))
    feed_part = jnp.sum(feed_part, axis=0)
    branch_rows = branch_rows.reshape(row_count, model_width)
    feed_terms = jnp.dot(activation, down_weight, preferred_element_type=jnp.float32).reshape(
        rows_shape
    )
    branch_rows, feed_terms = lax.optimization_barrier((branch_rows, feed_terms.astype(BF16)))
    feed_sum = lax.psum_scatter(feed_terms, "head", scatter_dimension=1, tiled=True)
    grad_grouped = contract_cols(output_weight, branch_rows)
    shares = lax.axis_size("dp") * parts
    wgrads = wgrads.reshape(3, groups, 2, model_width // shares, wgrads.shape[-1])
    grad_query, grad_key, grad_value, group_part, lambda_part, feed_sums = attend_back(
        dims, groups, lambda_head, queries, kv_all,
        grad_grouped, gain_col, mixed, second, lse, tables, wgrads)
    feed_sum, grad_query = lax.optimization_barrier((feed_sum, grad_query))
    block_out = (hidden + feed_sum.astype(F32)).astype(BF16)
    group_part = jnp.sum(group_part, axis=1) * SHRINK
    lambda_part = jnp.sum(lambda_part, axis=(1, 2))
    third = jnp.pad(
        jnp.concatenate([group_part, lambda_part]), (0, model_width - qwidth - heads_here))
    small = jnp.pad(jnp.stack([jnp.zeros_like(feed_part), feed_part, third]), ((0, 5), (0, 0)))
    grad_rows_shape = (slots, tile, model_width)
    block_slots = jnp.take(block_out, order, axis=0).reshape(
        parts, pair_count, strip, model_width)
    input_grad, attn_sums, vectors, block_out = finish(
        dims, groups, head_total, 4, model_width // shares, grad_query, grad_key, grad_value,
        query_weight, key_weight, value_weight, normed_rows.reshape(grad_rows_shape),
        branch_rows.reshape(grad_rows_shape), grouped.reshape(part_shape), inputs_here,
        grad_hidden, mixer_gain.reshape(1, model_width), small, block_slots)
    block_out = block_out.reshape(inputs.shape)
    input_grad = unspread(input_grad).astype(F32)
    group_grad = vectors[2, :qwidth]
    lambda_grad = vectors[2, qwidth:qwidth + heads_here]
    qone_grad = (lambda_grad * lambda_one)[:, None] * lambda_kone
    kone_grad = (lambda_grad * lambda_one)[:, None] * lambda_qone
    qtwo_grad = -(lambda_grad * lambda_two)[:, None] * lambda_ktwo
    ktwo_grad = -(lambda_grad * lambda_two)[:, None] * lambda_qtwo
    return (
        block_out,
        input_grad,
        vectors[0],
        attn_sums[0],
        attn_sums[1],
        attn_sums[2],
        qone_grad,
        kone_grad,
        qtwo_grad,
        ktwo_grad,
        group_grad,
        attn_sums[3].T,
        vectors[1],
        feed_sums[0],
        feed_sums[1],
        feed_sums[2].T,
    )


def solution(mesh):
    return jax.shard_map(
        per_device,
        mesh=mesh,
        in_specs=(
            P("dp", "ctx", "head", None),
            P("dp", None),
            P(),
            P(None, "head"),
            P(None, "head"),
            P(None, "head"),
            P("head", None),
            P("head", None),
            P("head", None),
            P("head", None),
            P("head"),
            P("head", None),
            P(),
            P(None, "head"),
            P(None, "head"),
            P("head", None),
            P("dp", "ctx", "head", None),
        ),
        out_specs=(
            P("dp", "ctx", "head", None),
            P("dp", "ctx", "head", None),
            P(),
            P(("dp", "ctx"), "head"),
            P(("dp", "ctx"), "head"),
            P(("dp", "ctx"), "head"),
            P("head", None),
            P("head", None),
            P("head", None),
            P("head", None),
            P("head"),
            P("head", ("dp", "ctx")),
            P(),
            P(("dp", "ctx"), "head"),
            P(("dp", "ctx"), "head"),
            P("head", ("dp", "ctx")),
        ),
        check_vma=False,
    )
```

```python
from functools import partial
import math

import jax
import jax.numpy as jnp
from jax import lax
from jax.experimental import pallas as pl
from jax.experimental.pallas import tpu as pltpu
from jax.sharding import PartitionSpec as P

EPSILON = 1e-05
LAMBDA_INIT = 0.8 - 0.6 * math.exp(-0.3 * 12)
SHRINK = 1.0 - LAMBDA_INIT
THETA = 10000.0
NEGATIVE = -1e30
F32 = jnp.float32
BF16 = jnp.bfloat16


def rms_scale(value_rows):
    return lax.rsqrt(jnp.mean(value_rows * value_rows, axis=-1, keepdims=True) + EPSILON)


def norm_back(grad_in, value_rows, scale, gain):
    upstream = grad_in * gain
    return scale * upstream - value_rows * scale**3 * jnp.mean(
        upstream * value_rows, axis=-1, keepdims=True
    )


def rotate(tensor, places, direction):
    half_dim = tensor.shape[-1] // 2
    frequency = THETA ** (-jnp.arange(half_dim, dtype=jnp.float32) / half_dim)
    angles = places.astype(jnp.float32)[..., None] * frequency
    angles = angles.reshape(places.shape + (1,) * (tensor.ndim - places.ndim - 1) + (half_dim,))
    cosine = jnp.cos(angles)
    sine_part = jnp.sin(angles) * direction
    leading = tensor[..., :half_dim]
    trailing = tensor[..., half_dim:]
    return jnp.concatenate(
        [leading * cosine - trailing * sine_part, leading * sine_part + trailing * cosine], axis=-1
    )


def contract_rows(left, right):
    return lax.dot_general(
        left, right, (((0,), (0,)), ((), ())), preferred_element_type=jnp.float32
    )


def contract_cols(left, right):
    return lax.dot_general(
        left, right, (((1,), (1,)), ((), ())), preferred_element_type=jnp.float32
    )


def dot(left, right):
    return lax.dot_general(left, right, (((1,), (0,)), ((), ())), preferred_element_type=F32)


def offsets_of(part, parts, strip, axis, shape):
    index = lax.broadcasted_iota(jnp.int32, shape, axis)
    return (index // strip) * (parts * strip) + part * strip + index % strip


def block_diag_cols(turned, half, lanes):
    row = lax.broadcasted_iota(jnp.int32, (turned.shape[0], lanes), 0)
    zero = jnp.zeros_like(turned)
    return jnp.concatenate(
        [jnp.where(row < half, turned, zero), jnp.where(row >= half, turned, zero)], axis=1
    )


def attend_kernel(dims, part_ref, lam_ref, q_ref, kv_ref, gain_ref,
                  grouped_ref, mixed_ref, second_ref, lse_ref, vt_ref, qbd_ref, acc_ref):
    slots, parts, heads, tile, width, strip = dims
    half = width // 2
    cols = 2 * tile

    def turn(slot, carry):
        for h in range(heads):
            for c in range(parts):
                vt_ref[h, slot, :, c * tile:(c + 1) * tile] = jnp.transpose(
                    kv_ref[c, slot, 1, :, h * width:(h + 1) * width])
        return carry

    lax.fori_loop(0, slots, turn, 0)
    query_off = offsets_of(part_ref[0], parts, strip, 1, (1, tile))
    query_off = jnp.concatenate([query_off, query_off], axis=1)

    def one_block(slot, diag, state):
        out = []
        for h in range(heads):
            peak, total = state[2 * h], state[2 * h + 1]
            scores = []
            for c in range(parts):
                s = dot(kv_ref[c, slot, 0, :, h * width:(h + 1) * width], qbd_ref[h])
                if diag:
                    key_off = offsets_of(c, parts, strip, 0, (tile, 1))
                    s = jnp.where(key_off <= query_off, s, NEGATIVE)
                scores.append(s)
            top = scores[0]
            for s in scores[1:]:
                top = jnp.maximum(top, s)
            higher = jnp.maximum(peak, jnp.max(top, axis=0, keepdims=True))
            keep = jnp.exp(peak - higher)
            weights = [jnp.exp(s - higher) for s in scores]
            added = weights[0]
            for w in weights[1:]:
                added = added + w
            total = total * keep + jnp.sum(added, axis=0, keepdims=True)
            low = jnp.concatenate([w.astype(BF16) for w in weights], axis=0)
            acc_ref[h] = acc_ref[h] * keep + dot(vt_ref[h, slot], low)
            out += [higher, total]
        return tuple(out)

    def one_place(place, carry):
        for h in range(heads):
            turned = jnp.transpose(q_ref[place, :, h * width:(h + 1) * width])
            turned = turned * jnp.asarray(half ** -0.5, turned.dtype)
            qbd_ref[h] = block_diag_cols(turned, half, tile)
            acc_ref[h] = jnp.zeros((width, cols), F32)
        state = (jnp.full((1, cols), NEGATIVE, F32), jnp.zeros((1, cols), F32)) * heads
        state = one_block(place, True, state)
        state = lax.fori_loop(
            0, place, lambda j, st: one_block(j, False, st), state)
        for h in range(heads):
            peak, total = state[2 * h], state[2 * h + 1]
            result = acc_ref[h] / total
            second = result[:, tile:]
            mixed = result[:, :tile] - lam_ref[h] * second
            scale = lax.rsqrt(jnp.mean(mixed * mixed, axis=0, keepdims=True) + EPSILON)
            gain = gain_ref[h * width:(h + 1) * width, :] * SHRINK
            grouped = (mixed * scale * gain).astype(BF16)
            grouped_ref[place, :, h * width:(h + 1) * width] = jnp.transpose(grouped)
            mixed_ref[place, h] = mixed
            second_ref[place, h] = second
            lse_ref[place, h] = peak + jnp.log(total)
        return carry

    lax.fori_loop(0, slots, one_place, 0)


def mesh_copy(src, dst, send_sem, recv_sem, device):
    return pltpu.make_async_remote_copy(
        src_ref=src, dst_ref=dst, send_sem=send_sem, recv_sem=recv_sem,
        device_id=device, device_id_type=pl.DeviceIdType.MESH)


def greet(devices):
    barrier = pltpu.get_barrier_semaphore()
    for device in devices:
        pl.semaphore_signal(
            barrier, inc=1, device_id=device, device_id_type=pl.DeviceIdType.MESH)
    pl.semaphore_wait(barrier, len(devices))


def swap_halves(rows, half):
    quarter = half // 2
    lane = lax.broadcasted_iota(jnp.int32, rows.shape, 1)
    back = pltpu.roll(rows, rows.shape[1] - quarter, 1)
    ahead = pltpu.roll(rows, quarter, 1)
    return jnp.where(lane % half < quarter, back, ahead)


def attend_back_kernel(dims, groups, lam_ref, q_ref, kv_ref, gg_ref, gain_ref,
                       mixed_ref, second_ref, lse_ref, cost_ref, sint_ref, cosn_ref, sinn_ref,
                       wg_ref,
                       gq_ref, gk_ref, gv_ref, gpart_ref, lpart_ref, wsum_ref,
                       kt_ref, qbdt_ref, qbd_ref, gt_ref, g_ref, delta_ref, dqt_ref,
                       dka_ref, dva_ref, sb_ref, r1_ref, s2_ref, r2_ref,
                       wr2_ref,
                       s1_sem, r1_sem, s2_sem, r2_sem, w2s_sem, w2r_sem):
    slots, parts, heads, tile, width, strip = dims
    half = width // 2
    scale = half ** -0.5
    part = lax.axis_index("ctx")
    row = lax.axis_index("dp")
    core = part % 2
    y = part // 2
    other_core = 1 - core
    other_y = 1 - y
    me = row * 2 + y
    sibling = {"ctx": y * 2 + other_core}
    across = {"ctx": other_y * 2 + core}

    def group_device(index):
        return {"dp": index // 2, "ctx": (index % 2) * 2 + core}

    others = [lax.rem(me + step, groups) for step in range(1, groups)]
    greet([sibling] + [group_device(index) for index in others])

    def weights_send(step):
        index = others[step]
        return mesh_copy(wg_ref.at[:, index], wr2_ref.at[step], w2s_sem.at[step],
                         w2r_sem.at[step], group_device(index))

    for step in range(groups - 1):
        weights_send(step).start()

    def weights_finish():
        for step in range(groups - 1):
            weights_send(step).wait()
        for t in range(wg_ref.shape[0]):
            total = wg_ref[t, me].astype(F32)
            for step in range(groups - 1):
                total = total + wr2_ref[step, t].astype(F32)
            wsum_ref[t] = total

    def first_copy(j):
        return mesh_copy(sb_ref.at[j, other_core], r1_ref.at[j], s1_sem.at[j], r1_sem.at[j],
                         sibling)

    def second_copy(j):
        return mesh_copy(s2_ref.at[j], r2_ref.at[j], s2_sem.at[j], r2_sem.at[j], across)

    def pass_on(j):
        first_copy(j).wait()
        s2_ref[j] = (
            sb_ref[j, core, other_y].astype(F32) + r1_ref[j, other_y].astype(F32)).astype(BF16)

    def finish(j):
        second_copy(j).wait()
        total = (sb_ref[j, core, y].astype(F32) + r1_ref[j, y].astype(F32)
                 + r2_ref[j].astype(F32))
        gv_ref[j] = total[1].astype(BF16)
        for h in range(heads):
            lanes = slice(h * width, (h + 1) * width)
            grad = total[0, :, lanes]
            gk_ref[j, :, lanes] = (
                grad * cosn_ref[j] + swap_halves(grad, half) * sinn_ref[j]).astype(BF16)

    gpart_ref[...] = jnp.zeros_like(gpart_ref)
    lpart_ref[...] = jnp.zeros_like(lpart_ref)
    query_off = offsets_of(part, parts, strip, 1, (1, tile))
    query_off = jnp.concatenate([query_off, query_off], axis=1)

    def prepare(place, carry):
        for h in range(heads):
            lanes = slice(h * width, (h + 1) * width)
            lam = lam_ref[h]
            grad = gg_ref[lanes, pl.ds(pl.multiple_of(place * tile, tile), tile)]
            mixed = mixed_ref[place, h]
            second = second_ref[place, h]
            rg = lax.rsqrt(jnp.mean(mixed * mixed, axis=0, keepdims=True) + EPSILON)
            gpart_ref[lanes, :] += grad * (mixed * rg)
            up = grad * (gain_ref[lanes, :] * SHRINK)
            gm = rg * up - mixed * (rg * rg * rg * jnp.mean(up * mixed, axis=0, keepdims=True))
            lpart_ref[h] -= gm * second
            along = jnp.sum(gm * second, axis=0, keepdims=True)
            first = jnp.sum(gm * mixed, axis=0, keepdims=True) + lam * along
            delta_ref[place, h] = jnp.concatenate([first, -lam * along], axis=1)
            both = jnp.concatenate([gm, -lam * gm], axis=1)
            gt_ref[place, h] = both.astype(BF16)
            g_ref[place, h] = jnp.transpose(both).astype(BF16)
            query = q_ref[place, :, lanes]
            query = query * jnp.asarray(scale, query.dtype)
            qbdt_ref[place, h] = block_diag_cols(jnp.transpose(query), half, tile)
            lane = lax.broadcasted_iota(jnp.int32, (tile, width), 1)
            zero = jnp.zeros_like(query)
            qbd_ref[place, h, :tile] = jnp.where(lane < half, query, zero)
            qbd_ref[place, h, tile:] = jnp.where(lane >= half, query, zero)
            dqt_ref[place, h] = jnp.zeros((width, tile), F32)
        return carry

    lax.fori_loop(0, slots, prepare, 0)

    def one_block(place, slot, diag):
        for h in range(heads):
            lse = lse_ref[place, h]
            delta = delta_ref[place, h]
            lanes = slice(h * width, (h + 1) * width)
            turned = []
            for c in range(parts):
                keys = kv_ref[c, slot, 0, :, lanes]
                s = dot(keys, qbdt_ref[place, h])
                if diag:
                    key_off = offsets_of(c, parts, strip, 0, (tile, 1))
                    s = jnp.where(key_off <= query_off, s, NEGATIVE)
                weights = jnp.exp(s - lse)
                probs = dot(kv_ref[c, slot, 1, :, lanes], gt_ref[place, h])
                ds = (weights * (probs - delta)).astype(BF16)
                dv = dot(weights.astype(BF16), g_ref[place, h])
                dk = dot(ds, qbd_ref[place, h])
                if diag:
                    dva_ref[h, c] = dv
                    dka_ref[h, c] = dk
                else:
                    dva_ref[h, c] += dv
                    dka_ref[h, c] += dk
                turned.append(ds)
            dq = dot(kt_ref[h], jnp.concatenate(turned, axis=0))
            dqt_ref[place, h, :half] += dq[:half, :tile]
            dqt_ref[place, h, half:] += dq[half:, tile:]

    def one_key_block(j, carry):
        slot = j
        for h in range(heads):
            for c in range(parts):
                kt_ref[h, :, c * tile:(c + 1) * tile] = jnp.transpose(
                    kv_ref[c, slot, 0, :, h * width:(h + 1) * width])
        one_block(j, slot, True)

        def rest(place, inner):
            one_block(place, slot, False)
            return inner

        lax.fori_loop(j + 1, slots, rest, 0)
        for h in range(heads):
            lanes = slice(h * width, (h + 1) * width)
            for c in range(parts):
                sb_ref[j, c % 2, c // 2, 0, :, lanes] = dka_ref[h, c].astype(BF16)
                sb_ref[j, c % 2, c // 2, 1, :, lanes] = dva_ref[h, c].astype(BF16)

        @pl.when(j >= 1)
        def _():
            pass_on(j - 1)

        @pl.when(j >= 2)
        def _():
            finish(j - 2)

        first_copy(j).start()

        @pl.when(j >= 1)
        def _():
            second_copy(j - 1).start()

        return carry

    lax.fori_loop(0, slots, one_key_block, 0)

    pass_on(slots - 1)

    def put(place, carry):
        quarter = half // 2
        for h in range(heads):
            pieces = []
            for m in range(2):
                lead = dqt_ref[place, h, m * half:m * half + quarter]
                trail = dqt_ref[place, h, m * half + quarter:(m + 1) * half]
                pieces.append(lead * cost_ref[place] + trail * sint_ref[place])
                pieces.append(trail * cost_ref[place] - lead * sint_ref[place])
            turned = jnp.concatenate(pieces, axis=0) * scale
            gq_ref[place, :, h * width:(h + 1) * width] = jnp.transpose(turned).astype(BF16)
        return carry

    lax.fori_loop(0, 1, put, 0)
    second_copy(slots - 1).start()
    lax.fori_loop(1, slots, put, 0)
    finish(slots - 2)
    weights_finish()
    finish(slots - 1)


def specs(count, smem):
    return [pl.BlockSpec(memory_space=pltpu.SMEM)] * smem + [
        pl.BlockSpec(memory_space=pltpu.VMEM)] * (count - smem)


def attend(dims, part, lam, queries, kv_all, gain):
    slots, parts, heads, tile, width, strip = dims
    return pl.pallas_call(
        partial(attend_kernel, dims),
        out_shape=(
            jax.ShapeDtypeStruct((slots, tile, heads * width), BF16),
            jax.ShapeDtypeStruct((slots, heads, width, tile), F32),
            jax.ShapeDtypeStruct((slots, heads, width, tile), F32),
            jax.ShapeDtypeStruct((slots, heads, 1, 2 * tile), F32),
        ),
        in_specs=specs(5, 2),
        out_specs=specs(4, 0),
        scratch_shapes=[
            pltpu.VMEM((heads, slots, width, parts * tile), BF16),
            pltpu.VMEM((heads, width, 2 * tile), BF16),
            pltpu.VMEM((heads, width, 2 * tile), F32),
        ],
        compiler_params=pltpu.CompilerParams(vmem_limit_bytes=48 << 20),
        cost_estimate=pl.CostEstimate(
            flops=20_000_000_000, bytes_accessed=12_000_000, transcendentals=14_000_000),
        name="attend",
    )(part, lam, queries, kv_all, gain)


def attend_back(dims, groups, lam, queries, kv_all, gg, gain, mixed, second,
                lse, tables, wgrads):
    slots, parts, heads, tile, width, strip = dims
    assert parts == 4
    full = heads * width
    kinds, rows, cols = wgrads.shape[0], wgrads.shape[-2], wgrads.shape[-1]
    rows_low = jax.ShapeDtypeStruct((slots, tile, full), BF16)
    return pl.pallas_call(
        partial(attend_back_kernel, dims, groups),
        out_shape=(
            rows_low,
            rows_low,
            rows_low,
            jax.ShapeDtypeStruct((full, tile), F32),
            jax.ShapeDtypeStruct((heads, width, tile), F32),
            jax.ShapeDtypeStruct((kinds, rows, cols), F32),
        ),
        in_specs=specs(13, 1),
        out_specs=specs(6, 0),
        scratch_shapes=[
            pltpu.VMEM((heads, width, parts * tile), BF16),
            pltpu.VMEM((slots, heads, width, 2 * tile), BF16),
            pltpu.VMEM((slots, heads, 2 * tile, width), BF16),
            pltpu.VMEM((slots, heads, width, 2 * tile), BF16),
            pltpu.VMEM((slots, heads, 2 * tile, width), BF16),
            pltpu.VMEM((slots, heads, 1, 2 * tile), F32),
            pltpu.VMEM((slots, heads, width, tile), F32),
            pltpu.VMEM((heads, parts, tile, width), F32),
            pltpu.VMEM((heads, parts, tile, width), F32),
            pltpu.VMEM((slots, 2, 2, 2, tile, full), BF16),
            pltpu.VMEM((slots, 2, 2, tile, full), BF16),
            pltpu.VMEM((slots, 2, tile, full), BF16),
            pltpu.VMEM((slots, 2, tile, full), BF16),
            pltpu.VMEM((groups - 1, kinds, rows, cols), BF16),
            pltpu.SemaphoreType.DMA((slots,)),
            pltpu.SemaphoreType.DMA((slots,)),
            pltpu.SemaphoreType.DMA((slots,)),
            pltpu.SemaphoreType.DMA((slots,)),
            pltpu.SemaphoreType.DMA((groups - 1,)),
            pltpu.SemaphoreType.DMA((groups - 1,)),
        ],
        compiler_params=pltpu.CompilerParams(
            vmem_limit_bytes=60 << 20, collective_id=1, has_side_effects=True),
        cost_estimate=pl.CostEstimate(
            flops=60_000_000_000, bytes_accessed=24_000_000, transcendentals=14_000_000),
        name="attend_back",
    )(lam, queries, kv_all, gg, gain, mixed, second, lse, *tables, wgrads)


def dot_turned(left, right):
    return lax.dot_general(left, right, (((1,), (1,)), ((), ())), preferred_element_type=F32)


def dot_rows(left, right):
    return lax.dot_general(left, right, (((0,), (0,)), ((), ())), preferred_element_type=F32)


class LineSum:
    def __init__(self, axis, size, own, from_left, from_right, sems):
        self.axis, self.size = axis, size
        self.me = lax.axis_index(axis)
        self.own, self.buffers, self.sems = own, (from_left, from_right), sems

    def copy(self, q, t, side):
        target = self.size - 1 - t + self.me if side == 0 else t - (self.size - 1) + self.me
        target = jnp.clip(target, 0, self.size - 1)
        neighbour = jnp.clip(self.me + (1 if side == 0 else -1), 0, self.size - 1)
        return target, mesh_copy(
            self.own.at[q, target], self.buffers[side].at[q, t], self.sems.at[0, side, q, t],
            self.sems.at[1, side, q, t], {self.axis: neighbour})

    def rank(self, side):
        return self.me if side == 0 else self.size - 1 - self.me

    def step(self, q, t):
        for side in range(2):
            rank = self.rank(side)
            target, copy = self.copy(q, t, side)

            if t > 0:
                @pl.when((rank <= t) & (rank > 0))
                def _():
                    self.copy(q, t - 1, side)[1].wait_recv()
                    self.own[q, target] = (
                        self.own[q, target].astype(F32)
                        + self.buffers[side][q, t - 1].astype(F32)).astype(BF16)

            @pl.when(rank <= t)
            def _():
                copy.start()

    def total(self, q, acc):
        acc[...] = self.own[q, self.me].astype(F32)
        for side in range(2):
            @pl.when(self.rank(side) > 0)
            def _():
                self.copy(q, self.size - 2, side)[1].wait_recv()
                acc[...] += self.buffers[side][q, self.size - 2].astype(F32)

    def drain(self, q):
        for t in range(self.size - 1):
            for side in range(2):
                @pl.when(self.rank(side) <= t)
                def _():
                    self.copy(q, t, side)[1].wait_send()


def line_scratch(chunks, size, rows, width):
    return [
        pltpu.VMEM((chunks, size, rows, width), BF16),
        pltpu.VMEM((chunks, size - 1, rows, width), BF16),
        pltpu.VMEM((chunks, size - 1, rows, width), BF16),
        pltpu.VMEM((rows, width), F32),
        pltpu.SemaphoreType.DMA((2, 2, chunks, size - 1)),
    ]


def finish_kernel(dims, groups, lines, gq_ref, gk_ref, gv_ref, wq_ref, wk_ref, wv_ref, normed_ref,
                  branch_ref, grouped_ref, inputs_ref, gh_ref, gain_ref, small_ref, bo_ref,
                  ig_ref, wsum_ref, vec_ref, bout_ref,
                  own_ref, left_ref, right_ref, acc_ref, line_sem,
                  wloc_ref, wr1_ref, wr2_ref, mixer_ref, va_ref, vb_ref, vc_ref, v2_ref,
                  w1_sem, w2_sem, va_sem, vb_sem, vc_sem, bo_sem):
    slots, parts, heads, tile, width, strip = dims
    full = heads * width
    model = normed_ref.shape[-1]
    chunks = own_ref.shape[0]
    per = slots // chunks
    part = lax.axis_index("ctx")
    row = lax.axis_index("dp")
    place = lax.axis_index("head")
    core = part % 2
    y = part // 2
    other_core = 1 - core
    me = row * 2 + y
    sibling = {"ctx": y * 2 + other_core}

    def group_device(index):
        return {"dp": index // 2, "ctx": (index % 2) * 2 + core}

    others = [lax.rem(me + step, groups) for step in range(1, groups)]
    line_others = [lax.rem(place + step, lines) for step in range(1, lines)]
    targets = [lax.rem(part + step, parts) for step in range(1, parts)]
    greet([sibling, {"ctx": (1 - y) * 2 + other_core}]
          + [group_device(index) for index in others]
          + [{"head": index} for index in line_others])
    line = LineSum("head", lines, own_ref, left_ref, right_ref, line_sem)
    mixer_ref[...] = jnp.zeros_like(mixer_ref)

    def out_copy(step):
        return mesh_copy(bo_ref.at[targets[step]], bout_ref.at[:, part], bo_sem.at[0, step],
                         bo_sem.at[1, step], {"ctx": targets[step]})

    block = 256

    def product(q):
        grads = [ref[q * per:(q + 1) * per].reshape(per * tile, full)
                 for ref in (gq_ref, gk_ref, gv_ref)]

        def columns(index, carry):
            cols = pl.ds(pl.multiple_of(index * block, block), block)
            terms = dot_turned(grads[0], wq_ref[cols, :])
            terms += dot_turned(grads[1], wk_ref[cols, :])
            terms += dot_turned(grads[2], wv_ref[cols, :])
            terms = terms.astype(BF16)
            for p in range(per):
                for z in range(lines):
                    own_ref[q, z, p * strip:(p + 1) * strip, cols] = (
                        terms[p * tile + z * strip:p * tile + (z + 1) * strip])
            return carry

        lax.fori_loop(0, model // block, columns, 0)

    rows = wsum_ref.shape[1]
    narrow = 128

    def weight_term(kind):
        rows_ref = branch_ref if kind == 3 else normed_ref
        grad_ref = (gq_ref, gk_ref, gv_ref, grouped_ref)[kind]

        def columns(index, carry):
            cols = pl.ds(pl.multiple_of(index * narrow, narrow), narrow)
            term = jnp.zeros((narrow, full), F32)
            for s in range(0, slots, 2):
                left = rows_ref[s:s + 2, :, cols].reshape(2 * tile, narrow)
                grad = grad_ref[s:s + 2].reshape(2 * tile, full)
                term += dot(jnp.transpose(left), grad)
            wloc_ref[kind, cols] = term.astype(BF16)
            return carry

        lax.fori_loop(0, model // narrow, columns, 0)

    def share(index, which):
        return pl.ds(pl.multiple_of((index * 2 + which) * rows, 16), rows)

    def weights_out(kind, index):
        return mesh_copy(wloc_ref.at[kind, share(index, other_core)], wr1_ref.at[kind, index],
                         w1_sem.at[0, kind, index], w1_sem.at[1, kind, index], sibling)

    def weights_send(kind, step):
        index = others[step]
        return mesh_copy(wloc_ref.at[kind, share(index, core)], wr2_ref.at[step, kind],
                         w2_sem.at[0, kind, step], w2_sem.at[1, kind, step],
                         group_device(index))

    def weights_cross(kind):
        for index in range(groups):
            weights_out(kind, index).wait()

        def add(index, carry):
            wloc_ref[kind, share(index, core)] = (
                wloc_ref[kind, share(index, core)].astype(F32)
                + wr1_ref[kind, index].astype(F32)).astype(BF16)
            return carry

        lax.fori_loop(0, groups, add, 0)

    def weights_finish():
        for k in range(4):
            for step in range(groups - 1):
                weights_send(k, step).wait()
            total = wloc_ref[k, share(me, core)].astype(F32)
            for step in range(groups - 1):
                total = total + wr2_ref[step, k].astype(F32)
            wsum_ref[k] = total

    def close(q):
        line.total(q, acc_ref)
        grad = acc_ref[...]
        x = inputs_ref[q * per:(q + 1) * per].reshape(per * strip, model).astype(F32)
        scale = lax.rsqrt(jnp.mean(x * x, axis=1, keepdims=True) + EPSILON)
        mixer_ref[...] += jnp.sum((grad * (x * scale)).reshape(per * strip // 8, 8, model), axis=0)
        up = grad * gain_ref[...]
        result = (gh_ref[q * per:(q + 1) * per].reshape(per * strip, model) + scale * up
                  - x * (scale * scale * scale * jnp.mean(up * x, axis=1, keepdims=True)))
        ig_ref[q * per:(q + 1) * per] = result.astype(BF16).reshape(per, strip, model)

    for slot in range(chunks + lines - 1):
        if slot < chunks:
            product(slot)
        for t in range(lines - 1):
            if 0 <= slot - t < chunks:
                line.step(slot - t, t)
        if slot == 0:
            for step in range(parts - 1):
                out_copy(step).start()
            bout_ref[:, part] = bo_ref[part]
        if 1 <= slot < 5:
            weights_cross(slot - 1)
        if slot < 4:
            weight_term(slot)
            for index in range(groups):
                weights_out(slot, index).start()
        if 1 <= slot < 5:
            for step in range(groups - 1):
                weights_send(slot - 1, step).start()
        if slot - lines + 1 >= 0:
            close(slot - lines + 1)
    first_row = lax.broadcasted_iota(jnp.int32, small_ref.shape, 0) == 0
    mixer = jnp.broadcast_to(jnp.sum(mixer_ref[...], axis=0, keepdims=True), small_ref.shape)
    va_ref[0] = jnp.where(first_row, mixer, small_ref[...])
    swap = mesh_copy(va_ref.at[0], va_ref.at[1], va_sem.at[0], va_sem.at[1], sibling)
    swap.start()
    swap.wait()
    vb_ref[me] = va_ref[0] + va_ref[1]

    def group_copy(source, target, sem):
        return mesh_copy(vb_ref.at[source], vb_ref.at[source], vb_sem.at[0, sem],
                         vb_sem.at[1, source], group_device(target))

    for step, index in enumerate(others):
        group_copy(me, index, step).start()
    for step, index in enumerate(others):
        group_copy(index, index, step).wait_recv()
    total = vb_ref[0]
    for index in range(1, groups):
        total = total + vb_ref[index]
    vc_ref[place] = total
    v2_ref[...] = total

    def line_copy(source, target, sem):
        return mesh_copy(vc_ref.at[source], vc_ref.at[source], vc_sem.at[0, sem],
                         vc_sem.at[1, source], {"head": target})

    for step, index in enumerate(line_others):
        line_copy(place, index, step).start()
    for step, index in enumerate(line_others):
        line_copy(index, index, step).wait_recv()
    total = vc_ref[0]
    for index in range(1, lines):
        total = total + vc_ref[index]
    row_index = lax.broadcasted_iota(jnp.int32, total.shape, 0)
    vec_ref[...] = jnp.where(row_index < 2, total, v2_ref[...])
    weights_finish()
    for q in range(chunks):
        line.drain(q)
    for step in range(parts - 1):
        out_copy(step).wait()
    for step, index in enumerate(others):
        group_copy(me, index, step).wait_send()
    for step, index in enumerate(line_others):
        line_copy(place, index, step).wait_send()


def finish(dims, groups, lines, chunks, rows, *operands):
    slots, parts, heads, tile, width, strip = dims
    full = heads * width
    model = operands[6].shape[-1]
    pairs = operands[-1].shape[1]
    return pl.pallas_call(
        partial(finish_kernel, dims, groups, lines),
        out_shape=(
            jax.ShapeDtypeStruct((slots, strip, model), BF16),
            jax.ShapeDtypeStruct((4, rows, full), F32),
            jax.ShapeDtypeStruct((8, model), F32),
            jax.ShapeDtypeStruct((pairs, parts, strip, model), BF16),
        ),
        in_specs=specs(14, 0),
        out_specs=specs(4, 0),
        scratch_shapes=line_scratch(chunks, lines, slots // chunks * strip, model) + [
            pltpu.VMEM((4, model, full), BF16),
            pltpu.VMEM((4, groups, rows, full), BF16),
            pltpu.VMEM((groups - 1, 4, rows, full), BF16),
            pltpu.VMEM((8, model), F32),
            pltpu.VMEM((2, 8, model), F32),
            pltpu.VMEM((groups, 8, model), F32),
            pltpu.VMEM((lines, 8, model), F32),
            pltpu.VMEM((8, model), F32),
            pltpu.SemaphoreType.DMA((2, 4, groups)),
            pltpu.SemaphoreType.DMA((2, 4, groups - 1)),
            pltpu.SemaphoreType.DMA((2,)),
            pltpu.SemaphoreType.DMA((2, groups)),
            pltpu.SemaphoreType.DMA((2, lines)),
            pltpu.SemaphoreType.DMA((2, parts - 1)),
        ],
        compiler_params=pltpu.CompilerParams(
            vmem_limit_bytes=60 << 20, collective_id=2, has_side_effects=True),
        cost_estimate=pl.CostEstimate(
            flops=8_000_000_000, bytes_accessed=24_000_000, transcendentals=0),
        name="finish",
    )(*operands)


class LineGather:
    def __init__(self, axis, size, view, sems):
        self.axis, self.size, self.view, self.sems = axis, size, view, sems
        self.me = lax.axis_index(axis)

    def copy(self, q, t, side):
        source = jnp.clip(self.me - t if side == 0 else self.me + t, 0, self.size - 1)
        neighbour = jnp.clip(self.me + (1 if side == 0 else -1), 0, self.size - 1)
        return mesh_copy(
            self.view(q, source), self.view(q, source), self.sems.at[0, side, q, t],
            self.sems.at[1, side, q, source], {self.axis: neighbour})

    def rank(self, side):
        return self.me if side == 0 else self.size - 1 - self.me

    def step(self, q, t):
        for side in range(2):
            rank = self.rank(side)

            if t > 0:
                @pl.when(rank >= t)
                def _():
                    self.copy(q, t, side).wait_recv()

            if t < self.size - 1:
                @pl.when((rank >= t) & (rank < self.size - 1))
                def _():
                    self.copy(q, t, side).start()

    def drain(self, q):
        for t in range(self.size - 1):
            for side in range(2):
                rank = self.rank(side)

                @pl.when((rank >= t) & (rank < self.size - 1))
                def _():
                    self.copy(q, t, side).wait_send()


def open_kernel(dims, lines, chunks, x_ref, gain_ref, wq_ref, wk_ref, wv_ref, cosn_ref, sinn_ref,
                cot_ref, normed_ref, q_ref, kv_ref, cout_ref,
                line_sem, c_sem, sib_sem, far_sem, fwd_sem):
    slots, parts, heads, tile, width, strip = dims
    half = width // 2
    per = slots // chunks
    model = x_ref.shape[-1]
    part = lax.axis_index("ctx")
    place = lax.axis_index("head")
    core = part % 2
    y = part // 2
    sibling = {"ctx": y * 2 + 1 - core}
    across = {"ctx": (1 - y) * 2 + core}
    far = (1 - y) * 2 + core
    far_other = (1 - y) * 2 + 1 - core
    near = y * 2 + 1 - core
    targets = [lax.rem(part + step, parts) for step in range(1, parts)]
    greet([{"ctx": target} for target in targets]
          + [{"head": lax.rem(place + step, lines)} for step in range(1, lines)])
    line = LineGather(
        "head", lines, lambda q, s: normed_ref.at[pl.ds(q * per, per), s], line_sem)

    def norm(q):
        x = x_ref[q * per:(q + 1) * per].reshape(per * strip, model).astype(F32)
        scale = lax.rsqrt(jnp.mean(x * x, axis=1, keepdims=True) + EPSILON)
        low = (x * scale * gain_ref[...]).astype(BF16).reshape(per, strip, model)
        for p in range(per):
            normed_ref[q * per + p, place] = low[p]

    def cot_copy(step):
        return mesh_copy(cot_ref.at[:, targets[step]], cout_ref.at[part], c_sem.at[0, step],
                         c_sem.at[1, step], {"ctx": targets[step]})

    def chunk_view(source, q):
        return kv_ref.at[source, pl.ds(q * per, per)]

    def to_sibling(q):
        return mesh_copy(chunk_view(part, q), chunk_view(part, q), sib_sem.at[0, q],
                         sib_sem.at[1, q], sibling)

    def from_sibling(q):
        return mesh_copy(chunk_view(near, q), chunk_view(near, q), sib_sem.at[0, q],
                         sib_sem.at[1, q], sibling)

    def to_far(q):
        return mesh_copy(chunk_view(part, q), chunk_view(part, q), far_sem.at[0, q],
                         far_sem.at[1, q], across)

    def from_far(q):
        return mesh_copy(chunk_view(far, q), chunk_view(far, q), far_sem.at[0, q],
                         far_sem.at[1, q], across)

    def forward(q):
        return mesh_copy(chunk_view(far, q), chunk_view(far, q), fwd_sem.at[0, q],
                         fwd_sem.at[1, q], sibling)

    def forwarded(q):
        return mesh_copy(chunk_view(far_other, q), chunk_view(far_other, q), fwd_sem.at[0, q],
                         fwd_sem.at[1, q], sibling)

    def project(q):
        rows = normed_ref[q * per:(q + 1) * per].reshape(per * tile, model)
        for kind, weight_ref in ((1, wv_ref), (0, wk_ref), (2, wq_ref)):
            result = dot(rows, weight_ref[...])
            for p in range(per):
                at = q * per + p
                for h in range(heads):
                    lanes = slice(h * width, (h + 1) * width)
                    piece = result[p * tile:(p + 1) * tile, lanes]
                    if kind != 1:
                        piece = piece * cosn_ref[at] - swap_halves(piece, half) * sinn_ref[at]
                    if kind == 2:
                        q_ref[at, :, lanes] = piece.astype(BF16)
                    else:
                        kv_ref[part, at, kind, :, lanes] = piece.astype(BF16)

    for slot in range(chunks + lines - 1):
        if slot < chunks:
            norm(slot)
        for t in range(lines):
            if 0 <= slot - t < chunks:
                line.step(slot - t, t)
        if slot == 0:
            for step in range(parts - 1):
                cot_copy(step).start()
            cout_ref[part] = cot_ref[:, part]
        q = slot - lines + 1
        if q >= 0:
            project(q)
            to_far(q).start()
            to_sibling(q).start()
        if q >= 1:
            from_far(q - 1).wait_recv()
            forward(q - 1).start()
    from_far(chunks - 1).wait_recv()
    forward(chunks - 1).start()
    for step in range(parts - 1):
        cot_copy(step).wait()
    for q in range(chunks):
        line.drain(q)
        from_sibling(q).wait_recv()
        to_sibling(q).wait_send()
        to_far(q).wait_send()
    for q in range(chunks):
        forwarded(q).wait_recv()
        forward(q).wait_send()


def open_rows(dims, lines, chunks, *operands):
    slots, parts, heads, tile, width, strip = dims
    full = heads * width
    model = operands[0].shape[-1]
    pairs = operands[-1].shape[0]
    return pl.pallas_call(
        partial(open_kernel, dims, lines, chunks),
        out_shape=(
            jax.ShapeDtypeStruct((slots, lines, strip, model), BF16),
            jax.ShapeDtypeStruct((slots, tile, full), BF16),
            jax.ShapeDtypeStruct((parts, slots, 2, tile, full), BF16),
            jax.ShapeDtypeStruct((parts, pairs, strip, model), BF16),
        ),
        in_specs=specs(8, 0),
        out_specs=specs(4, 0),
        scratch_shapes=[
            pltpu.SemaphoreType.DMA((2, 2, chunks, lines)),
            pltpu.SemaphoreType.DMA((2, parts - 1)),
            pltpu.SemaphoreType.DMA((2, chunks)),
            pltpu.SemaphoreType.DMA((2, chunks)),
            pltpu.SemaphoreType.DMA((2, chunks)),
        ],
        compiler_params=pltpu.CompilerParams(
            vmem_limit_bytes=60 << 20, collective_id=3, has_side_effects=True),
        cost_estimate=pl.CostEstimate(
            flops=4_000_000_000, bytes_accessed=16_000_000, transcendentals=0),
        name="open_rows",
    )(*operands)


def greet_line(axis, size):
    place = lax.axis_index(axis)
    greet([{axis: lax.rem(place + step, size)} for step in range(1, size)])


def scatter_terms(own_ref, q, cols, terms, dims, lines):
    slots, parts, heads, tile, width, strip = dims
    for p in range(terms.shape[0] // tile):
        for z in range(lines):
            own_ref[q, z, p * strip:(p + 1) * strip, cols] = (
                terms[p * tile + z * strip:p * tile + (z + 1) * strip])


def line_turn(lines, chunks, summed, gathered, before, between, after=None):
    for slot in range(chunks + 2 * (lines - 1)):
        if slot < chunks:
            before(slot)
        for t in range(lines - 1):
            if 0 <= slot - t < chunks:
                summed.step(slot - t, t)
        q = slot - lines + 1
        if 0 <= q < chunks:
            between(q)
        for t in range(lines):
            if 0 <= q - t < chunks:
                gathered.step(q - t, t)
        if after is not None:
            after(slot)
    for q in range(chunks):
        summed.drain(q)
        gathered.drain(q)


def feed_open_kernel(dims, lines, chunks, grouped_ref, wo_ref, inputs_ref, gain_ref, grad_ref,
                     down_ref, hidden_ref, rows_ref, gact_ref,
                     own_ref, left_ref, right_ref, acc_ref, line_sem, gather_sem):
    slots, parts, heads, tile, width, strip = dims
    full = heads * width
    per = slots // chunks
    model = inputs_ref.shape[-1]
    units = down_ref.shape[0]
    block = 256
    place = lax.axis_index("head")
    greet_line("head", lines)
    summed = LineSum("head", lines, own_ref, left_ref, right_ref, line_sem)
    gathered = LineGather(
        "head", lines, lambda q, s: rows_ref.at[pl.ds(q * per, per), s], gather_sem)

    def before(q):
        left = grouped_ref[q * per:(q + 1) * per].reshape(per * tile, full)

        def columns(index, carry):
            cols = pl.ds(pl.multiple_of(index * block, block), block)
            scatter_terms(own_ref, q, cols, dot(left, wo_ref[:, cols]).astype(BF16), dims, lines)
            return carry

        lax.fori_loop(0, model // block, columns, 0)

    def between(q):
        summed.total(q, acc_ref)
        hidden = inputs_ref[q * per:(q + 1) * per].reshape(per * strip, model).astype(F32)
        hidden = hidden + acc_ref[...]
        hidden_ref[q * per:(q + 1) * per] = hidden.reshape(per, strip, model)
        scale = lax.rsqrt(jnp.mean(hidden * hidden, axis=1, keepdims=True) + EPSILON)
        low = (hidden * scale * gain_ref[...]).astype(BF16).reshape(per, strip, model)
        for p in range(per):
            rows_ref[q * per + p, place] = low[p]

    def extra(q):
        grads = grad_ref[q * per:(q + 1) * per].reshape(per * tile, model)

        def columns(index, carry):
            cols = pl.ds(pl.multiple_of(index * block, block), block)
            result = dot_turned(grads, down_ref[cols, :])
            gact_ref[q * per:(q + 1) * per, :, cols] = result.reshape(per, tile, block)
            return carry

        lax.fori_loop(0, units // block, columns, 0)

    def before_all(q):
        before(q)
        if q > 0:
            extra(q - 1)
        if q == chunks - 1:
            extra(q)

    line_turn(lines, chunks, summed, gathered, before_all, between)


def feed_open(dims, lines, chunks, *operands):
    slots, parts, heads, tile, width, strip = dims
    model, units = operands[1].shape[1], operands[5].shape[0]
    return pl.pallas_call(
        partial(feed_open_kernel, dims, lines, chunks),
        out_shape=(
            jax.ShapeDtypeStruct((slots, strip, model), F32),
            jax.ShapeDtypeStruct((slots, lines, strip, model), BF16),
            jax.ShapeDtypeStruct((slots, tile, units), F32),
        ),
        in_specs=specs(6, 0),
        out_specs=specs(3, 0),
        scratch_shapes=line_scratch(chunks, lines, slots // chunks * strip, model) + [
            pltpu.SemaphoreType.DMA((2, 2, chunks, lines)),
        ],
        compiler_params=pltpu.CompilerParams(
            vmem_limit_bytes=60 << 20, collective_id=4, has_side_effects=True),
        cost_estimate=pl.CostEstimate(
            flops=4_000_000_000, bytes_accessed=20_000_000, transcendentals=0),
        name="feed_open",
    )(*operands)


def feed_close_kernel(dims, lines, chunks, gg_ref, gu_ref, wg_ref, wu_ref, rows_ref, grad_ref,
                      act_ref, hidden_ref, cot_ref, gain_ref,
                      gh_ref, branch_ref, pair_ref, part_ref,
                      own_ref, left_ref, right_ref, acc_ref, line_sem, gather_sem,
                      terms_ref, landed_ref, pair_sem):
    slots, parts, heads, tile, width, strip = dims
    per = slots // chunks
    model = cot_ref.shape[-1]
    units = act_ref.shape[-1]
    block, narrow = 256, 128
    place = lax.axis_index("head")
    part_index = lax.axis_index("ctx")
    core = part_index % 2
    sibling = {"ctx": part_index + 1 - 2 * core}
    greet([sibling] + [{"head": lax.rem(place + step, lines)} for step in range(1, lines)])
    groups, rows = pair_ref.shape[1:3]

    def share(index, which):
        return pl.ds(pl.multiple_of((index * 2 + which) * rows, 16), rows)

    def pair_copy(kind, index):
        return mesh_copy(terms_ref.at[kind, share(index, 1 - core)], landed_ref.at[kind, index],
                         pair_sem.at[0, kind, index], pair_sem.at[1, kind, index], sibling)

    def pair_sum(kind):
        for index in range(groups):
            pair_copy(kind, index).wait()

        def add(index, carry):
            pair_ref[kind, index] = (
                terms_ref[kind, share(index, core)].astype(F32)
                + landed_ref[kind, index].astype(F32)).astype(BF16)
            return carry

        lax.fori_loop(0, groups, add, 0)

    summed = LineSum("head", lines, own_ref, left_ref, right_ref, line_sem)
    gathered = LineGather(
        "head", lines, lambda q, s: branch_ref.at[pl.ds(q * per, per), s], gather_sem)
    part_ref[...] = jnp.zeros_like(part_ref)

    def weight_term(kind):
        left_rows = grad_ref if kind == 2 else rows_ref
        right_rows = (gg_ref, gu_ref, act_ref)[kind]

        def columns(index, carry):
            cols = pl.ds(pl.multiple_of(index * narrow, narrow), narrow)
            term = jnp.zeros((narrow, units), F32)
            for s in range(0, slots, 2):
                left = left_rows[s:s + 2, :, cols].reshape(2 * tile, narrow)
                term += dot(jnp.transpose(left), right_rows[s:s + 2].reshape(2 * tile, units))
            terms_ref[kind, cols] = term.astype(BF16)
            return carry

        lax.fori_loop(0, model // narrow, columns, 0)

    def before(q):
        gate = gg_ref[q * per:(q + 1) * per].reshape(per * tile, units)
        up = gu_ref[q * per:(q + 1) * per].reshape(per * tile, units)

        def columns(index, carry):
            cols = pl.ds(pl.multiple_of(index * block, block), block)
            terms = dot_turned(gate, wg_ref[cols, :]) + dot_turned(up, wu_ref[cols, :])
            scatter_terms(own_ref, q, cols, terms.astype(BF16), dims, lines)
            return carry

        lax.fori_loop(0, model // block, columns, 0)
        if q > 0:
            weight_term(q - 1)
            for index in range(groups):
                pair_copy(q - 1, index).start()

    def between(q):
        summed.total(q, acc_ref)
        grad = acc_ref[...]
        hidden = hidden_ref[q * per:(q + 1) * per].reshape(per * strip, model)
        scale = lax.rsqrt(jnp.mean(hidden * hidden, axis=1, keepdims=True) + EPSILON)
        part_ref[...] += jnp.sum(
            (grad * (hidden * scale)).reshape(per * strip // 8, 8, model), axis=0)
        up = grad * gain_ref[...]
        result = (cot_ref[q * per:(q + 1) * per].reshape(per * strip, model).astype(F32)
                  + scale * up
                  - hidden * (scale * scale * scale * jnp.mean(up * hidden, axis=1, keepdims=True)))
        gh_ref[q * per:(q + 1) * per] = result.reshape(per, strip, model)
        low = result.astype(BF16).reshape(per, strip, model)
        for p in range(per):
            branch_ref[q * per + p, place] = low[p]

    def after(slot):
        if lines <= slot < lines + 3:
            pair_sum(slot - lines)

    line_turn(lines, chunks, summed, gathered, before, between, after)


def feed_close(dims, groups, lines, chunks, *operands):
    slots, parts, heads, tile, width, strip = dims
    model, units = operands[8].shape[-1], operands[6].shape[-1]
    return pl.pallas_call(
        partial(feed_close_kernel, dims, lines, chunks),
        out_shape=(
            jax.ShapeDtypeStruct((slots, strip, model), F32),
            jax.ShapeDtypeStruct((slots, lines, strip, model), BF16),
            jax.ShapeDtypeStruct((3, groups, model // groups // 2, units), BF16),
            jax.ShapeDtypeStruct((8, model), F32),
        ),
        in_specs=specs(10, 0),
        out_specs=specs(4, 0),
        scratch_shapes=line_scratch(chunks, lines, slots // chunks * strip, model) + [
            pltpu.SemaphoreType.DMA((2, 2, chunks, lines)),
            pltpu.VMEM((3, model, units), BF16),
            pltpu.VMEM((3, groups, model // groups // 2, units), BF16),
            pltpu.SemaphoreType.DMA((2, 3, groups)),
        ],
        compiler_params=pltpu.CompilerParams(
            vmem_limit_bytes=60 << 20, collective_id=5, has_side_effects=True),
        cost_estimate=pl.CostEstimate(
            flops=16_000_000_000, bytes_accessed=40_000_000, transcendentals=0),
        name="feed_close",
    )(*operands)


def per_device(
    inputs,
    block_order,
    mixer_gain,
    query_weight,
    key_weight,
    value_weight,
    lambda_qone,
    lambda_kone,
    lambda_qtwo,
    lambda_ktwo,
    group_gain,
    output_weight,
    feed_gain,
    gate_weight,
    up_weight,
    down_weight,
    cotangent,
):
    seq_count, pair_count, short_rows, model_width = inputs.shape
    assert seq_count == 1
    parts = lax.axis_size("ctx")
    head_total = lax.axis_size("head")
    part = lax.axis_index("ctx")
    head_place = lax.axis_index("head")
    block_len = short_rows * head_total
    slots = block_order.shape[1]
    heads_here, head_dim = lambda_qone.shape
    qwidth = query_weight.shape[1]
    width = 2 * head_dim
    tile = block_len // parts
    strip = short_rows // parts
    dims = (slots, parts, heads_here, tile, width, strip)
    row_count = slots * tile
    order = block_order.reshape(slots)
    slot_of = jnp.argsort(order).astype(jnp.int32)
    index = jnp.arange(tile, dtype=jnp.int32)
    row_offsets = (index // strip) * short_rows + part * strip + index % strip
    own_places = jnp.arange(slots, dtype=jnp.int32)[:, None] * block_len + row_offsets[None, :]
    groups = lax.axis_size("dp") * parts // 2
    quarter = head_dim // 2
    frequency = THETA ** (-jnp.arange(quarter, dtype=jnp.float32) / quarter)
    angles = own_places.astype(F32)[:, None, :] * frequency[None, :, None]
    cos_turned, sin_turned = jnp.cos(angles), jnp.sin(angles)
    cos_rows = jnp.tile(cos_turned.transpose(0, 2, 1), (1, 1, 4))
    sin_rows = jnp.tile(sin_turned.transpose(0, 2, 1), (1, 1, 4))
    lane = jnp.arange(width)
    sin_rows = jnp.where(lane % head_dim < quarter, sin_rows, -sin_rows)
    tables = (cos_turned, sin_turned, cos_rows, sin_rows)
    lambda_one = jnp.exp(jnp.sum(lambda_qone * lambda_kone, axis=-1))
    lambda_two = jnp.exp(jnp.sum(lambda_qtwo * lambda_ktwo, axis=-1))
    lambda_head = lambda_one - lambda_two + LAMBDA_INIT
    split_shape = (slots, tile, heads_here, 2, head_dim)
    rows_shape = (slots, tile, model_width)

    def spread(rows):
        cut = rows.reshape(pair_count, parts, strip, model_width).transpose(1, 0, 2, 3)
        cut = lax.all_to_all(cut, "ctx", 0, 0, tiled=True)
        return jnp.take(cut.reshape(slots, strip, model_width), slot_of, axis=0)

    def unspread(rows):
        cut = jnp.take(rows, order, axis=0).reshape(parts, pair_count, strip, model_width)
        cut = lax.all_to_all(cut, "ctx", 0, 0, tiled=True)
        return cut.transpose(1, 0, 2, 3).reshape(1, pair_count, short_rows, model_width)

    inputs_here = spread(inputs)
    tokens = inputs_here.astype(jnp.float32)
    part_shape = (slots, tile, qwidth)
    cut_shape = (pair_count, parts, strip, model_width)
    normed_rows, queries, kv_all, cotangent_slots = open_rows(
        dims, head_total, 4, inputs_here, mixer_gain.reshape(1, model_width), query_weight,
        key_weight, value_weight, cos_rows, sin_rows, cotangent.reshape(cut_shape))
    cotangent_here = jnp.take(
        cotangent_slots.reshape(slots, strip, model_width), slot_of, axis=0)
    grad_rows = lax.all_gather(cotangent_here, "head", axis=1, tiled=True)
    part_arr = part.reshape(1).astype(jnp.int32)
    gain_col = group_gain.reshape(qwidth, 1)
    grouped, mixed, second, lse = attend(
        dims, part_arr, lambda_head, queries, kv_all,
        gain_col)
    grouped, grad_rows = lax.optimization_barrier((grouped, grad_rows))
    hidden, feed_rows, grad_activ = feed_open(
        dims, head_total, 4, grouped, output_weight, inputs_here,
        feed_gain.reshape(1, model_width), grad_rows, down_weight)
    feed_rows = feed_rows.reshape(row_count, model_width)
    grad_activ = grad_activ.reshape(row_count, grad_activ.shape[-1])
    gate_vals = jnp.dot(feed_rows, gate_weight, preferred_element_type=jnp.float32)
    up_vals = jnp.dot(feed_rows, up_weight, preferred_element_type=jnp.float32)
    gate_sigmoid = jax.nn.sigmoid(gate_vals)
    silu_gate = gate_vals * gate_sigmoid
    activation = (silu_gate * up_vals).astype(jnp.bfloat16)
    grad_gate = (
        grad_activ * up_vals * gate_sigmoid * (1.0 + gate_vals * (1.0 - gate_sigmoid))
    ).astype(jnp.bfloat16)
    grad_up = (grad_activ * silu_gate).astype(jnp.bfloat16)
    unit_shape = (slots, tile, activation.shape[-1])
    grad_hidden, branch_rows, wgrads, feed_part = feed_close(
        dims, groups, head_total, 4, grad_gate.reshape(unit_shape), grad_up.reshape(unit_shape),
        gate_weight, up_weight, feed_rows.reshape(slots, tile, model_width), grad_rows,
        activation.reshape(unit_shape), hidden, cotangent_here, feed_gain.reshape(1, model_width))
    feed_part = jnp.sum(feed_part, axis=0)
    branch_rows = branch_rows.reshape(row_count, model_width)
    feed_terms = jnp.dot(activation, down_weight, preferred_element_type=jnp.float32).reshape(
        rows_shape
    )
    branch_rows, feed_terms = lax.optimization_barrier((branch_rows, feed_terms.astype(BF16)))
    feed_sum = lax.psum_scatter(feed_terms, "head", scatter_dimension=1, tiled=True)
    grad_grouped = contract_cols(output_weight, branch_rows)
    shares = lax.axis_size("dp") * parts
    grad_query, grad_key, grad_value, group_part, lambda_part, feed_sums = attend_back(
        dims, groups, lambda_head, queries, kv_all,
        grad_grouped, gain_col, mixed, second, lse, tables, wgrads)
    feed_sum, grad_query = lax.optimization_barrier((feed_sum, grad_query))
    block_out = (hidden + feed_sum.astype(F32)).astype(BF16)
    group_part = jnp.sum(group_part, axis=1) * SHRINK
    lambda_part = jnp.sum(lambda_part, axis=(1, 2))
    third = jnp.pad(
        jnp.concatenate([group_part, lambda_part]), (0, model_width - qwidth - heads_here))
    small = jnp.pad(jnp.stack([jnp.zeros_like(feed_part), feed_part, third]), ((0, 5), (0, 0)))
    grad_rows_shape = (slots, tile, model_width)
    block_slots = jnp.take(block_out, order, axis=0).reshape(
        parts, pair_count, strip, model_width)
    input_grad, attn_sums, vectors, block_out = finish(
        dims, groups, head_total, 4, model_width // shares, grad_query, grad_key, grad_value,
        query_weight, key_weight, value_weight, normed_rows.reshape(grad_rows_shape),
        branch_rows.reshape(grad_rows_shape), grouped.reshape(part_shape), inputs_here,
        grad_hidden, mixer_gain.reshape(1, model_width), small, block_slots)
    block_out = block_out.reshape(inputs.shape)
    input_grad = unspread(input_grad).astype(F32)
    group_grad = vectors[2, :qwidth]
    lambda_grad = vectors[2, qwidth:qwidth + heads_here]
    qone_grad = (lambda_grad * lambda_one)[:, None] * lambda_kone
    kone_grad = (lambda_grad * lambda_one)[:, None] * lambda_qone
    qtwo_grad = -(lambda_grad * lambda_two)[:, None] * lambda_ktwo
    ktwo_grad = -(lambda_grad * lambda_two)[:, None] * lambda_qtwo
    return (
        block_out,
        input_grad,
        vectors[0],
        attn_sums[0],
        attn_sums[1],
        attn_sums[2],
        qone_grad,
        kone_grad,
        qtwo_grad,
        ktwo_grad,
        group_grad,
        attn_sums[3].T,
        vectors[1],
        feed_sums[0],
        feed_sums[1],
        feed_sums[2].T,
    )


def solution(mesh):
    return jax.shard_map(
        per_device,
        mesh=mesh,
        in_specs=(
            P("dp", "ctx", "head", None),
            P("dp", None),
            P(),
            P(None, "head"),
            P(None, "head"),
            P(None, "head"),
            P("head", None),
            P("head", None),
            P("head", None),
            P("head", None),
            P("head"),
            P("head", None),
            P(),
            P(None, "head"),
            P(None, "head"),
            P("head", None),
            P("dp", "ctx", "head", None),
        ),
        out_specs=(
            P("dp", "ctx", "head", None),
            P("dp", "ctx", "head", None),
            P(),
            P(("dp", "ctx"), "head"),
            P(("dp", "ctx"), "head"),
            P(("dp", "ctx"), "head"),
            P("head", None),
            P("head", None),
            P("head", None),
            P("head", None),
            P("head"),
            P("head", ("dp", "ctx")),
            P(),
            P(("dp", "ctx"), "head"),
            P(("dp", "ctx"), "head"),
            P("head", ("dp", "ctx")),
        ),
        check_vma=False,
    )
```

```python
from functools import partial
import math

import jax
import jax.numpy as jnp
from jax import lax
from jax.experimental import pallas as pl
from jax.experimental.pallas import tpu as pltpu
from jax.sharding import PartitionSpec as P

EPSILON = 1e-05
LAMBDA_INIT = 0.8 - 0.6 * math.exp(-0.3 * 12)
SHRINK = 1.0 - LAMBDA_INIT
THETA = 10000.0
NEGATIVE = -1e30
F32 = jnp.float32
BF16 = jnp.bfloat16


def rms_scale(value_rows):
    return lax.rsqrt(jnp.mean(value_rows * value_rows, axis=-1, keepdims=True) + EPSILON)


def norm_back(grad_in, value_rows, scale, gain):
    upstream = grad_in * gain
    return scale * upstream - value_rows * scale**3 * jnp.mean(
        upstream * value_rows, axis=-1, keepdims=True
    )


def rotate(tensor, places, direction):
    half_dim = tensor.shape[-1] // 2
    frequency = THETA ** (-jnp.arange(half_dim, dtype=jnp.float32) / half_dim)
    angles = places.astype(jnp.float32)[..., None] * frequency
    angles = angles.reshape(places.shape + (1,) * (tensor.ndim - places.ndim - 1) + (half_dim,))
    cosine = jnp.cos(angles)
    sine_part = jnp.sin(angles) * direction
    leading = tensor[..., :half_dim]
    trailing = tensor[..., half_dim:]
    return jnp.concatenate(
        [leading * cosine - trailing * sine_part, leading * sine_part + trailing * cosine], axis=-1
    )


def contract_rows(left, right):
    return lax.dot_general(
        left, right, (((0,), (0,)), ((), ())), preferred_element_type=jnp.float32
    )


def contract_cols(left, right):
    return lax.dot_general(
        left, right, (((1,), (1,)), ((), ())), preferred_element_type=jnp.float32
    )


def dot(left, right):
    return lax.dot_general(left, right, (((1,), (0,)), ((), ())), preferred_element_type=F32)


def offsets_of(part, parts, strip, axis, shape):
    index = lax.broadcasted_iota(jnp.int32, shape, axis)
    return (index // strip) * (parts * strip) + part * strip + index % strip


def block_diag_cols(turned, half, lanes):
    row = lax.broadcasted_iota(jnp.int32, (turned.shape[0], lanes), 0)
    zero = jnp.zeros_like(turned)
    return jnp.concatenate(
        [jnp.where(row < half, turned, zero), jnp.where(row >= half, turned, zero)], axis=1
    )


def attend_kernel(dims, part_ref, lam_ref, q_ref, kv_ref, gain_ref,
                  grouped_ref, mixed_ref, second_ref, lse_ref, vt_ref, qbd_ref, acc_ref):
    slots, parts, heads, tile, width, strip = dims
    half = width // 2
    cols = 2 * tile

    def turn(slot, carry):
        for h in range(heads):
            for c in range(parts):
                vt_ref[h, slot, :, c * tile:(c + 1) * tile] = jnp.transpose(
                    kv_ref[c, slot, 1, :, h * width:(h + 1) * width])
        return carry

    lax.fori_loop(0, slots, turn, 0)
    query_off = offsets_of(part_ref[0], parts, strip, 1, (1, tile))
    query_off = jnp.concatenate([query_off, query_off], axis=1)

    def one_block(slot, diag, state):
        out = []
        for h in range(heads):
            peak, total = state[2 * h], state[2 * h + 1]
            scores = []
            for c in range(parts):
                s = dot(kv_ref[c, slot, 0, :, h * width:(h + 1) * width], qbd_ref[h])
                if diag:
                    key_off = offsets_of(c, parts, strip, 0, (tile, 1))
                    s = jnp.where(key_off <= query_off, s, NEGATIVE)
                scores.append(s)
            top = scores[0]
            for s in scores[1:]:
                top = jnp.maximum(top, s)
            higher = jnp.maximum(peak, jnp.max(top, axis=0, keepdims=True))
            keep = jnp.exp(peak - higher)
            weights = [jnp.exp(s - higher) for s in scores]
            added = weights[0]
            for w in weights[1:]:
                added = added + w
            total = total * keep + jnp.sum(added, axis=0, keepdims=True)
            low = jnp.concatenate([w.astype(BF16) for w in weights], axis=0)
            acc_ref[h] = acc_ref[h] * keep + dot(vt_ref[h, slot], low)
            out += [higher, total]
        return tuple(out)

    def one_place(place, carry):
        for h in range(heads):
            turned = jnp.transpose(q_ref[place, :, h * width:(h + 1) * width])
            turned = turned * jnp.asarray(half ** -0.5, turned.dtype)
            qbd_ref[h] = block_diag_cols(turned, half, tile)
            acc_ref[h] = jnp.zeros((width, cols), F32)
        state = (jnp.full((1, cols), NEGATIVE, F32), jnp.zeros((1, cols), F32)) * heads
        state = one_block(place, True, state)
        state = lax.fori_loop(
            0, place, lambda j, st: one_block(j, False, st), state)
        for h in range(heads):
            peak, total = state[2 * h], state[2 * h + 1]
            result = acc_ref[h] / total
            second = result[:, tile:]
            mixed = result[:, :tile] - lam_ref[h] * second
            scale = lax.rsqrt(jnp.mean(mixed * mixed, axis=0, keepdims=True) + EPSILON)
            gain = gain_ref[h * width:(h + 1) * width, :] * SHRINK
            grouped = (mixed * scale * gain).astype(BF16)
            grouped_ref[place, :, h * width:(h + 1) * width] = jnp.transpose(grouped)
            mixed_ref[place, h] = mixed
            second_ref[place, h] = second
            lse_ref[place, h] = peak + jnp.log(total)
        return carry

    lax.fori_loop(0, slots, one_place, 0)


def mesh_copy(src, dst, send_sem, recv_sem, device):
    return pltpu.make_async_remote_copy(
        src_ref=src, dst_ref=dst, send_sem=send_sem, recv_sem=recv_sem,
        device_id=device, device_id_type=pl.DeviceIdType.MESH)


def greet(devices):
    barrier = pltpu.get_barrier_semaphore()
    for device in devices:
        pl.semaphore_signal(
            barrier, inc=1, device_id=device, device_id_type=pl.DeviceIdType.MESH)
    pl.semaphore_wait(barrier, len(devices))


def swap_halves(rows, half):
    quarter = half // 2
    lane = lax.broadcasted_iota(jnp.int32, rows.shape, 1)
    back = pltpu.roll(rows, rows.shape[1] - quarter, 1)
    ahead = pltpu.roll(rows, quarter, 1)
    return jnp.where(lane % half < quarter, back, ahead)


def attend_back_kernel(dims, groups, lam_ref, q_ref, kv_ref, gg_ref, gain_ref,
                       mixed_ref, second_ref, lse_ref, cost_ref, sint_ref, cosn_ref, sinn_ref,
                       wg_ref,
                       gq_ref, gk_ref, gv_ref, gpart_ref, lpart_ref, wsum_ref,
                       kt_ref, qbdt_ref, qbd_ref, gt_ref, g_ref, delta_ref, dqt_ref,
                       dka_ref, dva_ref, sb_ref, r1_ref, s2_ref, r2_ref,
                       wr2_ref,
                       s1_sem, r1_sem, s2_sem, r2_sem, w2s_sem, w2r_sem):
    slots, parts, heads, tile, width, strip = dims
    half = width // 2
    scale = half ** -0.5
    part = lax.axis_index("ctx")
    row = lax.axis_index("dp")
    core = part % 2
    y = part // 2
    other_core = 1 - core
    other_y = 1 - y
    me = row * 2 + y
    sibling = {"ctx": y * 2 + other_core}
    across = {"ctx": other_y * 2 + core}

    def group_device(index):
        return {"dp": index // 2, "ctx": (index % 2) * 2 + core}

    others = [lax.rem(me + step, groups) for step in range(1, groups)]
    greet([sibling] + [group_device(index) for index in others])

    def weights_send(step):
        index = others[step]
        return mesh_copy(wg_ref.at[:, index], wr2_ref.at[step], w2s_sem.at[step],
                         w2r_sem.at[step], group_device(index))

    for step in range(groups - 1):
        weights_send(step).start()

    def weights_finish():
        for step in range(groups - 1):
            weights_send(step).wait()
        for t in range(wg_ref.shape[0]):
            total = wg_ref[t, me].astype(F32)
            for step in range(groups - 1):
                total = total + wr2_ref[step, t].astype(F32)
            wsum_ref[t] = total

    def first_copy(j):
        return mesh_copy(sb_ref.at[j, other_core], r1_ref.at[j], s1_sem.at[j], r1_sem.at[j],
                         sibling)

    def second_copy(j):
        return mesh_copy(s2_ref.at[j], r2_ref.at[j], s2_sem.at[j], r2_sem.at[j], across)

    def pass_on(j):
        first_copy(j).wait()
        s2_ref[j] = (
            sb_ref[j, core, other_y].astype(F32) + r1_ref[j, other_y].astype(F32)).astype(BF16)

    def finish(j):
        second_copy(j).wait()
        total = (sb_ref[j, core, y].astype(F32) + r1_ref[j, y].astype(F32)
                 + r2_ref[j].astype(F32))
        gv_ref[j] = total[1].astype(BF16)
        for h in range(heads):
            lanes = slice(h * width, (h + 1) * width)
            grad = total[0, :, lanes]
            gk_ref[j, :, lanes] = (
                grad * cosn_ref[j] + swap_halves(grad, half) * sinn_ref[j]).astype(BF16)

    gpart_ref[...] = jnp.zeros_like(gpart_ref)
    lpart_ref[...] = jnp.zeros_like(lpart_ref)
    query_off = offsets_of(part, parts, strip, 1, (1, tile))
    query_off = jnp.concatenate([query_off, query_off], axis=1)
    key_off = jnp.concatenate(
        [offsets_of(c, parts, strip, 0, (tile, 1)) for c in range(parts)], axis=0)

    def prepare(place, carry):
        for h in range(heads):
            lanes = slice(h * width, (h + 1) * width)
            lam = lam_ref[h]
            grad = gg_ref[lanes, pl.ds(pl.multiple_of(place * tile, tile), tile)]
            mixed = mixed_ref[place, h]
            second = second_ref[place, h]
            rg = lax.rsqrt(jnp.mean(mixed * mixed, axis=0, keepdims=True) + EPSILON)
            gpart_ref[lanes, :] += grad * (mixed * rg)
            up = grad * (gain_ref[lanes, :] * SHRINK)
            gm = rg * up - mixed * (rg * rg * rg * jnp.mean(up * mixed, axis=0, keepdims=True))
            lpart_ref[h] -= gm * second
            along = jnp.sum(gm * second, axis=0, keepdims=True)
            first = jnp.sum(gm * mixed, axis=0, keepdims=True) + lam * along
            delta_ref[place, h] = jnp.concatenate([first, -lam * along], axis=1)
            both = jnp.concatenate([gm, -lam * gm], axis=1)
            gt_ref[place, h] = both.astype(BF16)
            g_ref[place, h] = jnp.transpose(both).astype(BF16)
            query = q_ref[place, :, lanes]
            query = query * jnp.asarray(scale, query.dtype)
            qbdt_ref[place, h] = block_diag_cols(jnp.transpose(query), half, tile)
            lane = lax.broadcasted_iota(jnp.int32, (tile, width), 1)
            zero = jnp.zeros_like(query)
            qbd_ref[place, h, :tile] = jnp.where(lane < half, query, zero)
            qbd_ref[place, h, tile:] = jnp.where(lane >= half, query, zero)
            dqt_ref[place, h] = jnp.zeros((width, tile), F32)
        return carry

    lax.fori_loop(0, slots, prepare, 0)

    def one_block(place, slot, diag):
        for h in range(heads):
            lse = lse_ref[place, h]
            delta = delta_ref[place, h]
            lanes = slice(h * width, (h + 1) * width)
            keys = kv_ref[:, slot, 0, :, lanes].reshape(parts * tile, width)
            values = kv_ref[:, slot, 1, :, lanes].reshape(parts * tile, width)
            s = dot(keys, qbdt_ref[place, h])
            if diag:
                s = jnp.where(key_off <= query_off, s, NEGATIVE)
            weights = jnp.exp(s - lse)
            probs = dot(values, gt_ref[place, h])
            ds = (weights * (probs - delta)).astype(BF16)
            dv = dot(weights.astype(BF16), g_ref[place, h]).reshape(parts, tile, width)
            dk = dot(ds, qbd_ref[place, h]).reshape(parts, tile, width)
            if diag:
                dva_ref[h] = dv
                dka_ref[h] = dk
            else:
                dva_ref[h] += dv
                dka_ref[h] += dk
            dq = dot(kt_ref[h], ds)
            dqt_ref[place, h, :half] += dq[:half, :tile]
            dqt_ref[place, h, half:] += dq[half:, tile:]

    def one_key_block(j, carry):
        slot = j
        for h in range(heads):
            for c in range(parts):
                kt_ref[h, :, c * tile:(c + 1) * tile] = jnp.transpose(
                    kv_ref[c, slot, 0, :, h * width:(h + 1) * width])
        one_block(j, slot, True)

        def rest(place, inner):
            one_block(place, slot, False)
            return inner

        lax.fori_loop(j + 1, slots, rest, 0)
        for h in range(heads):
            lanes = slice(h * width, (h + 1) * width)
            for c in range(parts):
                sb_ref[j, c % 2, c // 2, 0, :, lanes] = dka_ref[h, c].astype(BF16)
                sb_ref[j, c % 2, c // 2, 1, :, lanes] = dva_ref[h, c].astype(BF16)

        @pl.when(j >= 1)
        def _():
            pass_on(j - 1)

        @pl.when(j >= 2)
        def _():
            finish(j - 2)

        first_copy(j).start()

        @pl.when(j >= 1)
        def _():
            second_copy(j - 1).start()

        return carry

    lax.fori_loop(0, slots, one_key_block, 0)

    pass_on(slots - 1)

    def put(place, carry):
        quarter = half // 2
        for h in range(heads):
            pieces = []
            for m in range(2):
                lead = dqt_ref[place, h, m * half:m * half + quarter]
                trail = dqt_ref[place, h, m * half + quarter:(m + 1) * half]
                pieces.append(lead * cost_ref[place] + trail * sint_ref[place])
                pieces.append(trail * cost_ref[place] - lead * sint_ref[place])
            turned = jnp.concatenate(pieces, axis=0) * scale
            gq_ref[place, :, h * width:(h + 1) * width] = jnp.transpose(turned).astype(BF16)
        return carry

    lax.fori_loop(0, 1, put, 0)
    second_copy(slots - 1).start()
    lax.fori_loop(1, slots, put, 0)
    finish(slots - 2)
    weights_finish()
    finish(slots - 1)


def specs(count, smem):
    return [pl.BlockSpec(memory_space=pltpu.SMEM)] * smem + [
        pl.BlockSpec(memory_space=pltpu.VMEM)] * (count - smem)


def attend(dims, part, lam, queries, kv_all, gain):
    slots, parts, heads, tile, width, strip = dims
    return pl.pallas_call(
        partial(attend_kernel, dims),
        out_shape=(
            jax.ShapeDtypeStruct((slots, tile, heads * width), BF16),
            jax.ShapeDtypeStruct((slots, heads, width, tile), F32),
            jax.ShapeDtypeStruct((slots, heads, width, tile), F32),
            jax.ShapeDtypeStruct((slots, heads, 1, 2 * tile), F32),
        ),
        in_specs=specs(5, 2),
        out_specs=specs(4, 0),
        scratch_shapes=[
            pltpu.VMEM((heads, slots, width, parts * tile), BF16),
            pltpu.VMEM((heads, width, 2 * tile), BF16),
            pltpu.VMEM((heads, width, 2 * tile), F32),
        ],
        compiler_params=pltpu.CompilerParams(vmem_limit_bytes=48 << 20),
        cost_estimate=pl.CostEstimate(
            flops=20_000_000_000, bytes_accessed=12_000_000, transcendentals=14_000_000),
        name="attend",
    )(part, lam, queries, kv_all, gain)


def attend_back(dims, groups, lam, queries, kv_all, gg, gain, mixed, second,
                lse, tables, wgrads):
    slots, parts, heads, tile, width, strip = dims
    assert parts == 4
    full = heads * width
    kinds, rows, cols = wgrads.shape[0], wgrads.shape[-2], wgrads.shape[-1]
    rows_low = jax.ShapeDtypeStruct((slots, tile, full), BF16)
    return pl.pallas_call(
        partial(attend_back_kernel, dims, groups),
        out_shape=(
            rows_low,
            rows_low,
            rows_low,
            jax.ShapeDtypeStruct((full, tile), F32),
            jax.ShapeDtypeStruct((heads, width, tile), F32),
            jax.ShapeDtypeStruct((kinds, rows, cols), F32),
        ),
        in_specs=specs(13, 1),
        out_specs=specs(6, 0),
        scratch_shapes=[
            pltpu.VMEM((heads, width, parts * tile), BF16),
            pltpu.VMEM((slots, heads, width, 2 * tile), BF16),
            pltpu.VMEM((slots, heads, 2 * tile, width), BF16),
            pltpu.VMEM((slots, heads, width, 2 * tile), BF16),
            pltpu.VMEM((slots, heads, 2 * tile, width), BF16),
            pltpu.VMEM((slots, heads, 1, 2 * tile), F32),
            pltpu.VMEM((slots, heads, width, tile), F32),
            pltpu.VMEM((heads, parts, tile, width), F32),
            pltpu.VMEM((heads, parts, tile, width), F32),
            pltpu.VMEM((slots, 2, 2, 2, tile, full), BF16),
            pltpu.VMEM((slots, 2, 2, tile, full), BF16),
            pltpu.VMEM((slots, 2, tile, full), BF16),
            pltpu.VMEM((slots, 2, tile, full), BF16),
            pltpu.VMEM((groups - 1, kinds, rows, cols), BF16),
            pltpu.SemaphoreType.DMA((slots,)),
            pltpu.SemaphoreType.DMA((slots,)),
            pltpu.SemaphoreType.DMA((slots,)),
            pltpu.SemaphoreType.DMA((slots,)),
            pltpu.SemaphoreType.DMA((groups - 1,)),
            pltpu.SemaphoreType.DMA((groups - 1,)),
        ],
        compiler_params=pltpu.CompilerParams(
            vmem_limit_bytes=60 << 20, collective_id=1, has_side_effects=True),
        cost_estimate=pl.CostEstimate(
            flops=60_000_000_000, bytes_accessed=24_000_000, transcendentals=14_000_000),
        name="attend_back",
    )(lam, queries, kv_all, gg, gain, mixed, second, lse, *tables, wgrads)


def dot_turned(left, right):
    return lax.dot_general(left, right, (((1,), (1,)), ((), ())), preferred_element_type=F32)


def dot_rows(left, right):
    return lax.dot_general(left, right, (((0,), (0,)), ((), ())), preferred_element_type=F32)


class LineSum:
    def __init__(self, axis, size, own, from_left, from_right, sems):
        self.axis, self.size = axis, size
        self.me = lax.axis_index(axis)
        self.own, self.buffers, self.sems = own, (from_left, from_right), sems

    def copy(self, q, t, side):
        target = self.size - 1 - t + self.me if side == 0 else t - (self.size - 1) + self.me
        target = jnp.clip(target, 0, self.size - 1)
        neighbour = jnp.clip(self.me + (1 if side == 0 else -1), 0, self.size - 1)
        return target, mesh_copy(
            self.own.at[q, target], self.buffers[side].at[q, t], self.sems.at[0, side, q, t],
            self.sems.at[1, side, q, t], {self.axis: neighbour})

    def rank(self, side):
        return self.me if side == 0 else self.size - 1 - self.me

    def step(self, q, t):
        for side in range(2):
            rank = self.rank(side)
            target, copy = self.copy(q, t, side)

            if t > 0:
                @pl.when((rank <= t) & (rank > 0))
                def _():
                    self.copy(q, t - 1, side)[1].wait_recv()
                    self.own[q, target] = (
                        self.own[q, target].astype(F32)
                        + self.buffers[side][q, t - 1].astype(F32)).astype(BF16)

            @pl.when(rank <= t)
            def _():
                copy.start()

    def total(self, q, acc):
        acc[...] = self.own[q, self.me].astype(F32)
        for side in range(2):
            @pl.when(self.rank(side) > 0)
            def _():
                self.copy(q, self.size - 2, side)[1].wait_recv()
                acc[...] += self.buffers[side][q, self.size - 2].astype(F32)

    def drain(self, q):
        for t in range(self.size - 1):
            for side in range(2):
                @pl.when(self.rank(side) <= t)
                def _():
                    self.copy(q, t, side)[1].wait_send()


def line_scratch(chunks, size, rows, width):
    return [
        pltpu.VMEM((chunks, size, rows, width), BF16),
        pltpu.VMEM((chunks, size - 1, rows, width), BF16),
        pltpu.VMEM((chunks, size - 1, rows, width), BF16),
        pltpu.VMEM((rows, width), F32),
        pltpu.SemaphoreType.DMA((2, 2, chunks, size - 1)),
    ]


def finish_kernel(dims, groups, lines, gq_ref, gk_ref, gv_ref, wq_ref, wk_ref, wv_ref, normed_ref,
                  branch_ref, grouped_ref, inputs_ref, gh_ref, gain_ref, small_ref, bo_ref,
                  ig_ref, wsum_ref, vec_ref, bout_ref,
                  own_ref, left_ref, right_ref, acc_ref, line_sem,
                  wloc_ref, wr1_ref, wr2_ref, mixer_ref, va_ref, vb_ref, vc_ref, v2_ref,
                  w1_sem, w2_sem, va_sem, vb_sem, vc_sem, bo_sem):
    slots, parts, heads, tile, width, strip = dims
    full = heads * width
    model = normed_ref.shape[-1]
    chunks = own_ref.shape[0]
    per = slots // chunks
    part = lax.axis_index("ctx")
    row = lax.axis_index("dp")
    place = lax.axis_index("head")
    core = part % 2
    y = part // 2
    other_core = 1 - core
    me = row * 2 + y
    sibling = {"ctx": y * 2 + other_core}

    def group_device(index):
        return {"dp": index // 2, "ctx": (index % 2) * 2 + core}

    others = [lax.rem(me + step, groups) for step in range(1, groups)]
    line_others = [lax.rem(place + step, lines) for step in range(1, lines)]
    targets = [lax.rem(part + step, parts) for step in range(1, parts)]
    greet([sibling, {"ctx": (1 - y) * 2 + other_core}]
          + [group_device(index) for index in others]
          + [{"head": index} for index in line_others])
    line = LineSum("head", lines, own_ref, left_ref, right_ref, line_sem)
    mixer_ref[...] = jnp.zeros_like(mixer_ref)

    def out_copy(step):
        return mesh_copy(bo_ref.at[targets[step]], bout_ref.at[:, part], bo_sem.at[0, step],
                         bo_sem.at[1, step], {"ctx": targets[step]})

    block = 256

    def product(q):
        grads = [ref[q * per:(q + 1) * per].reshape(per * tile, full)
                 for ref in (gq_ref, gk_ref, gv_ref)]

        def columns(index, carry):
            cols = pl.ds(pl.multiple_of(index * block, block), block)
            terms = dot_turned(grads[0], wq_ref[cols, :])
            terms += dot_turned(grads[1], wk_ref[cols, :])
            terms += dot_turned(grads[2], wv_ref[cols, :])
            terms = terms.astype(BF16)
            for p in range(per):
                for z in range(lines):
                    own_ref[q, z, p * strip:(p + 1) * strip, cols] = (
                        terms[p * tile + z * strip:p * tile + (z + 1) * strip])
            return carry

        lax.fori_loop(0, model // block, columns, 0)

    rows = wsum_ref.shape[1]
    narrow = 128

    def weight_term(kind):
        rows_ref = branch_ref if kind == 3 else normed_ref
        grad_ref = (gq_ref, gk_ref, gv_ref, grouped_ref)[kind]

        def columns(index, carry):
            cols = pl.ds(pl.multiple_of(index * narrow, narrow), narrow)
            term = jnp.zeros((narrow, full), F32)
            for s in range(0, slots, 2):
                left = rows_ref[s:s + 2, :, cols].reshape(2 * tile, narrow)
                grad = grad_ref[s:s + 2].reshape(2 * tile, full)
                term += dot(jnp.transpose(left), grad)
            wloc_ref[kind, cols] = term.astype(BF16)
            return carry

        lax.fori_loop(0, model // narrow, columns, 0)

    def share(index, which):
        return pl.ds(pl.multiple_of((index * 2 + which) * rows, 16), rows)

    def weights_out(kind, index):
        return mesh_copy(wloc_ref.at[kind, share(index, other_core)], wr1_ref.at[kind, index],
                         w1_sem.at[0, kind, index], w1_sem.at[1, kind, index], sibling)

    def weights_send(kind, step):
        index = others[step]
        return mesh_copy(wloc_ref.at[kind, share(index, core)], wr2_ref.at[step, kind],
                         w2_sem.at[0, kind, step], w2_sem.at[1, kind, step],
                         group_device(index))

    def weights_cross(kind):
        for index in range(groups):
            weights_out(kind, index).wait()

        def add(index, carry):
            wloc_ref[kind, share(index, core)] = (
                wloc_ref[kind, share(index, core)].astype(F32)
                + wr1_ref[kind, index].astype(F32)).astype(BF16)
            return carry

        lax.fori_loop(0, groups, add, 0)

    def weights_finish():
        for k in range(4):
            for step in range(groups - 1):
                weights_send(k, step).wait()
            total = wloc_ref[k, share(me, core)].astype(F32)
            for step in range(groups - 1):
                total = total + wr2_ref[step, k].astype(F32)
            wsum_ref[k] = total

    def close(q):
        line.total(q, acc_ref)
        grad = acc_ref[...]
        x = inputs_ref[q * per:(q + 1) * per].reshape(per * strip, model).astype(F32)
        scale = lax.rsqrt(jnp.mean(x * x, axis=1, keepdims=True) + EPSILON)
        mixer_ref[...] += jnp.sum((grad * (x * scale)).reshape(per * strip // 8, 8, model), axis=0)
        up = grad * gain_ref[...]
        result = (gh_ref[q * per:(q + 1) * per].reshape(per * strip, model) + scale * up
                  - x * (scale * scale * scale * jnp.mean(up * x, axis=1, keepdims=True)))
        ig_ref[q * per:(q + 1) * per] = result.astype(BF16).reshape(per, strip, model)

    for slot in range(chunks + lines - 1):
        if slot < chunks:
            product(slot)
        for t in range(lines - 1):
            if 0 <= slot - t < chunks:
                line.step(slot - t, t)
        if slot == 0:
            for step in range(parts - 1):
                out_copy(step).start()
            bout_ref[:, part] = bo_ref[part]
        if 1 <= slot < 5:
            weights_cross(slot - 1)
        if slot < 4:
            weight_term(slot)
            for index in range(groups):
                weights_out(slot, index).start()
        if 1 <= slot < 5:
            for step in range(groups - 1):
                weights_send(slot - 1, step).start()
        if slot - lines + 1 >= 0:
            close(slot - lines + 1)
    first_row = lax.broadcasted_iota(jnp.int32, small_ref.shape, 0) == 0
    mixer = jnp.broadcast_to(jnp.sum(mixer_ref[...], axis=0, keepdims=True), small_ref.shape)
    va_ref[0] = jnp.where(first_row, mixer, small_ref[...])
    swap = mesh_copy(va_ref.at[0], va_ref.at[1], va_sem.at[0], va_sem.at[1], sibling)
    swap.start()
    swap.wait()
    vb_ref[me] = va_ref[0] + va_ref[1]

    def group_copy(source, target, sem):
        return mesh_copy(vb_ref.at[source], vb_ref.at[source], vb_sem.at[0, sem],
                         vb_sem.at[1, source], group_device(target))

    for step, index in enumerate(others):
        group_copy(me, index, step).start()
    for step, index in enumerate(others):
        group_copy(index, index, step).wait_recv()
    total = vb_ref[0]
    for index in range(1, groups):
        total = total + vb_ref[index]
    vc_ref[place] = total
    v2_ref[...] = total

    def line_copy(source, target, sem):
        return mesh_copy(vc_ref.at[source], vc_ref.at[source], vc_sem.at[0, sem],
                         vc_sem.at[1, source], {"head": target})

    for step, index in enumerate(line_others):
        line_copy(place, index, step).start()
    for step, index in enumerate(line_others):
        line_copy(index, index, step).wait_recv()
    total = vc_ref[0]
    for index in range(1, lines):
        total = total + vc_ref[index]
    row_index = lax.broadcasted_iota(jnp.int32, total.shape, 0)
    vec_ref[...] = jnp.where(row_index < 2, total, v2_ref[...])
    weights_finish()
    for q in range(chunks):
        line.drain(q)
    for step in range(parts - 1):
        out_copy(step).wait()
    for step, index in enumerate(others):
        group_copy(me, index, step).wait_send()
    for step, index in enumerate(line_others):
        line_copy(place, index, step).wait_send()


def finish(dims, groups, lines, chunks, rows, *operands):
    slots, parts, heads, tile, width, strip = dims
    full = heads * width
    model = operands[6].shape[-1]
    pairs = operands[-1].shape[1]
    return pl.pallas_call(
        partial(finish_kernel, dims, groups, lines),
        out_shape=(
            jax.ShapeDtypeStruct((slots, strip, model), BF16),
            jax.ShapeDtypeStruct((4, rows, full), F32),
            jax.ShapeDtypeStruct((8, model), F32),
            jax.ShapeDtypeStruct((pairs, parts, strip, model), BF16),
        ),
        in_specs=specs(14, 0),
        out_specs=specs(4, 0),
        scratch_shapes=line_scratch(chunks, lines, slots // chunks * strip, model) + [
            pltpu.VMEM((4, model, full), BF16),
            pltpu.VMEM((4, groups, rows, full), BF16),
            pltpu.VMEM((groups - 1, 4, rows, full), BF16),
            pltpu.VMEM((8, model), F32),
            pltpu.VMEM((2, 8, model), F32),
            pltpu.VMEM((groups, 8, model), F32),
            pltpu.VMEM((lines, 8, model), F32),
            pltpu.VMEM((8, model), F32),
            pltpu.SemaphoreType.DMA((2, 4, groups)),
            pltpu.SemaphoreType.DMA((2, 4, groups - 1)),
            pltpu.SemaphoreType.DMA((2,)),
            pltpu.SemaphoreType.DMA((2, groups)),
            pltpu.SemaphoreType.DMA((2, lines)),
            pltpu.SemaphoreType.DMA((2, parts - 1)),
        ],
        compiler_params=pltpu.CompilerParams(
            vmem_limit_bytes=60 << 20, collective_id=2, has_side_effects=True),
        cost_estimate=pl.CostEstimate(
            flops=8_000_000_000, bytes_accessed=24_000_000, transcendentals=0),
        name="finish",
    )(*operands)


class LineGather:
    def __init__(self, axis, size, view, sems):
        self.axis, self.size, self.view, self.sems = axis, size, view, sems
        self.me = lax.axis_index(axis)

    def copy(self, q, t, side):
        source = jnp.clip(self.me - t if side == 0 else self.me + t, 0, self.size - 1)
        neighbour = jnp.clip(self.me + (1 if side == 0 else -1), 0, self.size - 1)
        return mesh_copy(
            self.view(q, source), self.view(q, source), self.sems.at[0, side, q, t],
            self.sems.at[1, side, q, source], {self.axis: neighbour})

    def rank(self, side):
        return self.me if side == 0 else self.size - 1 - self.me

    def step(self, q, t):
        for side in range(2):
            rank = self.rank(side)

            if t > 0:
                @pl.when(rank >= t)
                def _():
                    self.copy(q, t, side).wait_recv()

            if t < self.size - 1:
                @pl.when((rank >= t) & (rank < self.size - 1))
                def _():
                    self.copy(q, t, side).start()

    def drain(self, q):
        for t in range(self.size - 1):
            for side in range(2):
                rank = self.rank(side)

                @pl.when((rank >= t) & (rank < self.size - 1))
                def _():
                    self.copy(q, t, side).wait_send()


def open_kernel(dims, lines, chunks, x_ref, gain_ref, wq_ref, wk_ref, wv_ref, cosn_ref, sinn_ref,
                cot_ref, normed_ref, q_ref, kv_ref, cout_ref,
                line_sem, c_sem, sib_sem, far_sem, fwd_sem):
    slots, parts, heads, tile, width, strip = dims
    half = width // 2
    per = slots // chunks
    model = x_ref.shape[-1]
    part = lax.axis_index("ctx")
    place = lax.axis_index("head")
    core = part % 2
    y = part // 2
    sibling = {"ctx": y * 2 + 1 - core}
    across = {"ctx": (1 - y) * 2 + core}
    far = (1 - y) * 2 + core
    far_other = (1 - y) * 2 + 1 - core
    near = y * 2 + 1 - core
    targets = [lax.rem(part + step, parts) for step in range(1, parts)]
    greet([{"ctx": target} for target in targets]
          + [{"head": lax.rem(place + step, lines)} for step in range(1, lines)])
    line = LineGather(
        "head", lines, lambda q, s: normed_ref.at[pl.ds(q * per, per), s], line_sem)

    def norm(q):
        x = x_ref[q * per:(q + 1) * per].reshape(per * strip, model).astype(F32)
        scale = lax.rsqrt(jnp.mean(x * x, axis=1, keepdims=True) + EPSILON)
        low = (x * scale * gain_ref[...]).astype(BF16).reshape(per, strip, model)
        for p in range(per):
            normed_ref[q * per + p, place] = low[p]

    def cot_copy(step):
        return mesh_copy(cot_ref.at[:, targets[step]], cout_ref.at[part], c_sem.at[0, step],
                         c_sem.at[1, step], {"ctx": targets[step]})

    def chunk_view(source, q):
        return kv_ref.at[source, pl.ds(q * per, per)]

    def to_sibling(q):
        return mesh_copy(chunk_view(part, q), chunk_view(part, q), sib_sem.at[0, q],
                         sib_sem.at[1, q], sibling)

    def from_sibling(q):
        return mesh_copy(chunk_view(near, q), chunk_view(near, q), sib_sem.at[0, q],
                         sib_sem.at[1, q], sibling)

    def to_far(q):
        return mesh_copy(chunk_view(part, q), chunk_view(part, q), far_sem.at[0, q],
                         far_sem.at[1, q], across)

    def from_far(q):
        return mesh_copy(chunk_view(far, q), chunk_view(far, q), far_sem.at[0, q],
                         far_sem.at[1, q], across)

    def forward(q):
        return mesh_copy(chunk_view(far, q), chunk_view(far, q), fwd_sem.at[0, q],
                         fwd_sem.at[1, q], sibling)

    def forwarded(q):
        return mesh_copy(chunk_view(far_other, q), chunk_view(far_other, q), fwd_sem.at[0, q],
                         fwd_sem.at[1, q], sibling)

    def project(q):
        rows = normed_ref[q * per:(q + 1) * per].reshape(per * tile, model)
        for kind, weight_ref in ((1, wv_ref), (0, wk_ref), (2, wq_ref)):
            result = dot(rows, weight_ref[...])
            for p in range(per):
                at = q * per + p
                for h in range(heads):
                    lanes = slice(h * width, (h + 1) * width)
                    piece = result[p * tile:(p + 1) * tile, lanes]
                    if kind != 1:
                        piece = piece * cosn_ref[at] - swap_halves(piece, half) * sinn_ref[at]
                    if kind == 2:
                        q_ref[at, :, lanes] = piece.astype(BF16)
                    else:
                        kv_ref[part, at, kind, :, lanes] = piece.astype(BF16)

    for slot in range(chunks + lines - 1):
        if slot < chunks:
            norm(slot)
        for t in range(lines):
            if 0 <= slot - t < chunks:
                line.step(slot - t, t)
        if slot == 0:
            for step in range(parts - 1):
                cot_copy(step).start()
            cout_ref[part] = cot_ref[:, part]
        q = slot - lines + 1
        if q >= 0:
            project(q)
            to_far(q).start()
            to_sibling(q).start()
        if q >= 1:
            from_far(q - 1).wait_recv()
            forward(q - 1).start()
    from_far(chunks - 1).wait_recv()
    forward(chunks - 1).start()
    for step in range(parts - 1):
        cot_copy(step).wait()
    for q in range(chunks):
        line.drain(q)
        from_sibling(q).wait_recv()
        to_sibling(q).wait_send()
        to_far(q).wait_send()
    for q in range(chunks):
        forwarded(q).wait_recv()
        forward(q).wait_send()


def open_rows(dims, lines, chunks, *operands):
    slots, parts, heads, tile, width, strip = dims
    full = heads * width
    model = operands[0].shape[-1]
    pairs = operands[-1].shape[0]
    return pl.pallas_call(
        partial(open_kernel, dims, lines, chunks),
        out_shape=(
            jax.ShapeDtypeStruct((slots, lines, strip, model), BF16),
            jax.ShapeDtypeStruct((slots, tile, full), BF16),
            jax.ShapeDtypeStruct((parts, slots, 2, tile, full), BF16),
            jax.ShapeDtypeStruct((parts, pairs, strip, model), BF16),
        ),
        in_specs=specs(8, 0),
        out_specs=specs(4, 0),
        scratch_shapes=[
            pltpu.SemaphoreType.DMA((2, 2, chunks, lines)),
            pltpu.SemaphoreType.DMA((2, parts - 1)),
            pltpu.SemaphoreType.DMA((2, chunks)),
            pltpu.SemaphoreType.DMA((2, chunks)),
            pltpu.SemaphoreType.DMA((2, chunks)),
        ],
        compiler_params=pltpu.CompilerParams(
            vmem_limit_bytes=60 << 20, collective_id=3, has_side_effects=True),
        cost_estimate=pl.CostEstimate(
            flops=4_000_000_000, bytes_accessed=16_000_000, transcendentals=0),
        name="open_rows",
    )(*operands)


def greet_line(axis, size):
    place = lax.axis_index(axis)
    greet([{axis: lax.rem(place + step, size)} for step in range(1, size)])


def scatter_terms(own_ref, q, cols, terms, dims, lines):
    slots, parts, heads, tile, width, strip = dims
    for p in range(terms.shape[0] // tile):
        for z in range(lines):
            own_ref[q, z, p * strip:(p + 1) * strip, cols] = (
                terms[p * tile + z * strip:p * tile + (z + 1) * strip])


def line_turn(lines, chunks, summed, gathered, before, between, after=None):
    for slot in range(chunks + 2 * (lines - 1)):
        if slot < chunks:
            before(slot)
        for t in range(lines - 1):
            if 0 <= slot - t < chunks:
                summed.step(slot - t, t)
        q = slot - lines + 1
        if 0 <= q < chunks:
            between(q)
        for t in range(lines):
            if 0 <= q - t < chunks:
                gathered.step(q - t, t)
        if after is not None:
            after(slot)
    for q in range(chunks):
        summed.drain(q)
        gathered.drain(q)


def feed_open_kernel(dims, lines, chunks, grouped_ref, wo_ref, inputs_ref, gain_ref, grad_ref,
                     down_ref, hidden_ref, rows_ref, gact_ref,
                     own_ref, left_ref, right_ref, acc_ref, line_sem, gather_sem):
    slots, parts, heads, tile, width, strip = dims
    full = heads * width
    per = slots // chunks
    model = inputs_ref.shape[-1]
    units = down_ref.shape[0]
    block = 256
    place = lax.axis_index("head")
    greet_line("head", lines)
    summed = LineSum("head", lines, own_ref, left_ref, right_ref, line_sem)
    gathered = LineGather(
        "head", lines, lambda q, s: rows_ref.at[pl.ds(q * per, per), s], gather_sem)

    def before(q):
        left = grouped_ref[q * per:(q + 1) * per].reshape(per * tile, full)

        def columns(index, carry):
            cols = pl.ds(pl.multiple_of(index * block, block), block)
            scatter_terms(own_ref, q, cols, dot(left, wo_ref[:, cols]).astype(BF16), dims, lines)
            return carry

        lax.fori_loop(0, model // block, columns, 0)

    def between(q):
        summed.total(q, acc_ref)
        hidden = inputs_ref[q * per:(q + 1) * per].reshape(per * strip, model).astype(F32)
        hidden = hidden + acc_ref[...]
        hidden_ref[q * per:(q + 1) * per] = hidden.reshape(per, strip, model)
        scale = lax.rsqrt(jnp.mean(hidden * hidden, axis=1, keepdims=True) + EPSILON)
        low = (hidden * scale * gain_ref[...]).astype(BF16).reshape(per, strip, model)
        for p in range(per):
            rows_ref[q * per + p, place] = low[p]

    def extra(q):
        grads = grad_ref[q * per:(q + 1) * per].reshape(per * tile, model)

        def columns(index, carry):
            cols = pl.ds(pl.multiple_of(index * block, block), block)
            result = dot_turned(grads, down_ref[cols, :])
            gact_ref[q * per:(q + 1) * per, :, cols] = result.reshape(per, tile, block)
            return carry

        lax.fori_loop(0, units // block, columns, 0)

    def after(slot):
        if slot < chunks:
            extra(slot)

    line_turn(lines, chunks, summed, gathered, before, between, after)


def feed_open(dims, lines, chunks, *operands):
    slots, parts, heads, tile, width, strip = dims
    model, units = operands[1].shape[1], operands[5].shape[0]
    return pl.pallas_call(
        partial(feed_open_kernel, dims, lines, chunks),
        out_shape=(
            jax.ShapeDtypeStruct((slots, strip, model), F32),
            jax.ShapeDtypeStruct((slots, lines, strip, model), BF16),
            jax.ShapeDtypeStruct((slots, tile, units), F32),
        ),
        in_specs=specs(6, 0),
        out_specs=specs(3, 0),
        scratch_shapes=line_scratch(chunks, lines, slots // chunks * strip, model) + [
            pltpu.SemaphoreType.DMA((2, 2, chunks, lines)),
        ],
        compiler_params=pltpu.CompilerParams(
            vmem_limit_bytes=60 << 20, collective_id=4, has_side_effects=True),
        cost_estimate=pl.CostEstimate(
            flops=4_000_000_000, bytes_accessed=20_000_000, transcendentals=0),
        name="feed_open",
    )(*operands)


def feed_close_kernel(dims, lines, chunks, gg_ref, gu_ref, wg_ref, wu_ref, rows_ref, grad_ref,
                      act_ref, hidden_ref, cot_ref, gain_ref,
                      gh_ref, branch_ref, pair_ref, part_ref,
                      own_ref, left_ref, right_ref, acc_ref, line_sem, gather_sem,
                      terms_ref, landed_ref, pair_sem):
    slots, parts, heads, tile, width, strip = dims
    per = slots // chunks
    model = cot_ref.shape[-1]
    units = act_ref.shape[-1]
    block, narrow = 256, 128
    place = lax.axis_index("head")
    part_index = lax.axis_index("ctx")
    core = part_index % 2
    sibling = {"ctx": part_index + 1 - 2 * core}
    greet([sibling] + [{"head": lax.rem(place + step, lines)} for step in range(1, lines)])
    groups, rows = pair_ref.shape[1:3]

    def share(index, which):
        return pl.ds(pl.multiple_of((index * 2 + which) * rows, 16), rows)

    def pair_copy(kind, index):
        return mesh_copy(terms_ref.at[kind, share(index, 1 - core)], landed_ref.at[kind, index],
                         pair_sem.at[0, kind, index], pair_sem.at[1, kind, index], sibling)

    def pair_sum(kind):
        for index in range(groups):
            pair_copy(kind, index).wait()

        def add(index, carry):
            pair_ref[kind, index] = (
                terms_ref[kind, share(index, core)].astype(F32)
                + landed_ref[kind, index].astype(F32)).astype(BF16)
            return carry

        lax.fori_loop(0, groups, add, 0)

    summed = LineSum("head", lines, own_ref, left_ref, right_ref, line_sem)
    gathered = LineGather(
        "head", lines, lambda q, s: branch_ref.at[pl.ds(q * per, per), s], gather_sem)
    part_ref[...] = jnp.zeros_like(part_ref)

    def weight_term(kind):
        left_rows = grad_ref if kind == 2 else rows_ref
        right_rows = (gg_ref, gu_ref, act_ref)[kind]

        def columns(index, carry):
            cols = pl.ds(pl.multiple_of(index * narrow, narrow), narrow)
            term = jnp.zeros((narrow, units), F32)
            for s in range(0, slots, 2):
                left = left_rows[s:s + 2, :, cols].reshape(2 * tile, narrow)
                term += dot(jnp.transpose(left), right_rows[s:s + 2].reshape(2 * tile, units))
            terms_ref[kind, cols] = term.astype(BF16)
            return carry

        lax.fori_loop(0, model // narrow, columns, 0)

    def before(q):
        gate = gg_ref[q * per:(q + 1) * per].reshape(per * tile, units)
        up = gu_ref[q * per:(q + 1) * per].reshape(per * tile, units)

        def columns(index, carry):
            cols = pl.ds(pl.multiple_of(index * block, block), block)
            terms = dot_turned(gate, wg_ref[cols, :]) + dot_turned(up, wu_ref[cols, :])
            scatter_terms(own_ref, q, cols, terms.astype(BF16), dims, lines)
            return carry

        lax.fori_loop(0, model // block, columns, 0)

    def between(q):
        summed.total(q, acc_ref)
        grad = acc_ref[...]
        hidden = hidden_ref[q * per:(q + 1) * per].reshape(per * strip, model)
        scale = lax.rsqrt(jnp.mean(hidden * hidden, axis=1, keepdims=True) + EPSILON)
        part_ref[...] += jnp.sum(
            (grad * (hidden * scale)).reshape(per * strip // 8, 8, model), axis=0)
        up = grad * gain_ref[...]
        result = (cot_ref[q * per:(q + 1) * per].reshape(per * strip, model).astype(F32)
                  + scale * up
                  - hidden * (scale * scale * scale * jnp.mean(up * hidden, axis=1, keepdims=True)))
        gh_ref[q * per:(q + 1) * per] = result.reshape(per, strip, model)
        low = result.astype(BF16).reshape(per, strip, model)
        for p in range(per):
            branch_ref[q * per + p, place] = low[p]

    def after(slot):
        if slot < 3:
            weight_term(slot)
            for index in range(groups):
                pair_copy(slot, index).start()
        if lines <= slot < lines + 3:
            pair_sum(slot - lines)

    line_turn(lines, chunks, summed, gathered, before, between, after)


def feed_close(dims, groups, lines, chunks, *operands):
    slots, parts, heads, tile, width, strip = dims
    model, units = operands[8].shape[-1], operands[6].shape[-1]
    return pl.pallas_call(
        partial(feed_close_kernel, dims, lines, chunks),
        out_shape=(
            jax.ShapeDtypeStruct((slots, strip, model), F32),
            jax.ShapeDtypeStruct((slots, lines, strip, model), BF16),
            jax.ShapeDtypeStruct((3, groups, model // groups // 2, units), BF16),
            jax.ShapeDtypeStruct((8, model), F32),
        ),
        in_specs=specs(10, 0),
        out_specs=specs(4, 0),
        scratch_shapes=line_scratch(chunks, lines, slots // chunks * strip, model) + [
            pltpu.SemaphoreType.DMA((2, 2, chunks, lines)),
            pltpu.VMEM((3, model, units), BF16),
            pltpu.VMEM((3, groups, model // groups // 2, units), BF16),
            pltpu.SemaphoreType.DMA((2, 3, groups)),
        ],
        compiler_params=pltpu.CompilerParams(
            vmem_limit_bytes=60 << 20, collective_id=5, has_side_effects=True),
        cost_estimate=pl.CostEstimate(
            flops=16_000_000_000, bytes_accessed=40_000_000, transcendentals=0),
        name="feed_close",
    )(*operands)


def per_device(
    inputs,
    block_order,
    mixer_gain,
    query_weight,
    key_weight,
    value_weight,
    lambda_qone,
    lambda_kone,
    lambda_qtwo,
    lambda_ktwo,
    group_gain,
    output_weight,
    feed_gain,
    gate_weight,
    up_weight,
    down_weight,
    cotangent,
):
    seq_count, pair_count, short_rows, model_width = inputs.shape
    assert seq_count == 1
    parts = lax.axis_size("ctx")
    head_total = lax.axis_size("head")
    part = lax.axis_index("ctx")
    head_place = lax.axis_index("head")
    block_len = short_rows * head_total
    slots = block_order.shape[1]
    heads_here, head_dim = lambda_qone.shape
    qwidth = query_weight.shape[1]
    width = 2 * head_dim
    tile = block_len // parts
    strip = short_rows // parts
    dims = (slots, parts, heads_here, tile, width, strip)
    row_count = slots * tile
    order = block_order.reshape(slots)
    slot_of = jnp.argsort(order).astype(jnp.int32)
    index = jnp.arange(tile, dtype=jnp.int32)
    row_offsets = (index // strip) * short_rows + part * strip + index % strip
    own_places = jnp.arange(slots, dtype=jnp.int32)[:, None] * block_len + row_offsets[None, :]
    groups = lax.axis_size("dp") * parts // 2
    quarter = head_dim // 2
    frequency = THETA ** (-jnp.arange(quarter, dtype=jnp.float32) / quarter)
    angles = own_places.astype(F32)[:, None, :] * frequency[None, :, None]
    cos_turned, sin_turned = jnp.cos(angles), jnp.sin(angles)
    cos_rows = jnp.tile(cos_turned.transpose(0, 2, 1), (1, 1, 4))
    sin_rows = jnp.tile(sin_turned.transpose(0, 2, 1), (1, 1, 4))
    lane = jnp.arange(width)
    sin_rows = jnp.where(lane % head_dim < quarter, sin_rows, -sin_rows)
    tables = (cos_turned, sin_turned, cos_rows, sin_rows)
    lambda_one = jnp.exp(jnp.sum(lambda_qone * lambda_kone, axis=-1))
    lambda_two = jnp.exp(jnp.sum(lambda_qtwo * lambda_ktwo, axis=-1))
    lambda_head = lambda_one - lambda_two + LAMBDA_INIT
    split_shape = (slots, tile, heads_here, 2, head_dim)
    rows_shape = (slots, tile, model_width)

    def spread(rows):
        cut = rows.reshape(pair_count, parts, strip, model_width).transpose(1, 0, 2, 3)
        cut = lax.all_to_all(cut, "ctx", 0, 0, tiled=True)
        return jnp.take(cut.reshape(slots, strip, model_width), slot_of, axis=0, mode="clip")

    def unspread(rows):
        cut = jnp.take(rows, order, axis=0, mode="clip").reshape(parts, pair_count, strip, model_width)
        cut = lax.all_to_all(cut, "ctx", 0, 0, tiled=True)
        return cut.transpose(1, 0, 2, 3).reshape(1, pair_count, short_rows, model_width)

    inputs_here = spread(inputs)
    tokens = inputs_here.astype(jnp.float32)
    part_shape = (slots, tile, qwidth)
    cut_shape = (pair_count, parts, strip, model_width)
    normed_rows, queries, kv_all, cotangent_slots = open_rows(
        dims, head_total, 8, inputs_here, mixer_gain.reshape(1, model_width), query_weight,
        key_weight, value_weight, cos_rows, sin_rows, cotangent.reshape(cut_shape))
    cotangent_here = jnp.take(
        cotangent_slots.reshape(slots, strip, model_width), slot_of, axis=0, mode="clip")
    grad_rows = lax.all_gather(cotangent_here, "head", axis=1, tiled=True)
    part_arr = part.reshape(1).astype(jnp.int32)
    gain_col = group_gain.reshape(qwidth, 1)
    grouped, mixed, second, lse = attend(
        dims, part_arr, lambda_head, queries, kv_all,
        gain_col)
    grouped, grad_rows = lax.optimization_barrier((grouped, grad_rows))
    hidden, feed_rows, grad_activ = feed_open(
        dims, head_total, 8, grouped, output_weight, inputs_here,
        feed_gain.reshape(1, model_width), grad_rows, down_weight)
    feed_rows = feed_rows.reshape(row_count, model_width)
    grad_activ = grad_activ.reshape(row_count, grad_activ.shape[-1])
    gate_vals = jnp.dot(feed_rows, gate_weight, preferred_element_type=jnp.float32)
    up_vals = jnp.dot(feed_rows, up_weight, preferred_element_type=jnp.float32)
    gate_sigmoid = jax.nn.sigmoid(gate_vals)
    silu_gate = gate_vals * gate_sigmoid
    activation = (silu_gate * up_vals).astype(jnp.bfloat16)
    grad_gate = (
        grad_activ * up_vals * gate_sigmoid * (1.0 + gate_vals * (1.0 - gate_sigmoid))
    ).astype(jnp.bfloat16)
    grad_up = (grad_activ * silu_gate).astype(jnp.bfloat16)
    unit_shape = (slots, tile, activation.shape[-1])
    grad_hidden, branch_rows, wgrads, feed_part = feed_close(
        dims, groups, head_total, 4, grad_gate.reshape(unit_shape), grad_up.reshape(unit_shape),
        gate_weight, up_weight, feed_rows.reshape(slots, tile, model_width), grad_rows,
        activation.reshape(unit_shape), hidden, cotangent_here, feed_gain.reshape(1, model_width))
    feed_part = jnp.sum(feed_part, axis=0)
    branch_rows = branch_rows.reshape(row_count, model_width)
    feed_terms = jnp.dot(activation, down_weight, preferred_element_type=jnp.float32).reshape(
        rows_shape
    )
    branch_rows, feed_terms = lax.optimization_barrier((branch_rows, feed_terms.astype(BF16)))
    feed_sum = lax.psum_scatter(feed_terms, "head", scatter_dimension=1, tiled=True)
    grad_grouped = contract_cols(output_weight, branch_rows)
    shares = lax.axis_size("dp") * parts
    grad_query, grad_key, grad_value, group_part, lambda_part, feed_sums = attend_back(
        dims, groups, lambda_head, queries, kv_all,
        grad_grouped, gain_col, mixed, second, lse, tables, wgrads)
    feed_sum, grad_query = lax.optimization_barrier((feed_sum, grad_query))
    block_out = (hidden + feed_sum.astype(F32)).astype(BF16)
    group_part = jnp.sum(group_part, axis=1) * SHRINK
    lambda_part = jnp.sum(lambda_part, axis=(1, 2))
    third = jnp.pad(
        jnp.concatenate([group_part, lambda_part]), (0, model_width - qwidth - heads_here))
    small = jnp.pad(jnp.stack([jnp.zeros_like(feed_part), feed_part, third]), ((0, 5), (0, 0)))
    grad_rows_shape = (slots, tile, model_width)
    block_slots = jnp.take(block_out, order, axis=0, mode="clip").reshape(
        parts, pair_count, strip, model_width)
    input_grad, attn_sums, vectors, block_out = finish(
        dims, groups, head_total, 4, model_width // shares, grad_query, grad_key, grad_value,
        query_weight, key_weight, value_weight, normed_rows.reshape(grad_rows_shape),
        branch_rows.reshape(grad_rows_shape), grouped.reshape(part_shape), inputs_here,
        grad_hidden, mixer_gain.reshape(1, model_width), small, block_slots)
    block_out = block_out.reshape(inputs.shape)
    input_grad = unspread(input_grad).astype(F32)
    group_grad = vectors[2, :qwidth]
    lambda_grad = vectors[2, qwidth:qwidth + heads_here]
    qone_grad = (lambda_grad * lambda_one)[:, None] * lambda_kone
    kone_grad = (lambda_grad * lambda_one)[:, None] * lambda_qone
    qtwo_grad = -(lambda_grad * lambda_two)[:, None] * lambda_ktwo
    ktwo_grad = -(lambda_grad * lambda_two)[:, None] * lambda_qtwo
    return (
        block_out,
        input_grad,
        vectors[0],
        attn_sums[0],
        attn_sums[1],
        attn_sums[2],
        qone_grad,
        kone_grad,
        qtwo_grad,
        ktwo_grad,
        group_grad,
        attn_sums[3].T,
        vectors[1],
        feed_sums[0],
        feed_sums[1],
        feed_sums[2].T,
    )


def solution(mesh):
    return jax.shard_map(
        per_device,
        mesh=mesh,
        in_specs=(
            P("dp", "ctx", "head", None),
            P("dp", None),
            P(),
            P(None, "head"),
            P(None, "head"),
            P(None, "head"),
            P("head", None),
            P("head", None),
            P("head", None),
            P("head", None),
            P("head"),
            P("head", None),
            P(),
            P(None, "head"),
            P(None, "head"),
            P("head", None),
            P("dp", "ctx", "head", None),
        ),
        out_specs=(
            P("dp", "ctx", "head", None),
            P("dp", "ctx", "head", None),
            P(),
            P(("dp", "ctx"), "head"),
            P(("dp", "ctx"), "head"),
            P(("dp", "ctx"), "head"),
            P("head", None),
            P("head", None),
            P("head", None),
            P("head", None),
            P("head"),
            P("head", ("dp", "ctx")),
            P(),
            P(("dp", "ctx"), "head"),
            P(("dp", "ctx"), "head"),
            P("head", ("dp", "ctx")),
        ),
        check_vma=False,
    )
```
